32 devices in a mesh: rows: 2 (over x), cols: 8 (over z, y), frames: 2 (over core).
Axes of the slice: x: 2, y: 2, z: 4, core: 2. Of those that a mesh axis runs over, the one named last changes fastest.
Arguments:
- lidar_map: bfloat16 [8, 96, 192, 256], P('frames', ('rows', 'cols')), parts along dimension 0, may hold values from -6 to 6
- camera_map: bfloat16 [8, 96, 192, 80], P('frames', None, ('rows', 'cols')), parts along dimension 0, may hold values from -6 to 6
- joined_weight: bfloat16 [3, 3, 336, 256], replicated, may hold values from -0.15625 to 0.15625
- joined_bias: float32 [256], replicated, may hold values from -0.5 to 0.5
- block_weight: bfloat16 [3, 3, 256, 128], replicated, may hold values from -0.1875 to 0.1875
- block_bias: float32 [128], replicated, may hold values from -0.5 to 0.5
- down_weight: bfloat16 [3, 3, 128, 256], replicated, may hold values from -0.25 to 0.25
- down_bias: float32 [256], replicated, may hold values from -0.5 to 0.5
- proj_weight: bfloat16 [256, 128], replicated, may hold values from -0.5 to 0.5
- proj_bias: float32 [128], replicated, may hold values from -0.5 to 0.5
Outputs:
- encoded: bfloat16 [8, 96, 192, 256], P('frames', 'rows', 'cols'), parts along dimension 0
The draws below stay inside these ranges and needn't reach their ends.
There are 2 independent parts, one for each index of `frames`. The reference program is written for one: setup_inputs(seed, part) draws one part's arguments, and reference() takes and returns one part's arrays. A program takes and returns all parts, laid end to end along the dimension named above; an argument that names none is the same for every part. Nothing has to cross between parts.
All inputs are finite; a program needn't handle non-finite values.
Results may differ from the reference program's by a relative error of at most 0.0058.
Values may be sent and summed in bfloat16 or wider, within the bound.
No kernel may reach another device: no remote copies, remote signals or barrier semaphores. Data moves between devices by JAX's collectives and lax.ppermute only.
A program may use at most 64 MiB of HBM per device.

```python
import jax
import jax.numpy as jnp
from jax import lax

FR = 4
LIDAR_CH = 256
CAM_CH = 80
JOINED_CH = 256
MID = 128
DEEP = 256
H = 96
W = 192


def levels(stream_key, dims, shards, least, high):
    def one(position, shards_of):
        steps = jax.random.uniform(jax.random.fold_in(jax.random.fold_in(stream_key, 6), position), (shards_of,), jnp.float32, least / len(shards), high / len(shards))
        return jnp.repeat(jnp.exp(steps), dims[position] // shards_of).reshape((-1,) + (1,) * (len(dims) - position - 1))

    gain = one(*shards[0])
    for cut in shards[1:]:
        gain = gain * one(*cut)
    return gain


def gaussian(rng, shape, spread, limit, shards=(), held_as=jnp.bfloat16):
    loudness = levels(rng, shape, shards, -0.22, 0.18) if shards else 1.0
    array = jax.random.normal(rng, shape, jnp.float32) * spread * loudness
    return jnp.minimum(jnp.maximum(array, -limit), limit).astype(held_as)


def setup_inputs(seed: int = 0, part: int = 0) -> dict:
    key_list = jax.random.split(jax.random.key(seed), 11)
    part_keys = jax.random.split(jax.random.fold_in(key_list[10], part), 11)
    lidar_map = gaussian(part_keys[0], (FR, H, W, LIDAR_CH), 1.0, 6.0, ((1, 16),))
    camera_map = gaussian(part_keys[1], (FR, H, W, CAM_CH), 1.0, 6.0, ((2, 16),))
    joined_weight = gaussian(key_list[2], (3, 3, LIDAR_CH + CAM_CH, JOINED_CH), (4 * (LIDAR_CH + CAM_CH)) ** -0.5, 0.15625)
    joined_bias = jnp.clip(jax.random.uniform(key_list[3], (JOINED_CH,), jnp.float32, -0.5, 0.5), -0.5, 0.5)
    block_weight = gaussian(key_list[4], (3, 3, JOINED_CH, MID), (4 * JOINED_CH) ** -0.5, 0.1875)
    block_bias = jnp.clip(jax.random.uniform(key_list[5], (MID,), jnp.float32, -0.5, 0.5), -0.5, 0.5)
    down_weight = gaussian(key_list[6], (3, 3, MID, DEEP), (4 * MID) ** -0.5, 0.25)
    down_bias = jnp.clip(jax.random.uniform(key_list[7], (DEEP,), jnp.float32, -0.5, 0.5), -0.5, 0.5)
    proj_weight = gaussian(key_list[8], (DEEP, MID), (DEEP // 2) ** -0.5, 0.5)
    proj_bias = jnp.clip(jax.random.uniform(key_list[9], (MID,), jnp.float32, -0.5, 0.5), -0.5, 0.5)
    return dict(lidar_map=lidar_map, camera_map=camera_map, joined_weight=joined_weight, joined_bias=joined_bias, block_weight=block_weight, block_bias=block_bias, down_weight=down_weight, down_bias=down_bias, proj_weight=proj_weight, proj_bias=proj_bias)


def conv_same(inputs, kernel, stride):
    return lax.conv_general_dilated(inputs, kernel, (stride, stride), ((1, 1), (1, 1)), dimension_numbers=("NHWC", "HWIO", "NHWC"), preferred_element_type=jnp.float32)


def reference(lidar_map, camera_map, joined_weight, joined_bias, block_weight, block_bias, down_weight, down_bias, proj_weight, proj_bias):
    stacked = jnp.concatenate([lidar_map, camera_map], axis=-1)
    joined = jax.nn.relu(conv_same(stacked, joined_weight, 1) + joined_bias).astype(jnp.bfloat16)
    block = jax.nn.relu(conv_same(joined, block_weight, 1) + block_bias).astype(jnp.bfloat16)
    deep = jax.nn.relu(conv_same(block, down_weight, 2) + down_bias).astype(jnp.bfloat16)
    branch = jax.nn.relu(jnp.einsum("fijc,cd->fijd", deep.astype(jnp.float32), proj_weight.astype(jnp.float32)) + proj_bias).astype(jnp.bfloat16)
    upsampled = jnp.repeat(jnp.repeat(branch, 2, axis=1), 2, axis=2)
    return jnp.concatenate([block, upsampled], axis=-1)
```

```python
import jax
import jax.numpy as jnp
from jax import lax
from jax.experimental import pallas as pl
from jax.experimental.pallas import tpu as pltpu
from jax.sharding import PartitionSpec as P


AXES = ("rows", "cols")
HALVES = 2
SIDE = 4
UP, DOWN = 3, 2
BF = jnp.bfloat16


def rounded(n, to):
    return -(-n // to) * to


def whole(a):
    return pl.BlockSpec(a.shape, lambda *_: (0,) * a.ndim)


def weights_kernel(joint, square, w1, w2, *, lidar, camera):
    joined, block = joint.shape[1], square.shape[1]
    ch = lidar + camera
    deep = w1.shape[0] // 3
    for dy in range(3):
        base = dy * deep
        for dx in range(3):
            at = (dy * 3 + dx) * ch
            w1[base + dx * lidar : base + (dx + 1) * lidar, :] = joint[at : at + lidar, :]
            to = base + 3 * lidar + dx * camera
            w1[to : to + camera, :] = joint[at + lidar : at + ch, :]
        w1[base + 3 * ch : base + deep, :] = jnp.zeros((deep - 3 * ch, joined), BF)
    tall = square.shape[0]
    gap = w2.shape[0] - tall
    w2[0:tall, 0:block] = square[...]
    w2[tall:, 0:block] = jnp.zeros((gap, block), BF)
    w2[gap:, block:] = square[...]
    w2[0:gap, block:] = jnp.zeros((gap, block), BF)


def camera_pack_kernel(pos, x, *refs, groups, tr, span):
    outs, pad = refs[:groups], refs[groups]
    frames, _, ch, rows = x.shape
    lanes = pad.shape[2]
    place = pos[0]
    pad[...] = jnp.zeros(pad.shape, jnp.float32)
    for f in range(frames):
        pad[f, :, 0:rows] = x[f, 0].astype(jnp.float32)
    width = frames * span
    lane = lax.broadcasted_iota(jnp.int32, (ch, width), 1) // span
    for p in range(groups):
        start = lax.rem(place + p, groups) * tr - UP
        y = jnp.zeros((ch, width), jnp.float32)
        for f in range(frames):
            turned = pltpu.roll(pad[f], lax.rem(f * span - start + 2 * lanes, lanes), 1)
            y = jnp.where(lane == f, turned[:, 0:width], y)
        outs[p][0] = y.astype(BF)


def camera_unpack_kernel(pos, *refs, groups, sc, cam_ch):
    strips = refs[:groups]
    left, right, out, stage, cells = refs[groups:]
    group = pos[0]
    lanes = left.shape[2]
    pitch = cells.shape[1]
    for p in range(groups):
        q = lax.rem(group - p + groups, groups)
        stage[pl.ds(UP + q * sc, sc)] = strips[p][...]
    stage[0:UP] = left[...]
    n = UP + groups * sc + DOWN
    stage[n - DOWN : n] = right[...]
    lead = SIDE - UP
    cells[:, 0:8, :] = jnp.zeros((lanes, 8, 128), jnp.float32)
    low = (lead + n) // 8 * 8
    cells[:, low:, :] = jnp.zeros((lanes, pitch - low, 128), jnp.float32)
    for c in range(n):
        x = stage[c].astype(jnp.float32)
        x = jnp.concatenate([x, jnp.zeros((128 - cam_ch, lanes), jnp.float32)], axis=0)
        cells[:, lead + c, :] = x.T
    step = 8
    flat = step * pitch
    lane = lax.broadcasted_iota(jnp.int32, (flat, 128), 1)

    def widen(i, _):
        x = cells[pl.ds(i * step, step)].reshape(flat, 128)
        taps = [pltpu.roll(x, 1, 0), x, pltpu.roll(x, flat - 1, 0)]
        for v in range(out.shape[2] // 128):
            y = jnp.zeros((flat, 128), jnp.float32)
            for t in range(3):
                lo, hi = t * cam_ch - v * 128, (t + 1) * cam_ch - v * 128
                if hi > 0 and lo < 128:
                    turned = pltpu.roll(taps[t], lo % 128, 1) if lo % 128 else taps[t]
                    y = jnp.where((lane >= lo) & (lane < hi), turned, y)
            out[pl.ds(i * step, step), :, v * 128 : (v + 1) * 128] = y.astype(BF).reshape(step, pitch, 128)
        return 0

    lax.fori_loop(0, lanes // step, widen, 0)


def pick_kernel(pos, *refs, parts, first, last, dim):
    sources = refs[:parts]
    tail, head, sems = refs[parts:]
    size = sources[0].shape[dim]

    def cut(ref, lo, n):
        return ref.at[(slice(None),) * dim + (pl.ds(lo, n),)]

    for d in range(parts):

        @pl.when(pos[0] == d)
        def _():
            pltpu.make_async_copy(cut(sources[d], size - last, last), tail, sems.at[0]).start()

        @pl.when(pos[1] == d)
        def _():
            pltpu.make_async_copy(cut(sources[d], 0, first), head, sems.at[1]).start()

    pltpu.make_async_copy(cut(sources[0], size - last, last), tail, sems.at[0]).wait()
    pltpu.make_async_copy(cut(sources[0], 0, first), head, sems.at[1]).wait()


def pick(arrays, tail_of, head_of, dim, name):
    shape = list(arrays[0].shape)
    shapes = []
    for n in (UP, DOWN):
        shape[dim] = n
        shapes.append(jax.ShapeDtypeStruct(tuple(shape), BF))
    return pl.pallas_call(
        lambda *refs: pick_kernel(*refs, parts=len(arrays), first=DOWN, last=UP, dim=dim),
        grid_spec=pltpu.PrefetchScalarGridSpec(
            num_scalar_prefetch=1,
            grid=(1,),
            in_specs=[pl.BlockSpec(memory_space=pl.ANY)] * len(arrays),
            out_specs=[pl.BlockSpec(memory_space=pl.ANY)] * 2,
            scratch_shapes=[pltpu.SemaphoreType.DMA((2,))],
        ),
        out_shape=shapes,
        name=name,
    )(jnp.stack([tail_of, head_of]).astype(jnp.int32), *arrays)


def conv_kernel(pos, *refs, parts, sh, tr, pitch, rows, cols):
    windows = refs[:parts]
    above, below, camera, w1, b1, w2, b2 = refs[parts : parts + 7]
    outs = refs[parts + 7 : parts + 7 + HALVES]
    tile, taps, mid, cells = refs[parts + 7 + HALVES :]
    group, member, half_id = pos[0], pos[1], pos[2]
    wide = windows[0].shape[2]
    lidar = windows[0].shape[3]
    joined = w1.shape[1]
    block = w2.shape[1] // 2

    @pl.when(pl.program_id(0) == 0)
    def _():
        tile[...] = jnp.zeros(tile.shape, BF)

    tile[0:UP, 0:wide, :] = above[0]
    for d in range(parts):
        source = lax.rem(member - d + parts, parts)
        tile[pl.ds(UP + source * sh, sh), 0:wide, :] = windows[d][0]
    tile[UP + tr : UP + tr + DOWN, 0:wide, :] = below[0]

    step = 6
    flat = step * pitch

    def shift(i, _):
        r = i * step
        x = tile[pl.ds(r, step)].reshape(flat, lidar)
        x32 = x.astype(jnp.float32)
        taps[pl.ds(r, step), :, 0:lidar] = pltpu.roll(x32, 1, 0).astype(BF).reshape(step, pitch, lidar)
        taps[pl.ds(r, step), :, lidar : 2 * lidar] = x.reshape(step, pitch, lidar)
        taps[pl.ds(r, step), :, 2 * lidar :] = pltpu.roll(x32, flat - 1, 0).astype(BF).reshape(step, pitch, lidar)
        return 0

    lax.fori_loop(0, (tr + 6) // step, shift, 0)

    n1 = 4
    m1 = n1 * pitch
    col0 = member * (wide - 2 * SIDE) - SIDE

    def first(i, _):
        r = i * n1
        lhs = []
        for dy in range(3):
            lhs.append(taps[pl.ds(r + dy, n1)].reshape(m1, 3 * lidar))
            lhs.append(camera[0, pl.ds(r + dy, n1)].reshape(m1, camera.shape[3]))
        acc = jnp.dot(jnp.concatenate(lhs, axis=1), w1[...], preferred_element_type=jnp.float32)
        v = jnp.maximum(acc + b1[...], 0.0)
        at = lax.broadcasted_iota(jnp.int32, (m1, joined), 0)
        row = group * tr - 2 + r + at // pitch
        col = col0 + at % pitch
        keep = (row >= 0) & (row < rows) & (col >= 0) & (col < cols)
        v = jnp.where(keep, v, 0.0)
        shape = (n1 // 2, 2, pitch, joined)
        p = pl.ds(i * (n1 // 2), n1 // 2)
        mid[p, :, :, 0:joined] = pltpu.roll(v, 1, 0).astype(BF).reshape(shape)
        mid[p, :, :, joined : 2 * joined] = v.astype(BF).reshape(shape)
        mid[p, :, :, 2 * joined :] = pltpu.roll(v, m1 - 1, 0).astype(BF).reshape(shape)
        return 0

    lax.fori_loop(0, (tr + 4) // n1, first, 0)

    n2 = (tr + 2) // 2
    m2 = n2 * pitch
    lhs = [mid[i // 2 : i // 2 + n2, i % 2].reshape(m2, 3 * joined) for i in range(4)]
    acc = jnp.dot(jnp.concatenate(lhs, axis=1), w2[...], preferred_element_type=jnp.float32)
    v = jnp.maximum(acc + b2[...], 0.0)
    at = lax.broadcasted_iota(jnp.int32, (m2, 2 * block), 0)
    half = lax.broadcasted_iota(jnp.int32, (m2, 2 * block), 1) // block
    row = group * tr - 1 + (at // pitch) * 2 + half
    col = col0 + at % pitch
    keep = (row >= 0) & (row < rows) & (col >= 0) & (col < cols)
    v = jnp.where(keep, v, 0.0)
    cells[:, 0] = v[:, :block].reshape(n2, pitch, block)
    cells[:, 1] = v[:, block:].reshape(n2, pitch, block)
    pairs = tr // 2
    w = (wide - 2 * SIDE) // HALVES
    for sub in range(HALVES):
        c = SIDE + sub * w
        even = cells[0:pairs, 1, c : c + w, :].astype(BF)
        odd = cells[1 : pairs + 1, 0, c : c + w, :].astype(BF)
        top = cells[0, 0, c : c + w, :]
        corner = jnp.broadcast_to(cells[pairs, 0, c - 1 : c, :], (w, block))
        edge = jnp.where(half_id == 0, top, corner).astype(BF)
        beside = cells[0:pairs, :, c - 1, :].reshape(tr, block).astype(BF)
        for h in range(HALVES):

            @pl.when(lax.rem(half_id + h, HALVES) == sub)
            def _():
                outs[h][0, 0:pairs, 0] = even
                outs[h][0, 0:pairs, 1] = odd
                outs[h][0, pairs, 0] = edge
                outs[h][0, pairs, 1] = beside


def encode_kernel(pos, *refs, parts, half_rows, w):
    pieces = refs[:parts]
    w3, b3, wp, bp = refs[parts : parts + 4]
    out, grid, grown = refs[-3:]
    me = pos[0]
    block = pieces[0].shape[4]
    for h in range(parts):
        part = lax.rem(me - h + parts, parts)
        base = part * half_rows
        x = pieces[h]
        grid[pl.ds(base, half_rows), 1, 1 : w + 1, :] = x[0, 0:half_rows, 0].astype(jnp.float32)
        grid[pl.ds(base + 1, half_rows), 0, 1 : w + 1, :] = x[0, 0:half_rows, 1].astype(jnp.float32)
        beside = x[0, half_rows, 1].astype(jnp.float32)
        for r in range(2 * half_rows):
            grid[base + r // 2, r % 2, 0:1, :] = beside[r : r + 1]
        edge = x[0, half_rows, 0].astype(jnp.float32)

        @pl.when(part == 0)
        def _():
            grid[0, 0, 1 : w + 1, :] = edge

        @pl.when(part == parts - 1)
        def _():
            grid[parts * half_rows, 0, 0:1, :] = edge[0:1]

    n = parts * half_rows
    jd = rounded(w // 2, 8)
    m = n * jd
    lhs = []
    for a in range(3):
        for b in range(3):
            x = grid[pl.ds(a // 2, n), a % 2, pl.ds(b, jd, stride=2), :]
            lhs.append(x.reshape(m, block).astype(BF))
    deep = jnp.dot(jnp.concatenate(lhs, axis=1), w3[...], preferred_element_type=jnp.float32)
    deep = jnp.maximum(deep + b3[...], 0.0).astype(BF)
    branch = jnp.dot(deep, wp[...], preferred_element_type=jnp.float32)
    branch = jnp.maximum(branch + bp[...], 0.0).astype(BF).astype(jnp.float32).reshape(n, jd, wp.shape[1])
    grown[:, pl.ds(0, jd, stride=2), :] = branch
    grown[:, pl.ds(1, jd, stride=2), :] = branch
    up = grown[:, 0:w, :].astype(BF)
    out[0, :, 0, :, 0:block] = grid[0:n, 1, 1 : w + 1, :].astype(BF)
    out[0, :, 1, :, 0:block] = grid[1 : n + 1, 0, 1 : w + 1, :].astype(BF)
    out[0, :, 0, :, block:] = up
    out[0, :, 1, :, block:] = up


def solution(mesh):
    n_rows, n_cols = mesh.shape["rows"], mesh.shape["cols"]
    members = n_cols // HALVES
    groups = n_rows * HALVES
    total = n_rows * n_cols

    def local(lidar, camera, joined_weight, joined_bias, block_weight, block_bias, down_weight, down_bias, proj_weight, proj_bias):
        frames, sh, cols, lidar_ch = lidar.shape
        rows, sc, cam_ch = camera.shape[1:]
        tr = sh * members
        tw = cols // members
        wide = tw + 2 * SIDE
        pitch = rounded(wide, 16)
        w = cols // n_cols
        joined = joined_weight.shape[3]
        block = block_weight.shape[3]
        place = lax.axis_index(AXES)
        group = place // members
        member = place % members
        cindex = lax.axis_index("cols")
        kgroup = cindex // members

        def send(x, pairs):
            return lax.ppermute(x, AXES, pairs)

        def across(x, by_group, by_member):
            pairs = []
            for g in range(groups):
                for j in range(members):
                    if 0 <= g + by_group < groups and 0 <= j + by_member < members:
                        pairs.append((g * members + j, (g + by_group) * members + j + by_member))
            return send(x, pairs)

        joint = joined_weight.reshape(-1, joined)
        square = block_weight.reshape(-1, block)
        deep1 = 3 * (3 * lidar_ch + rounded(3 * cam_ch, 256))
        w1, w2 = pl.pallas_call(
            lambda *refs: weights_kernel(*refs, lidar=lidar_ch, camera=cam_ch),
            out_shape=[
                jax.ShapeDtypeStruct((deep1, joined), BF),
                jax.ShapeDtypeStruct((4 * 3 * joined, 2 * block), BF),
            ],
            name="weights",
        )(joint, square)
        w3 = down_weight.reshape(-1, down_weight.shape[3])
        b1 = joined_bias.reshape(1, -1)
        b2 = jnp.concatenate([block_bias, block_bias]).reshape(1, -1)
        b3 = down_bias.reshape(1, -1)
        bp = proj_bias.reshape(1, -1)

        span = rounded(tr + UP + DOWN, 8)
        lanes = frames * span
        turned = jnp.transpose(camera, (0, 2, 3, 1))
        strip = jax.ShapeDtypeStruct((sc, cam_ch, lanes), BF)
        packed = pl.pallas_call(
            lambda *refs: camera_pack_kernel(*refs, groups=groups, tr=tr, span=span),
            grid_spec=pltpu.PrefetchScalarGridSpec(
                num_scalar_prefetch=1,
                grid=(sc,),
                in_specs=[pl.BlockSpec((frames, 1, cam_ch, rows), lambda c, p: (0, c, 0, 0))],
                out_specs=[pl.BlockSpec((1, cam_ch, lanes), lambda c, p: (c, 0, 0))] * groups,
                scratch_shapes=[pltpu.VMEM((frames, cam_ch, rounded(rows + span, 128)), jnp.float32)],
            ),
            out_shape=[strip] * groups,
            name="camera_pack",
        )(place.reshape(1).astype(jnp.int32), turned)
        arrived = [
            send(packed[p], [(s, ((s + p) % groups) * members + s // groups) for s in range(total)])
            for p in range(groups)
        ]
        tail, head = pick(arrived, (group + 1) % groups, group, 0, "camera_edges")
        left = across(tail, 0, 1)
        right = across(head, 0, -1)
        cam = pl.pallas_call(
            lambda *refs: camera_unpack_kernel(*refs, groups=groups, sc=sc, cam_ch=cam_ch),
            grid_spec=pltpu.PrefetchScalarGridSpec(
                num_scalar_prefetch=1,
                grid=(1,),
                in_specs=[whole(x) for x in arrived] + [whole(left), whole(right)],
                out_specs=pl.BlockSpec((lanes, pitch, rounded(3 * cam_ch, 256)), lambda i, p: (0, 0, 0)),
                scratch_shapes=[
                    pltpu.VMEM((tw + UP + DOWN, cam_ch, lanes), BF),
                    pltpu.VMEM((lanes, pitch, 128), jnp.float32),
                ],
            ),
            out_shape=jax.ShapeDtypeStruct((lanes, pitch, rounded(3 * cam_ch, 256)), BF),
            compiler_params=pltpu.CompilerParams(vmem_limit_bytes=48 * 2**20),
            name="camera_unpack",
        )(group.reshape(1).astype(jnp.int32), *arrived, left, right)
        cam = cam.reshape(frames, span, pitch, -1)

        step = frames // 2 if frames % 2 == 0 else frames
        padded = jnp.pad(lidar, ((0, 0), (0, 0), (SIDE, SIDE), (0, 0)))
        pos = jnp.stack([group, member, kgroup]).astype(jnp.int32)
        encoded = None
        for f0 in range(0, frames, step):
            windows = []
            for d in range(members):
                x = lax.dynamic_slice(padded, (f0, 0, ((member + d) % members) * tw, 0), (step, sh, wide, lidar_ch))
                if d:
                    x = send(x, [(g * members + j, g * members + (j + d) % members) for g in range(groups) for j in range(members)])
                windows.append(x)
            last, head = pick(windows, (member + 1) % members, member, 1, "lidar_edges")
            above = across(last, 1, 0)
            below = across(head, -1, 0)
            pairs2 = (tr + 2) // 2
            flops = 2 * step * pitch * ((tr + 4) * w1.shape[0] * joined + pairs2 * w2.shape[0] * 2 * block)
            framed = lambda a: pl.BlockSpec((1,) + a.shape[1:], lambda f, p: (f,) + (0,) * (a.ndim - 1))
            camf = pl.BlockSpec((1,) + cam.shape[1:], lambda f, p, f0=f0: (f + f0, 0, 0, 0))
            tiles = pl.pallas_call(
                lambda *refs: conv_kernel(*refs, parts=members, sh=sh, tr=tr, pitch=pitch, rows=rows, cols=cols),
                grid_spec=pltpu.PrefetchScalarGridSpec(
                    num_scalar_prefetch=1,
                    grid=(step,),
                    in_specs=[framed(x) for x in windows] + [framed(above), framed(below), camf, whole(w1), whole(b1), whole(w2), whole(b2)],
                    out_specs=[pl.BlockSpec((1, pairs2, 2, w, block), lambda f, p: (f, 0, 0, 0, 0))] * HALVES,
                    scratch_shapes=[
                        pltpu.VMEM((tr + 6, pitch, lidar_ch), BF),
                        pltpu.VMEM((tr + 6, pitch, 3 * lidar_ch), BF),
                        pltpu.VMEM(((tr + 4) // 2, 2, pitch, 3 * joined), BF),
                        pltpu.VMEM((pairs2, 2, pitch, block), jnp.float32),
                    ],
                ),
                out_shape=[jax.ShapeDtypeStruct((step, pairs2, 2, w, block), BF)] * HALVES,
                compiler_params=pltpu.CompilerParams(vmem_limit_bytes=48 * 2**20),
                cost_estimate=pl.CostEstimate(flops=flops, bytes_accessed=2 * 10**6 * step, transcendentals=0),
                name="convs",
            )(pos, *windows, above, below, cam, w1, b1, w2, b2)
            pieces = []
            for h in range(HALVES):
                pairs = []
                for s in range(total):
                    r, c = divmod(s, n_cols)
                    k, j = divmod(c, members)
                    pairs.append((s, r * n_cols + HALVES * j + (k + h) % HALVES))
                pieces.append(send(tiles[h], pairs))
            half_rows = tr // 2
            n = HALVES * half_rows
            jd = rounded(w // 2, 8)
            out_shape = jax.ShapeDtypeStruct((frames, n, 2, w, 2 * block), BF)
            old = [] if encoded is None else [encoded]
            encoded = pl.pallas_call(
                lambda *refs: encode_kernel(*refs, parts=HALVES, half_rows=half_rows, w=w),
                grid_spec=pltpu.PrefetchScalarGridSpec(
                    num_scalar_prefetch=1,
                    grid=(step,),
                    in_specs=[framed(x) for x in pieces] + [whole(w3), whole(b3), whole(proj_weight), whole(bp)] + [pl.BlockSpec(memory_space=pl.ANY)] * len(old),
                    out_specs=pl.BlockSpec((1, n, 2, w, 2 * block), lambda f, p, f0=f0: (f + f0, 0, 0, 0, 0)),
                    scratch_shapes=[
                        pltpu.VMEM((n + 1, 2, rounded(w + 1, 8) + 16, block), jnp.float32),
                        pltpu.VMEM((n, 2 * jd, block), jnp.float32),
                    ],
                ),
                out_shape=out_shape,
                input_output_aliases={5 + HALVES: 0} if old else {},
                compiler_params=pltpu.CompilerParams(vmem_limit_bytes=48 * 2**20),
                cost_estimate=pl.CostEstimate(flops=2 * step * n * jd * w3.shape[0] * 256, bytes_accessed=10**6 * step, transcendentals=0),
                name="encode",
            )(cindex.reshape(1).astype(jnp.int32), *pieces, w3, b3, proj_weight, bp, *old)
        return encoded.reshape(frames, 2 * n, w, 2 * block)

    return jax.shard_map(
        local,
        mesh=mesh,
        in_specs=(
            P("frames", AXES, None, None),
            P("frames", None, AXES, None),
            P(), P(), P(), P(), P(), P(), P(), P(),
        ),
        out_specs=P("frames", "rows", "cols", None),
        check_vma=False,
    )
```

```python
import jax
import jax.numpy as jnp
from jax import lax
from jax.experimental import pallas as pl
from jax.experimental.pallas import tpu as pltpu
from jax.sharding import PartitionSpec as P


AXES = ("rows", "cols")
CHUNKS = 2
RUN = 1
HALVES = 2
SIDE = 4
UP, DOWN = 3, 2
BF = jnp.bfloat16


def rounded(n, to):
    return -(-n // to) * to


def limit(mib):
    return pltpu.CompilerParams(vmem_limit_bytes=mib * 2**20)


def whole(a):
    return pl.BlockSpec(a.shape, lambda *_: (0,) * a.ndim)


def weights_kernel(joint, square, w1, w2, *, lidar, camera):
    joined, block = joint.shape[1], square.shape[1]
    ch = lidar + camera
    deep = w1.shape[0] // 3
    for dy in range(3):
        base = dy * deep
        for dx in range(3):
            at = (dy * 3 + dx) * ch
            w1[base + dx * lidar : base + (dx + 1) * lidar, :] = joint[at : at + lidar, :]
            to = base + 3 * lidar + dx * camera
            w1[to : to + camera, :] = joint[at + lidar : at + ch, :]
        w1[base + 3 * ch : base + deep, :] = jnp.zeros((deep - 3 * ch, joined), BF)
    tall = square.shape[0]
    gap = w2.shape[0] - tall
    w2[0:tall, 0:block] = square[...]
    w2[tall:, 0:block] = jnp.zeros((gap, block), BF)
    w2[gap:, block:] = square[...]
    w2[0:gap, block:] = jnp.zeros((gap, block), BF)


def camera_pack_kernel(pos, x, *outs, tr, span):
    frames, sc, ch, rows = x.shape
    groups = len(outs)
    width = frames * span
    place = pos[0]
    row = lax.broadcasted_iota(jnp.int32, (rows, width), 0)
    lane = lax.broadcasted_iota(jnp.int32, (rows, width), 1)
    picks = []
    for f in range(frames):
        parts = []
        for p in range(groups):
            start = lax.rem(place + p, groups) * tr - UP
            parts.append(jnp.where(row + f * span == lane + start, jnp.where(lane // span == f, 1.0, 0.0), 0.0).astype(BF))
        picks.append(jnp.concatenate(parts, axis=1))
    y = None
    for f in range(frames):
        part = jnp.dot(x[f].reshape(sc * ch, rows), picks[f], preferred_element_type=jnp.float32)
        y = part if y is None else y + part
    for p in range(groups):
        outs[p][...] = y[:, p * width : (p + 1) * width].astype(BF).reshape(sc, ch, width)


def camera_unpack_kernel(pos, *refs, groups, sc, cam_ch):
    strips = refs[:groups]
    left, right, out, stage, cells = refs[groups:]
    group = pos[0]
    lanes = left.shape[2]
    pitch = cells.shape[1]
    for p in range(groups):
        q = lax.rem(group - p + groups, groups)
        stage[pl.ds(UP + q * sc, sc)] = strips[p][...]
    stage[0:UP] = left[...]
    n = UP + groups * sc + DOWN
    stage[n - DOWN : n] = right[...]
    lead = SIDE - UP
    cells[:, 0:8, :] = jnp.zeros((lanes, 8, 128), jnp.float32)
    low = (lead + n) // 8 * 8
    cells[:, low:, :] = jnp.zeros((lanes, pitch - low, 128), jnp.float32)
    for c in range(n):
        x = stage[c].astype(jnp.float32)
        x = jnp.concatenate([x, jnp.zeros((128 - cam_ch, lanes), jnp.float32)], axis=0)
        cells[:, lead + c, :] = x.T
    step = 8
    flat = step * pitch
    lane = lax.broadcasted_iota(jnp.int32, (flat, 128), 1)

    def widen(i, _):
        x = cells[pl.ds(i * step, step)].reshape(flat, 128)
        taps = [pltpu.roll(x, 1, 0), x, pltpu.roll(x, flat - 1, 0)]
        for v in range(out.shape[2] // 128):
            y = jnp.zeros((flat, 128), jnp.float32)
            for t in range(3):
                lo, hi = t * cam_ch - v * 128, (t + 1) * cam_ch - v * 128
                if hi > 0 and lo < 128:
                    turned = pltpu.roll(taps[t], lo % 128, 1) if lo % 128 else taps[t]
                    y = jnp.where((lane >= lo) & (lane < hi), turned, y)
            out[pl.ds(i * step, step), :, v * 128 : (v + 1) * 128] = y.astype(BF).reshape(step, pitch, 128)
        return 0

    lax.fori_loop(0, lanes // step, widen, 0)


def pick_kernel(pos, *refs):
    parts = (len(refs) - 2) // 2
    tail, head = refs[-2:]
    for d in range(parts):

        @pl.when(pos[0] == d)
        def _():
            tail[...] = refs[d][...]

        @pl.when(pos[1] == d)
        def _():
            head[...] = refs[parts + d][...]


def pick(arrays, tail_of, head_of, dim):
    size = arrays[0].shape[dim]
    specs, shapes, outs = [], [], []
    for n, at in ((UP, size // UP - 1), (DOWN, 0)):
        shape = arrays[0].shape[:dim] + (n,) + arrays[0].shape[dim + 1 :]
        where = tuple(at if i == dim else 0 for i in range(len(shape)))
        specs += [pl.BlockSpec(shape, lambda i, p, where=where: where)] * len(arrays)
        shapes.append(jax.ShapeDtypeStruct(shape, BF))
        outs.append(pl.BlockSpec(shape, lambda i, p, n=len(shape): (0,) * n))
    return pl.pallas_call(
        pick_kernel,
        grid_spec=pltpu.PrefetchScalarGridSpec(num_scalar_prefetch=1, grid=(1,), in_specs=specs, out_specs=outs),
        out_shape=shapes,
        compiler_params=limit(3),
    )(jnp.stack([tail_of, head_of]).astype(jnp.int32), *arrays, *arrays)


def conv_kernel(pos, *refs, parts, sh, tr, pitch, rows, cols):
    windows = refs[:parts]
    above, below, camera, w1, b1, w2, b2 = refs[parts : parts + 7]
    outs = refs[parts + 7 : parts + 7 + HALVES]
    tile, taps, mid, cells = refs[parts + 7 + HALVES :]
    group, member, half_id = pos[0], pos[1], pos[2]
    wide = windows[0].shape[2]
    lidar = windows[0].shape[3]
    joined = w1.shape[1]
    block = w2.shape[1] // 2

    @pl.when(pl.program_id(0) == 0)
    def _():
        tile[...] = jnp.zeros(tile.shape, BF)

    tile[0:UP, 0:wide, :] = above[0]
    for d in range(parts):
        source = lax.rem(member - d + parts, parts)
        tile[pl.ds(UP + source * sh, sh), 0:wide, :] = windows[d][0]
    tile[UP + tr : UP + tr + DOWN, 0:wide, :] = below[0]

    step = 6
    flat = step * pitch

    def shift(i, _):
        r = i * step
        x = tile[pl.ds(r, step)].reshape(flat, lidar)
        x32 = x.astype(jnp.float32)
        taps[pl.ds(r, step), :, 0:lidar] = pltpu.roll(x32, 1, 0).astype(BF).reshape(step, pitch, lidar)
        taps[pl.ds(r, step), :, lidar : 2 * lidar] = x.reshape(step, pitch, lidar)
        taps[pl.ds(r, step), :, 2 * lidar :] = pltpu.roll(x32, flat - 1, 0).astype(BF).reshape(step, pitch, lidar)
        return 0

    lax.fori_loop(0, (tr + 6) // step, shift, 0)

    n1 = 4
    m1 = n1 * pitch
    col0 = member * (wide - 2 * SIDE) - SIDE

    def first(i, _):
        r = i * n1
        lhs = []
        for dy in range(3):
            lhs.append(taps[pl.ds(r + dy, n1)].reshape(m1, 3 * lidar))
            lhs.append(camera[0, pl.ds(r + dy, n1)].reshape(m1, camera.shape[3]))
        acc = jnp.dot(jnp.concatenate(lhs, axis=1), w1[...], preferred_element_type=jnp.float32)
        v = jnp.maximum(acc + b1[...], 0.0)
        at = lax.broadcasted_iota(jnp.int32, (m1, joined), 0)
        row = group * tr - 2 + r + at // pitch
        col = col0 + at % pitch
        keep = (row >= 0) & (row < rows) & (col >= 0) & (col < cols)
        v = jnp.where(keep, v, 0.0)
        shape = (n1 // 2, 2, pitch, joined)
        p = pl.ds(i * (n1 // 2), n1 // 2)
        mid[p, :, :, 0:joined] = pltpu.roll(v, 1, 0).astype(BF).reshape(shape)
        mid[p, :, :, joined : 2 * joined] = v.astype(BF).reshape(shape)
        mid[p, :, :, 2 * joined :] = pltpu.roll(v, m1 - 1, 0).astype(BF).reshape(shape)
        return 0

    lax.fori_loop(0, (tr + 4) // n1, first, 0)

    n2 = (tr + 2) // 2
    m2 = n2 * pitch
    lhs = [mid[i // 2 : i // 2 + n2, i % 2].reshape(m2, 3 * joined) for i in range(4)]
    acc = jnp.dot(jnp.concatenate(lhs, axis=1), w2[...], preferred_element_type=jnp.float32)
    v = jnp.maximum(acc + b2[...], 0.0)
    at = lax.broadcasted_iota(jnp.int32, (m2, 2 * block), 0)
    half = lax.broadcasted_iota(jnp.int32, (m2, 2 * block), 1) // block
    row = group * tr - 1 + (at // pitch) * 2 + half
    col = col0 + at % pitch
    keep = (row >= 0) & (row < rows) & (col >= 0) & (col < cols)
    v = jnp.where(keep, v, 0.0)
    cells[:, 0] = v[:, :block].reshape(n2, pitch, block)
    cells[:, 1] = v[:, block:].reshape(n2, pitch, block)
    pairs = tr // 2
    w = (wide - 2 * SIDE) // HALVES
    for sub in range(HALVES):
        c = SIDE + sub * w
        even = cells[0:pairs, 1, c : c + w, :].astype(BF)
        odd = cells[1 : pairs + 1, 0, c : c + w, :].astype(BF)
        top = cells[0, 0, c : c + w, :]
        corner = jnp.broadcast_to(cells[pairs, 0, c - 1 : c, :], (w, block))
        edge = jnp.where(half_id == 0, top, corner).astype(BF)
        beside = cells[0:pairs, :, c - 1, :].reshape(tr, block).astype(BF)
        for h in range(HALVES):

            @pl.when(lax.rem(half_id + h, HALVES) == sub)
            def _():
                outs[h][0, 0:pairs, 0] = even
                outs[h][0, 0:pairs, 1] = odd
                outs[h][0, pairs, 0] = edge
                outs[h][0, pairs, 1] = beside


def encode_kernel(pos, *refs, parts, half_rows, w):
    pieces = refs[:parts]
    w3, b3, wp, bp = refs[parts : parts + 4]
    out, grid, grown = refs[-3:]
    me = pos[0]
    block = pieces[0].shape[4]
    for h in range(parts):
        part = lax.rem(me - h + parts, parts)
        base = part * half_rows
        x = pieces[h]
        grid[pl.ds(base, half_rows), 1, 1 : w + 1, :] = x[0, 0:half_rows, 0].astype(jnp.float32)
        grid[pl.ds(base + 1, half_rows), 0, 1 : w + 1, :] = x[0, 0:half_rows, 1].astype(jnp.float32)
        beside = x[0, half_rows, 1].astype(jnp.float32)
        for r in range(2 * half_rows):
            grid[base + r // 2, r % 2, 0:1, :] = beside[r : r + 1]
        edge = x[0, half_rows, 0].astype(jnp.float32)

        @pl.when(part == 0)
        def _():
            grid[0, 0, 1 : w + 1, :] = edge

        @pl.when(part == parts - 1)
        def _():
            grid[parts * half_rows, 0, 0:1, :] = edge[0:1]

    n = parts * half_rows
    jd = rounded(w // 2, 8)
    m = n * jd
    lhs = []
    for a in range(3):
        for b in range(3):
            x = grid[pl.ds(a // 2, n), a % 2, pl.ds(b, jd, stride=2), :]
            lhs.append(x.reshape(m, block).astype(BF))
    deep = jnp.dot(jnp.concatenate(lhs, axis=1), w3[...], preferred_element_type=jnp.float32)
    deep = jnp.maximum(deep + b3[...], 0.0).astype(BF)
    branch = jnp.dot(deep, wp[...], preferred_element_type=jnp.float32)
    branch = jnp.maximum(branch + bp[...], 0.0).astype(BF).astype(jnp.float32).reshape(n, jd, wp.shape[1])
    grown[:, pl.ds(0, jd, stride=2), :] = branch
    grown[:, pl.ds(1, jd, stride=2), :] = branch
    up = grown[:, 0:w, :].astype(BF)
    out[0, :, 0, :, 0:block] = grid[0:n, 1, 1 : w + 1, :].astype(BF)
    out[0, :, 1, :, 0:block] = grid[1 : n + 1, 0, 1 : w + 1, :].astype(BF)
    out[0, :, 0, :, block:] = up
    out[0, :, 1, :, block:] = up


def solution(mesh):
    n_rows, n_cols = mesh.shape["rows"], mesh.shape["cols"]
    members = n_cols // HALVES
    groups = n_rows * HALVES
    total = n_rows * n_cols

    def local(lidar, camera, joined_weight, joined_bias, block_weight, block_bias, down_weight, down_bias, proj_weight, proj_bias):
        frames, sh, cols, lidar_ch = lidar.shape
        rows, sc, cam_ch = camera.shape[1:]
        tr = sh * members
        tw = cols // members
        wide = tw + 2 * SIDE
        pitch = rounded(wide, 16)
        w = cols // n_cols
        joined = joined_weight.shape[3]
        block = block_weight.shape[3]
        place = lax.axis_index(AXES)
        group = place // members
        member = place % members
        cindex = lax.axis_index("cols")
        kgroup = cindex // members

        def send(x, pairs):
            return lax.ppermute(x, AXES, pairs)

        def across(x, by_group, by_member):
            pairs = []
            for g in range(groups):
                for j in range(members):
                    if 0 <= g + by_group < groups and 0 <= j + by_member < members:
                        pairs.append((g * members + j, (g + by_group) * members + j + by_member))
            return send(x, pairs)

        joint = joined_weight.reshape(-1, joined)
        square = block_weight.reshape(-1, block)
        deep1 = 3 * (3 * lidar_ch + rounded(3 * cam_ch, 256))
        w1, w2 = pl.pallas_call(
            lambda *refs: weights_kernel(*refs, lidar=lidar_ch, camera=cam_ch),
            out_shape=[
                jax.ShapeDtypeStruct((deep1, joined), BF),
                jax.ShapeDtypeStruct((4 * 3 * joined, 2 * block), BF),
            ],
            compiler_params=limit(14),
            name="weights",
        )(joint, square)
        w3 = down_weight.reshape(-1, down_weight.shape[3])
        b1 = joined_bias.reshape(1, -1)
        b2 = jnp.concatenate([block_bias, block_bias]).reshape(1, -1)
        b3 = down_bias.reshape(1, -1)
        bp = proj_bias.reshape(1, -1)

        span = rounded(tr + UP + DOWN, 8)
        lanes = frames * span
        turned = jnp.transpose(camera, (0, 2, 3, 1))
        strip = jax.ShapeDtypeStruct((sc, cam_ch, lanes), BF)
        packed = pl.pallas_call(
            lambda *refs: camera_pack_kernel(*refs, tr=tr, span=span),
            grid_spec=pltpu.PrefetchScalarGridSpec(
                num_scalar_prefetch=1,
                grid=(1,),
                in_specs=[whole(turned)],
                out_specs=[whole(strip)] * groups,
            ),
            out_shape=[strip] * groups,
            compiler_params=limit(14),
            name="camera_pack",
        )(place.reshape(1).astype(jnp.int32), turned)
        lidar, packed = lax.optimization_barrier((lidar, packed))
        arrived = [
            send(packed[p], [(s, ((s + p) % groups) * members + s // groups) for s in range(total)])
            for p in range(groups)
        ]
        tail, head = pick(arrived, (group + 1) % groups, group, 0)
        left = across(tail, 0, 1)
        right = across(head, 0, -1)
        cam = pl.pallas_call(
            lambda *refs: camera_unpack_kernel(*refs, groups=groups, sc=sc, cam_ch=cam_ch),
            grid_spec=pltpu.PrefetchScalarGridSpec(
                num_scalar_prefetch=1,
                grid=(1,),
                in_specs=[whole(x) for x in arrived] + [whole(left), whole(right)],
                out_specs=pl.BlockSpec((lanes, pitch, rounded(3 * cam_ch, 256)), lambda i, p: (0, 0, 0)),
                scratch_shapes=[
                    pltpu.VMEM((tw + UP + DOWN, cam_ch, lanes), BF),
                    pltpu.VMEM((lanes, pitch, 128), jnp.float32),
                ],
            ),
            out_shape=jax.ShapeDtypeStruct((lanes, pitch, rounded(3 * cam_ch, 256)), BF),
            compiler_params=limit(16),
            name="camera_unpack",
        )(group.reshape(1).astype(jnp.int32), *arrived, left, right)
        cam = cam.reshape(frames, span, pitch, -1)

        padded = jnp.pad(lidar, ((0, 0), (0, 0), (SIDE, SIDE), (0, 0)))
        pos = jnp.stack([group, member, kgroup]).astype(jnp.int32)
        pairs2 = (tr + 2) // 2
        half_rows = tr // 2
        n = HALVES * half_rows
        jd = rounded(w // 2, 8)
        blocks = jax.ShapeDtypeStruct((RUN, pairs2, 2, w, block), BF)
        flops = 2 * RUN * pitch * ((tr + 4) * w1.shape[0] * joined + pairs2 * w2.shape[0] * 2 * block)
        encoded = None
        step = frames // CHUNKS
        for f0 in range(0, frames, step):
            windows = []
            for d in range(members):
                x = lax.dynamic_slice(padded, (f0, 0, ((member + d) % members) * tw, 0), (step, sh, wide, lidar_ch))
                if d:
                    x = send(x, [(g * members + j, g * members + (j + d) % members) for g in range(groups) for j in range(members)])
                windows.append(x)
            last, head = pick(windows, (member + 1) % members, member, 1)
            above = across(last, 1, 0)
            below = across(head, -1, 0)
            for f1 in range(f0, f0 + step, RUN):
                framed = lambda a, lo: pl.BlockSpec((1,) + a.shape[1:], lambda f, p: (f + lo,) + (0,) * (a.ndim - 1))
                lo = f1 - f0
                tiles = pl.pallas_call(
                    lambda *refs: conv_kernel(*refs, parts=members, sh=sh, tr=tr, pitch=pitch, rows=rows, cols=cols),
                    grid_spec=pltpu.PrefetchScalarGridSpec(
                        num_scalar_prefetch=1,
                        grid=(RUN,),
                        in_specs=[framed(x, lo) for x in [*windows, above, below]] + [framed(cam, f1), whole(w1), whole(b1), whole(w2), whole(b2)],
                        out_specs=[framed(blocks, 0)] * HALVES,
                        scratch_shapes=[
                            pltpu.VMEM((tr + 6, pitch, lidar_ch), BF),
                            pltpu.VMEM((tr + 6, pitch, 3 * lidar_ch), BF),
                            pltpu.VMEM(((tr + 4) // 2, 2, pitch, 3 * joined), BF),
                            pltpu.VMEM((pairs2, 2, pitch, block), jnp.float32),
                        ],
                    ),
                    out_shape=[blocks] * HALVES,
                    compiler_params=limit(28),
                    cost_estimate=pl.CostEstimate(flops=flops, bytes_accessed=2 * 10**6 * RUN, transcendentals=0),
                    name="convs",
                )(pos, *windows, above, below, cam, w1, b1, w2, b2)
                pieces = []
                for h in range(HALVES):
                    pairs = []
                    for s in range(total):
                        r, c = divmod(s, n_cols)
                        k, j = divmod(c, members)
                        pairs.append((s, r * n_cols + HALVES * j + (k + h) % HALVES))
                    pieces.append(send(tiles[h], pairs))
                old = [] if encoded is None else [encoded]
                encoded = pl.pallas_call(
                    lambda *refs: encode_kernel(*refs, parts=HALVES, half_rows=half_rows, w=w),
                    grid_spec=pltpu.PrefetchScalarGridSpec(
                        num_scalar_prefetch=1,
                        grid=(RUN,),
                        in_specs=[framed(x, 0) for x in pieces] + [whole(x) for x in (w3, b3, proj_weight, bp)] + [pl.BlockSpec(memory_space=pl.ANY)] * len(old),
                        out_specs=pl.BlockSpec((1, n, 2, w, 2 * block), lambda f, p, f1=f1: (f + f1, 0, 0, 0, 0)),
                        scratch_shapes=[
                            pltpu.VMEM((n + 1, 2, rounded(w + 1, 8) + 16, block), jnp.float32),
                            pltpu.VMEM((n, 2 * jd, block), jnp.float32),
                        ],
                    ),
                    out_shape=jax.ShapeDtypeStruct((frames, n, 2, w, 2 * block), BF),
                    input_output_aliases={5 + HALVES: 0} if old else {},
                    compiler_params=limit(12),
                    cost_estimate=pl.CostEstimate(flops=2 * RUN * n * jd * w3.shape[0] * 256, bytes_accessed=10**6 * RUN, transcendentals=0),
                    name="encode",
                )(cindex.reshape(1).astype(jnp.int32), *pieces, w3, b3, proj_weight, bp, *old)
        return encoded.reshape(frames, 2 * n, w, 2 * block)

    return jax.shard_map(
        local,
        mesh=mesh,
        in_specs=(
            P("frames", AXES, None, None),
            P("frames", None, AXES, None),
            P(), P(), P(), P(), P(), P(), P(), P(),
        ),
        out_specs=P("frames", "rows", "cols", None),
        check_vma=False,
    )
```

```python
import jax
import jax.numpy as jnp
from jax import lax
from jax.experimental import pallas as pl
from jax.experimental.pallas import tpu as pltpu
from jax.sharding import PartitionSpec as P


AXES = ("rows", "cols")
CHUNKS = 2
RUN = 1
HALVES = 2
SIDE = 4
UP, DOWN = 3, 2
BF = jnp.bfloat16


def rounded(n, to):
    return -(-n // to) * to


def limit(mib):
    return pltpu.CompilerParams(vmem_limit_bytes=mib * 2**20)


def whole(a):
    return pl.BlockSpec(a.shape, lambda *_: (0,) * a.ndim)


def weights_kernel(joint, square, w1, w2, *, lidar, camera):
    joined, block = joint.shape[1], square.shape[1]
    ch = lidar + camera
    deep = w1.shape[0] // 3
    for dy in range(3):
        base = dy * deep
        for dx in range(3):
            at = (dy * 3 + dx) * ch
            w1[base + dx * lidar : base + (dx + 1) * lidar, :] = joint[at : at + lidar, :]
            to = base + 3 * lidar + dx * camera
            w1[to : to + camera, :] = joint[at + lidar : at + ch, :]
        w1[base + 3 * ch : base + deep, :] = jnp.zeros((deep - 3 * ch, joined), BF)
    tall = square.shape[0]
    gap = w2.shape[0] - tall
    w2[0:tall, 0:block] = square[...]
    w2[tall:, 0:block] = jnp.zeros((gap, block), BF)
    w2[gap:, block:] = square[...]
    w2[0:gap, block:] = jnp.zeros((gap, block), BF)


def camera_pack_kernel(pos, x, *outs, tr, span):
    frames, sc, ch, rows = x.shape
    groups = len(outs)
    width = frames * span
    place = pos[0]
    row = lax.broadcasted_iota(jnp.int32, (rows, width), 0)
    lane = lax.broadcasted_iota(jnp.int32, (rows, width), 1)
    picks = []
    for f in range(frames):
        parts = []
        for p in range(groups):
            start = lax.rem(place + p, groups) * tr - UP
            parts.append(jnp.where(row + f * span == lane + start, jnp.where(lane // span == f, 1.0, 0.0), 0.0).astype(BF))
        picks.append(jnp.concatenate(parts, axis=1))
    y = None
    for f in range(frames):
        part = jnp.dot(x[f].reshape(sc * ch, rows), picks[f], preferred_element_type=jnp.float32)
        y = part if y is None else y + part
    for p in range(groups):
        outs[p][...] = y[:, p * width : (p + 1) * width].astype(BF).reshape(sc, ch, width)


def camera_unpack_kernel(pos, *refs, groups, sc, cam_ch):
    strips = refs[:groups]
    left, right, out, stage, cells = refs[groups:]
    group = pos[0]
    lanes = left.shape[2]
    pitch = cells.shape[1]
    for p in range(groups):
        q = lax.rem(group - p + groups, groups)
        stage[pl.ds(UP + q * sc, sc)] = strips[p][...]
    stage[0:UP] = left[...]
    n = UP + groups * sc + DOWN
    stage[n - DOWN : n] = right[...]
    lead = SIDE - UP
    cells[:, 0:8, :] = jnp.zeros((lanes, 8, 128), jnp.float32)
    low = (lead + n) // 8 * 8
    cells[:, low:, :] = jnp.zeros((lanes, pitch - low, 128), jnp.float32)
    for c in range(n):
        x = stage[c].astype(jnp.float32)
        x = jnp.concatenate([x, jnp.zeros((128 - cam_ch, lanes), jnp.float32)], axis=0)
        cells[:, lead + c, :] = x.T
    step = 8
    flat = step * pitch
    lane = lax.broadcasted_iota(jnp.int32, (flat, 128), 1)

    def widen(i, _):
        x = cells[pl.ds(i * step, step)].reshape(flat, 128)
        taps = [pltpu.roll(x, 1, 0), x, pltpu.roll(x, flat - 1, 0)]
        for v in range(out.shape[2] // 128):
            y = jnp.zeros((flat, 128), jnp.float32)
            for t in range(3):
                lo, hi = t * cam_ch - v * 128, (t + 1) * cam_ch - v * 128
                if hi > 0 and lo < 128:
                    turned = pltpu.roll(taps[t], lo % 128, 1) if lo % 128 else taps[t]
                    y = jnp.where((lane >= lo) & (lane < hi), turned, y)
            out[pl.ds(i * step, step), :, v * 128 : (v + 1) * 128] = y.astype(BF).reshape(step, pitch, 128)
        return 0

    lax.fori_loop(0, lanes // step, widen, 0)


def pick_kernel(pos, *refs):
    parts = (len(refs) - 2) // 2
    tail, head = refs[-2:]
    for d in range(parts):

        @pl.when(pos[0] == d)
        def _():
            tail[...] = refs[d][...]

        @pl.when(pos[1] == d)
        def _():
            head[...] = refs[parts + d][...]


def pick(arrays, tail_of, head_of, dim):
    size = arrays[0].shape[dim]
    specs, shapes, outs = [], [], []
    for n, at in ((UP, size // UP - 1), (DOWN, 0)):
        shape = arrays[0].shape[:dim] + (n,) + arrays[0].shape[dim + 1 :]
        where = tuple(at if i == dim else 0 for i in range(len(shape)))
        specs += [pl.BlockSpec(shape, lambda i, p, where=where: where)] * len(arrays)
        shapes.append(jax.ShapeDtypeStruct(shape, BF))
        outs.append(pl.BlockSpec(shape, lambda i, p, n=len(shape): (0,) * n))
    return pl.pallas_call(
        pick_kernel,
        grid_spec=pltpu.PrefetchScalarGridSpec(num_scalar_prefetch=1, grid=(1,), in_specs=specs, out_specs=outs),
        out_shape=shapes,
        compiler_params=limit(3),
    )(jnp.stack([tail_of, head_of]).astype(jnp.int32), *arrays, *arrays)


def conv_kernel(pos, *refs, parts, sh, tr, pitch, rows, cols):
    windows = refs[:parts]
    above, below, camera, w1, b1, w2, b2 = refs[parts : parts + 7]
    outs = refs[parts + 7 : parts + 7 + HALVES]
    tile, taps, mid, cells = refs[parts + 7 + HALVES :]
    group, member, half_id, column = pos[0], pos[1], pos[2], pos[3]
    wide = windows[0].shape[2]
    lidar = windows[0].shape[3]
    joined = w1.shape[1]
    block = w2.shape[1] // 2

    @pl.when(pl.program_id(0) == 0)
    def _():
        tile[...] = jnp.zeros(tile.shape, BF)

    tile[0:UP, 0:wide, :] = above[0]
    for d in range(parts):
        source = lax.rem(member - d + parts, parts)
        tile[pl.ds(UP + source * sh, sh), 0:wide, :] = windows[d][0]
    tile[UP + tr : UP + tr + DOWN, 0:wide, :] = below[0]

    step = 6
    flat = step * pitch

    def shift(i, _):
        r = i * step
        x = tile[pl.ds(r, step)].reshape(flat, lidar)
        x32 = x.astype(jnp.float32)
        taps[pl.ds(r, step), :, 0:lidar] = pltpu.roll(x32, 1, 0).astype(BF).reshape(step, pitch, lidar)
        taps[pl.ds(r, step), :, lidar : 2 * lidar] = x.reshape(step, pitch, lidar)
        taps[pl.ds(r, step), :, 2 * lidar :] = pltpu.roll(x32, flat - 1, 0).astype(BF).reshape(step, pitch, lidar)
        return 0

    lax.fori_loop(0, (tr + 6) // step, shift, 0)

    n1 = 4
    m1 = n1 * pitch
    col0 = column * (wide - 2 * SIDE) - SIDE

    def first(i, _):
        r = i * n1
        lhs = []
        for dy in range(3):
            lhs.append(taps[pl.ds(r + dy, n1)].reshape(m1, 3 * lidar))
            lhs.append(camera[0, pl.ds(r + dy, n1)].reshape(m1, camera.shape[3]))
        acc = jnp.dot(jnp.concatenate(lhs, axis=1), w1[...], preferred_element_type=jnp.float32)
        v = jnp.maximum(acc + b1[...], 0.0)
        at = lax.broadcasted_iota(jnp.int32, (m1, joined), 0)
        row = group * tr - 2 + r + at // pitch
        col = col0 + at % pitch
        keep = (row >= 0) & (row < rows) & (col >= 0) & (col < cols)
        v = jnp.where(keep, v, 0.0)
        shape = (n1 // 2, 2, pitch, joined)
        p = pl.ds(i * (n1 // 2), n1 // 2)
        mid[p, :, :, 0:joined] = pltpu.roll(v, 1, 0).astype(BF).reshape(shape)
        mid[p, :, :, joined : 2 * joined] = v.astype(BF).reshape(shape)
        mid[p, :, :, 2 * joined :] = pltpu.roll(v, m1 - 1, 0).astype(BF).reshape(shape)
        return 0

    lax.fori_loop(0, (tr + 4) // n1, first, 0)

    n2 = (tr + 2) // 2
    m2 = n2 * pitch
    lhs = [mid[i // 2 : i // 2 + n2, i % 2].reshape(m2, 3 * joined) for i in range(4)]
    acc = jnp.dot(jnp.concatenate(lhs, axis=1), w2[...], preferred_element_type=jnp.float32)
    v = jnp.maximum(acc + b2[...], 0.0)
    at = lax.broadcasted_iota(jnp.int32, (m2, 2 * block), 0)
    half = lax.broadcasted_iota(jnp.int32, (m2, 2 * block), 1) // block
    row = group * tr - 1 + (at // pitch) * 2 + half
    col = col0 + at % pitch
    keep = (row >= 0) & (row < rows) & (col >= 0) & (col < cols)
    v = jnp.where(keep, v, 0.0)
    cells[:, 0] = v[:, :block].reshape(n2, pitch, block)
    cells[:, 1] = v[:, block:].reshape(n2, pitch, block)
    pairs = tr // 2
    w = (wide - 2 * SIDE) // HALVES
    for sub in range(HALVES):
        c = SIDE + sub * w
        even = cells[0:pairs, 1, c : c + w, :].astype(BF)
        odd = cells[1 : pairs + 1, 0, c : c + w, :].astype(BF)
        top = cells[0, 0, c : c + w, :]
        corner = jnp.broadcast_to(cells[pairs, 0, c - 1 : c, :], (w, block))
        edge = jnp.where(half_id == 0, top, corner).astype(BF)
        beside = cells[0:pairs, :, c - 1, :].reshape(tr, block).astype(BF)
        for h in range(HALVES):

            @pl.when(lax.rem(half_id + h, HALVES) == sub)
            def _():
                outs[h][0, 0:pairs, 0] = even
                outs[h][0, 0:pairs, 1] = odd
                outs[h][0, pairs, 0] = edge
                outs[h][0, pairs, 1] = beside


def encode_kernel(pos, *refs, parts, half_rows, w):
    pieces = refs[:parts]
    w3, b3, wp, bp = refs[parts : parts + 4]
    out, grid, grown = refs[-3:]
    me = pos[0]
    block = pieces[0].shape[4]
    for h in range(parts):
        part = lax.rem(me - h + parts, parts)
        base = part * half_rows
        x = pieces[h]
        grid[pl.ds(base, half_rows), 1, 1 : w + 1, :] = x[0, 0:half_rows, 0].astype(jnp.float32)
        grid[pl.ds(base + 1, half_rows), 0, 1 : w + 1, :] = x[0, 0:half_rows, 1].astype(jnp.float32)
        beside = x[0, half_rows, 1].astype(jnp.float32)
        for r in range(2 * half_rows):
            grid[base + r // 2, r % 2, 0:1, :] = beside[r : r + 1]
        edge = x[0, half_rows, 0].astype(jnp.float32)

        @pl.when(part == 0)
        def _():
            grid[0, 0, 1 : w + 1, :] = edge

        @pl.when(part == parts - 1)
        def _():
            grid[parts * half_rows, 0, 0:1, :] = edge[0:1]

    n = parts * half_rows
    jd = rounded(w // 2, 8)
    m = n * jd
    lhs = []
    for a in range(3):
        for b in range(3):
            x = grid[pl.ds(a // 2, n), a % 2, pl.ds(b, jd, stride=2), :]
            lhs.append(x.reshape(m, block).astype(BF))
    deep = jnp.dot(jnp.concatenate(lhs, axis=1), w3[...], preferred_element_type=jnp.float32)
    deep = jnp.maximum(deep + b3[...], 0.0).astype(BF)
    branch = jnp.dot(deep, wp[...], preferred_element_type=jnp.float32)
    branch = jnp.maximum(branch + bp[...], 0.0).astype(BF).astype(jnp.float32).reshape(n, jd, wp.shape[1])
    grown[:, pl.ds(0, jd, stride=2), :] = branch
    grown[:, pl.ds(1, jd, stride=2), :] = branch
    up = grown[:, 0:w, :].astype(BF)
    out[0, :, 0, :, 0:block] = grid[0:n, 1, 1 : w + 1, :].astype(BF)
    out[0, :, 1, :, 0:block] = grid[1 : n + 1, 0, 1 : w + 1, :].astype(BF)
    out[0, :, 0, :, block:] = up
    out[0, :, 1, :, block:] = up


def solution(mesh):
    n_rows, n_cols = mesh.shape["rows"], mesh.shape["cols"]
    members = n_cols // HALVES
    groups = n_rows * HALVES
    total = n_rows * n_cols
    half = members // 2
    tile_of = [2 * m if m < half else 2 * (members - 1 - m) + 1 for m in range(members)]
    holder = [tile_of.index(j) for j in range(members)]

    def local(lidar, camera, joined_weight, joined_bias, block_weight, block_bias, down_weight, down_bias, proj_weight, proj_bias):
        frames, sh, cols, lidar_ch = lidar.shape
        rows, sc, cam_ch = camera.shape[1:]
        tr = sh * members
        tw = cols // members
        wide = tw + 2 * SIDE
        pitch = rounded(wide, 16)
        w = cols // n_cols
        joined = joined_weight.shape[3]
        block = block_weight.shape[3]
        place = lax.axis_index(AXES)
        group = place // members
        member = place % members
        cindex = lax.axis_index("cols")
        kgroup = cindex // members

        def send(x, pairs):
            return lax.ppermute(x, AXES, pairs)

        def across(x, by_group, by_column):
            pairs = []
            for g in range(groups):
                for j in range(members):
                    if 0 <= g + by_group < groups and 0 <= j + by_column < members:
                        pairs.append((g * members + holder[j], (g + by_group) * members + holder[j + by_column]))
            return send(x, pairs)

        def column_of(m):
            return jnp.where(m < half, 2 * m, 2 * (members - 1 - m) + 1)

        joint = joined_weight.reshape(-1, joined)
        square = block_weight.reshape(-1, block)
        deep1 = 3 * (3 * lidar_ch + rounded(3 * cam_ch, 256))
        w1, w2 = pl.pallas_call(
            lambda *refs: weights_kernel(*refs, lidar=lidar_ch, camera=cam_ch),
            out_shape=[
                jax.ShapeDtypeStruct((deep1, joined), BF),
                jax.ShapeDtypeStruct((4 * 3 * joined, 2 * block), BF),
            ],
            compiler_params=limit(14),
            name="weights",
        )(joint, square)
        w3 = down_weight.reshape(-1, down_weight.shape[3])
        b1 = joined_bias.reshape(1, -1)
        b2 = jnp.concatenate([block_bias, block_bias]).reshape(1, -1)
        b3 = down_bias.reshape(1, -1)
        bp = proj_bias.reshape(1, -1)

        span = rounded(tr + UP + DOWN, 8)
        lanes = frames * span
        turned = jnp.transpose(camera, (0, 2, 3, 1))
        strip = jax.ShapeDtypeStruct((sc, cam_ch, lanes), BF)
        packed = pl.pallas_call(
            lambda *refs: camera_pack_kernel(*refs, tr=tr, span=span),
            grid_spec=pltpu.PrefetchScalarGridSpec(
                num_scalar_prefetch=1,
                grid=(1,),
                in_specs=[whole(turned)],
                out_specs=[whole(strip)] * groups,
            ),
            out_shape=[strip] * groups,
            compiler_params=limit(14),
            name="camera_pack",
        )(place.reshape(1).astype(jnp.int32), turned)
        lidar, packed = lax.optimization_barrier((lidar, packed))
        arrived = [
            send(packed[p], [(s, ((s + p) % groups) * members + holder[s // groups]) for s in range(total)])
            for p in range(groups)
        ]
        tail, head = pick(arrived, (group + 1) % groups, group, 0)
        left = across(tail, 0, 1)
        right = across(head, 0, -1)
        cam = pl.pallas_call(
            lambda *refs: camera_unpack_kernel(*refs, groups=groups, sc=sc, cam_ch=cam_ch),
            grid_spec=pltpu.PrefetchScalarGridSpec(
                num_scalar_prefetch=1,
                grid=(1,),
                in_specs=[whole(x) for x in arrived] + [whole(left), whole(right)],
                out_specs=pl.BlockSpec((lanes, pitch, rounded(3 * cam_ch, 256)), lambda i, p: (0, 0, 0)),
                scratch_shapes=[
                    pltpu.VMEM((tw + UP + DOWN, cam_ch, lanes), BF),
                    pltpu.VMEM((lanes, pitch, 128), jnp.float32),
                ],
            ),
            out_shape=jax.ShapeDtypeStruct((lanes, pitch, rounded(3 * cam_ch, 256)), BF),
            compiler_params=limit(16),
            name="camera_unpack",
        )(group.reshape(1).astype(jnp.int32), *arrived, left, right)
        cam = cam.reshape(frames, span, pitch, -1)

        padded = jnp.pad(lidar, ((0, 0), (0, 0), (SIDE, SIDE), (0, 0)))
        pos = jnp.stack([group, member, kgroup, column_of(member)]).astype(jnp.int32)
        pairs2 = (tr + 2) // 2
        half_rows = tr // 2
        n = HALVES * half_rows
        jd = rounded(w // 2, 8)
        blocks = jax.ShapeDtypeStruct((RUN, pairs2, 2, w, block), BF)
        flops = 2 * RUN * pitch * ((tr + 4) * w1.shape[0] * joined + pairs2 * w2.shape[0] * 2 * block)
        encoded = None
        step = frames // CHUNKS
        for f0 in range(0, frames, step):
            windows = []
            for d in range(members):
                x = lax.dynamic_slice(padded, (f0, 0, column_of((member + d) % members) * tw, 0), (step, sh, wide, lidar_ch))
                if d:
                    x = send(x, [(g * members + j, g * members + (j + d) % members) for g in range(groups) for j in range(members)])
                windows.append(x)
            last, head = pick(windows, (member + 1) % members, member, 1)
            above = across(last, 1, 0)
            below = across(head, -1, 0)
            for f1 in range(f0, f0 + step, RUN):
                framed = lambda a, lo: pl.BlockSpec((1,) + a.shape[1:], lambda f, p: (f + lo,) + (0,) * (a.ndim - 1))
                lo = f1 - f0
                tiles = pl.pallas_call(
                    lambda *refs: conv_kernel(*refs, parts=members, sh=sh, tr=tr, pitch=pitch, rows=rows, cols=cols),
                    grid_spec=pltpu.PrefetchScalarGridSpec(
                        num_scalar_prefetch=1,
                        grid=(RUN,),
                        in_specs=[framed(x, lo) for x in [*windows, above, below]] + [framed(cam, f1), whole(w1), whole(b1), whole(w2), whole(b2)],
                        out_specs=[framed(blocks, 0)] * HALVES,
                        scratch_shapes=[
                            pltpu.VMEM((tr + 6, pitch, lidar_ch), BF),
                            pltpu.VMEM((tr + 6, pitch, 3 * lidar_ch), BF),
                            pltpu.VMEM(((tr + 4) // 2, 2, pitch, 3 * joined), BF),
                            pltpu.VMEM((pairs2, 2, pitch, block), jnp.float32),
                        ],
                    ),
                    out_shape=[blocks] * HALVES,
                    compiler_params=limit(28),
                    cost_estimate=pl.CostEstimate(flops=flops, bytes_accessed=2 * 10**6 * RUN, transcendentals=0),
                )(pos, *windows, above, below, cam, w1, b1, w2, b2)
                pieces = []
                for h in range(HALVES):
                    pairs = []
                    for s in range(total):
                        r, c = divmod(s, n_cols)
                        k, m = divmod(c, members)
                        pairs.append((s, r * n_cols + HALVES * tile_of[m] + (k + h) % HALVES))
                    pieces.append(send(tiles[h], pairs))
                old = [] if encoded is None else [encoded]
                encoded = pl.pallas_call(
                    lambda *refs: encode_kernel(*refs, parts=HALVES, half_rows=half_rows, w=w),
                    grid_spec=pltpu.PrefetchScalarGridSpec(
                        num_scalar_prefetch=1,
                        grid=(RUN,),
                        in_specs=[framed(x, 0) for x in pieces] + [whole(x) for x in (w3, b3, proj_weight, bp)] + [pl.BlockSpec(memory_space=pl.ANY)] * len(old),
                        out_specs=pl.BlockSpec((1, n, 2, w, 2 * block), lambda f, p, f1=f1: (f + f1, 0, 0, 0, 0)),
                        scratch_shapes=[
                            pltpu.VMEM((n + 1, 2, rounded(w + 1, 8) + 16, block), jnp.float32),
                            pltpu.VMEM((n, 2 * jd, block), jnp.float32),
                        ],
                    ),
                    out_shape=jax.ShapeDtypeStruct((frames, n, 2, w, 2 * block), BF),
                    input_output_aliases={5 + HALVES: 0} if old else {},
                    compiler_params=limit(12),
                    cost_estimate=pl.CostEstimate(flops=2 * RUN * n * jd * w3.shape[0] * 256, bytes_accessed=10**6 * RUN, transcendentals=0),
                )(cindex.reshape(1).astype(jnp.int32), *pieces, w3, b3, proj_weight, bp, *old)
        return encoded.reshape(frames, 2 * n, w, 2 * block)

    return jax.shard_map(
        local,
        mesh=mesh,
        in_specs=(
            P("frames", AXES, None, None),
            P("frames", None, AXES, None),
            P(), P(), P(), P(), P(), P(), P(), P(),
        ),
        out_specs=P("frames", "rows", "cols", None),
        check_vma=False,
    )
```

```python
import functools

import jax
import jax.numpy as jnp
from jax import lax
from jax.experimental import pallas as pl
from jax.experimental.pallas import tpu as pltpu
from jax.sharding import PartitionSpec as P


AXES = ("rows", "cols")
CHUNKS = 2
HALVES = 2
SIDE = 4
UP, DOWN = 3, 2
BF = jnp.bfloat16


def rounded(n, to):
    return -(-n // to) * to


def limit(mib):
    return pltpu.CompilerParams(vmem_limit_bytes=mib * 2**20)


def whole(a):
    return pl.BlockSpec(a.shape, lambda *_: (0,) * a.ndim)


def weights_kernel(joint, square, w1, w2, *, lidar, camera):
    joined, block = joint.shape[1], square.shape[1]
    ch = lidar + camera
    deep = w1.shape[0] // 3
    for dy in range(3):
        base = dy * deep
        for dx in range(3):
            at = (dy * 3 + dx) * ch
            to = base + (1, 0, 2)[dx] * lidar
            w1[to : to + lidar, :] = joint[at : at + lidar, :]
            to = base + 3 * lidar + dx * camera
            w1[to : to + camera, :] = joint[at + lidar : at + ch, :]
        w1[base + 3 * ch : base + deep, :] = jnp.zeros((deep - 3 * ch, joined), BF)
    tall = square.shape[0]
    gap = w2.shape[0] - tall
    w2[0:tall, 0:block] = square[...]
    w2[tall:, 0:block] = jnp.zeros((gap, block), BF)
    w2[gap:, block:] = square[...]
    w2[0:gap, block:] = jnp.zeros((gap, block), BF)


def camera_pack_kernel(pos, x, *outs, tr, span):
    frames, sc, ch, rows = x.shape
    groups = len(outs)
    width = frames * span
    place = pos[0]
    row = lax.broadcasted_iota(jnp.int32, (rows, width), 0)
    lane = lax.broadcasted_iota(jnp.int32, (rows, width), 1)
    picks = []
    for f in range(frames):
        parts = []
        for p in range(groups):
            start = lax.rem(place + p, groups) * tr - UP
            parts.append(jnp.where(row + f * span == lane + start, jnp.where(lane // span == f, 1.0, 0.0), 0.0).astype(BF))
        picks.append(jnp.concatenate(parts, axis=1))
    y = None
    for f in range(frames):
        part = jnp.dot(x[f].reshape(sc * ch, rows), picks[f], preferred_element_type=jnp.float32)
        y = part if y is None else y + part
    for p in range(groups):
        outs[p][...] = y[:, p * width : (p + 1) * width].astype(BF).reshape(sc, ch, width)


def camera_unpack_kernel(pos, *refs, groups, sc, cam_ch):
    strips = refs[:groups]
    left, right, out, stage, cells = refs[groups:]
    group = pos[0]
    lanes = left.shape[2]
    pitch = cells.shape[1]
    for p in range(groups):
        q = lax.rem(group - p + groups, groups)
        stage[pl.ds(UP + q * sc, sc)] = strips[p][...]
    stage[0:UP] = left[...]
    n = UP + groups * sc + DOWN
    stage[n - DOWN : n] = right[...]
    lead = SIDE - UP
    cells[:, 0:8, :] = jnp.zeros((lanes, 8, 128), jnp.float32)
    low = (lead + n) // 8 * 8
    cells[:, low:, :] = jnp.zeros((lanes, pitch - low, 128), jnp.float32)
    for c in range(n):
        x = stage[c].astype(jnp.float32)
        x = jnp.concatenate([x, jnp.zeros((128 - cam_ch, lanes), jnp.float32)], axis=0)
        cells[:, lead + c, :] = x.T
    step = 8
    flat = step * pitch
    lane = lax.broadcasted_iota(jnp.int32, (flat, 128), 1)

    def widen(i, _):
        x = cells[pl.ds(i * step, step)].reshape(flat, 128)
        taps = [pltpu.roll(x, 1, 0), x, pltpu.roll(x, flat - 1, 0)]
        for v in range(out.shape[2] // 128):
            y = jnp.zeros((flat, 128), jnp.float32)
            for t in range(3):
                lo, hi = t * cam_ch - v * 128, (t + 1) * cam_ch - v * 128
                if hi > 0 and lo < 128:
                    turned = pltpu.roll(taps[t], lo % 128, 1) if lo % 128 else taps[t]
                    y = jnp.where((lane >= lo) & (lane < hi), turned, y)
            out[pl.ds(i * step, step), :, v * 128 : (v + 1) * 128] = y.astype(BF).reshape(step, pitch, 128)
        return 0

    lax.fori_loop(0, lanes // step, widen, 0)


def pick_kernel(pos, *refs):
    parts = (len(refs) - 2) // 2
    tail, head = refs[-2:]
    for d in range(parts):

        @pl.when(pos[0] == d)
        def _():
            tail[...] = refs[d][...]

        @pl.when(pos[1] == d)
        def _():
            head[...] = refs[parts + d][...]


def pick(arrays, tail_of, head_of, dim):
    size = arrays[0].shape[dim]
    specs, shapes, outs = [], [], []
    for n, at in ((UP, size // UP - 1), (DOWN, 0)):
        shape = arrays[0].shape[:dim] + (n,) + arrays[0].shape[dim + 1 :]
        where = tuple(at if i == dim else 0 for i in range(len(shape)))
        specs += [pl.BlockSpec(shape, lambda i, p, where=where: where)] * len(arrays)
        shapes.append(jax.ShapeDtypeStruct(shape, BF))
        outs.append(pl.BlockSpec(shape, lambda i, p, n=len(shape): (0,) * n))
    return pl.pallas_call(
        pick_kernel,
        grid_spec=pltpu.PrefetchScalarGridSpec(num_scalar_prefetch=1, grid=(1,), in_specs=specs, out_specs=outs),
        out_shape=shapes,
        compiler_params=limit(3),
    )(jnp.stack([tail_of, head_of]).astype(jnp.int32), *arrays, *arrays)


def conv_scratch(tr, pitch, lidar, joined, block, pairs):
    return [
        pltpu.VMEM((tr + 6, pitch, lidar), BF),
        pltpu.VMEM((tr + 6, pitch, 2 * lidar), BF),
        pltpu.VMEM(((tr + 4) // 2, 2, pitch, 3 * joined), BF),
        pltpu.VMEM((pairs, 2, pitch, block), jnp.float32),
        pltpu.VMEM((pitch, joined), jnp.float32),
    ]


def conv_kernel(pos, *refs, parts, sh, tr, pitch, rows, cols, at, cam_at):
    windows = refs[:parts]
    above, below, camera, w1, b1, w2, b2 = refs[parts : parts + 7]
    outs = refs[parts + 7 : parts + 7 + HALVES]
    tile, taps, mid, cells, inside = refs[parts + 7 + HALVES :]
    group, member, half_id, column = pos[0], pos[1], pos[2], pos[3]
    wide = windows[0].shape[2]
    lidar = windows[0].shape[3]
    joined = w1.shape[1]
    block = w2.shape[1] // 2
    col0 = column * (wide - 2 * SIDE) - SIDE

    edge_cols = pitch - wide
    tile[:, wide:, :] = jnp.zeros((tr + 6, edge_cols, lidar), BF)
    tile[tr + UP + DOWN :, 0:wide, :] = jnp.zeros((tr + 6 - tr - UP - DOWN, wide, lidar), BF)
    col = lax.broadcasted_iota(jnp.int32, inside.shape, 0) + col0
    inside[...] = jnp.where((col >= 0) & (col < cols), 1.0, 0.0)

    tile[0:UP, 0:wide, :] = above[at]
    for d in range(parts):
        source = lax.rem(member - d + parts, parts)
        tile[pl.ds(UP + source * sh, sh), 0:wide, :] = windows[d][at]
    tile[UP + tr : UP + tr + DOWN, 0:wide, :] = below[at]

    step = 6
    flat = step * pitch

    def shift(i, _):
        r = i * step
        x = tile[pl.ds(r, step)].reshape(flat, lidar).astype(jnp.float32)
        taps[pl.ds(r, step), :, 0:lidar] = pltpu.roll(x, 1, 0).astype(BF).reshape(step, pitch, lidar)
        taps[pl.ds(r, step), :, lidar:] = pltpu.roll(x, flat - 1, 0).astype(BF).reshape(step, pitch, lidar)
        return 0

    lax.fori_loop(0, (tr + 6) // step, shift, 0)

    n1 = (tr + 4) // 2
    m1 = n1 * pitch

    def first(i, _):
        r = i * n1
        lhs = []
        for dy in range(3):
            lhs.append(tile[pl.ds(r + dy, n1)].reshape(m1, lidar))
            lhs.append(taps[pl.ds(r + dy, n1)].reshape(m1, 2 * lidar))
            lhs.append(camera[cam_at, pl.ds(r + dy, n1)].reshape(m1, camera.shape[3]))
        acc = jnp.dot(jnp.concatenate(lhs, axis=1), w1[...], preferred_element_type=jnp.float32)
        v = jnp.maximum(acc + b1[...], 0.0).reshape(n1, pitch, joined)
        kept = []
        for y in range(n1):
            row = group * tr - 2 + r + y
            kept.append(v[y] * (inside[...] * jnp.where((row >= 0) & (row < rows), 1.0, 0.0)))
        v = jnp.concatenate(kept, axis=0)
        shape = (n1 // 2, 2, pitch, joined)
        p = pl.ds(i * (n1 // 2), n1 // 2)
        mid[p, :, :, 0:joined] = pltpu.roll(v, 1, 0).astype(BF).reshape(shape)
        mid[p, :, :, joined : 2 * joined] = v.astype(BF).reshape(shape)
        mid[p, :, :, 2 * joined :] = pltpu.roll(v, m1 - 1, 0).astype(BF).reshape(shape)
        return 0

    lax.fori_loop(0, (tr + 4) // n1, first, 0)

    n2 = (tr + 2) // 2
    m2 = n2 * pitch
    lhs = [mid[i // 2 : i // 2 + n2, i % 2].reshape(m2, 3 * joined) for i in range(4)]
    acc = jnp.dot(jnp.concatenate(lhs, axis=1), w2[...], preferred_element_type=jnp.float32)
    v = pltpu.roll(jnp.maximum(acc + b2[...], 0.0), SIDE, 0)
    cells[:, 0] = v[:, :block].reshape(n2, pitch, block)
    cells[:, 1] = v[:, block:].reshape(n2, pitch, block)
    pairs = tr // 2
    w = (wide - 2 * SIDE) // HALVES
    for sub in range(HALVES):
        c = 2 * SIDE + sub * w
        even = cells[0:pairs, 1, c : c + w, :].astype(BF)
        odd = cells[1 : pairs + 1, 0, c : c + w, :].astype(BF)
        top = jnp.where(group > 0, cells[0, 0, c : c + w, :], 0.0)
        corner = jnp.broadcast_to(cells[pairs, 0, c - 1 : c, :], (w, block))
        beside = cells[0:pairs, :, c - 1, :].reshape(tr, block)
        if sub == 0:
            corner = jnp.where(column > 0, corner, 0.0)
            beside = jnp.where(column > 0, beside, 0.0)
        row = lax.broadcasted_iota(jnp.int32, beside.shape, 0)
        beside = jnp.where((row == 0) & (group == 0), 0.0, beside)
        edge = jnp.where(half_id == 0, top, corner).astype(BF)
        beside = beside.astype(BF)
        for h in range(HALVES):

            @pl.when(lax.rem(half_id + h, HALVES) == sub)
            def _():
                outs[h][0, 0:pairs, 0] = even
                outs[h][0, 0:pairs, 1] = odd
                outs[h][0, pairs, 0] = edge
                outs[h][0, pairs, 1] = beside


def encode_kernel(pos, *refs, parts, half_rows, w):
    pieces = refs[:parts]
    w3, b3, wp, bp = refs[parts : parts + 4]
    out, grid, grown = refs[-3:]
    me = pos[0]
    block = pieces[0].shape[4]
    for h in range(parts):
        part = lax.rem(me - h + parts, parts)
        base = part * half_rows
        x = pieces[h]
        grid[pl.ds(base, half_rows), 1, 1 : w + 1, :] = x[0, 0:half_rows, 0].astype(jnp.float32)
        grid[pl.ds(base + 1, half_rows), 0, 1 : w + 1, :] = x[0, 0:half_rows, 1].astype(jnp.float32)
        beside = x[0, half_rows, 1].astype(jnp.float32)
        for r in range(2 * half_rows):
            grid[base + r // 2, r % 2, 0:1, :] = beside[r : r + 1]
        edge = x[0, half_rows, 0].astype(jnp.float32)

        @pl.when(part == 0)
        def _():
            grid[0, 0, 1 : w + 1, :] = edge

        @pl.when(part == parts - 1)
        def _():
            grid[parts * half_rows, 0, 0:1, :] = edge[0:1]

    n = parts * half_rows
    jd = rounded(w // 2, 8)
    m = n * jd
    lhs = []
    for a in range(3):
        for b in range(3):
            x = grid[pl.ds(a // 2, n), a % 2, pl.ds(b, jd, stride=2), :]
            lhs.append(x.reshape(m, block).astype(BF))
    deep = jnp.dot(jnp.concatenate(lhs, axis=1), w3[...], preferred_element_type=jnp.float32)
    deep = jnp.maximum(deep + b3[...], 0.0).astype(BF)
    branch = jnp.dot(deep, wp[...], preferred_element_type=jnp.float32)
    branch = jnp.maximum(branch + bp[...], 0.0).astype(BF).astype(jnp.float32).reshape(n, jd, wp.shape[1])
    grown[:, pl.ds(0, jd, stride=2), :] = branch
    grown[:, pl.ds(1, jd, stride=2), :] = branch
    up = grown[:, 0:w, :].astype(BF)
    out[0, :, 0, :, 0:block] = grid[0:n, 1, 1 : w + 1, :].astype(BF)
    out[0, :, 1, :, 0:block] = grid[1 : n + 1, 0, 1 : w + 1, :].astype(BF)
    out[0, :, 0, :, block:] = up
    out[0, :, 1, :, block:] = up


def solution(mesh):
    n_rows, n_cols = mesh.shape["rows"], mesh.shape["cols"]
    members = n_cols // HALVES
    groups = n_rows * HALVES
    total = n_rows * n_cols
    half = members // 2
    turn = 2 if members % 4 == 0 else 0

    tile_of = [[(2 * m if m < half else 2 * (members - 1 - m) + 1) ^ t for m in range(members)] for t in (0, turn)]
    holder = [[tiles.index(j) for j in range(members)] for tiles in tile_of]

    def seat(g, j):
        return g * members + holder[g // HALVES % 2][j]

    def local(lidar, camera, joined_weight, joined_bias, block_weight, block_bias, down_weight, down_bias, proj_weight, proj_bias):
        frames, sh, cols, lidar_ch = lidar.shape
        rows, sc, cam_ch = camera.shape[1:]
        tr = sh * members
        tw = cols // members
        wide = tw + 2 * SIDE
        pitch = rounded(wide, 16)
        w = cols // n_cols
        joined = joined_weight.shape[3]
        block = block_weight.shape[3]
        place = lax.axis_index(AXES)
        group = place // members
        member = place % members
        cindex = lax.axis_index("cols")
        kgroup = cindex // members

        def send(x, pairs):
            return lax.ppermute(x, AXES, pairs)

        def across(x, by_group, by_column):
            pairs = []
            for g in range(groups):
                for j in range(members):
                    if 0 <= g + by_group < groups and 0 <= j + by_column < members:
                        pairs.append((seat(g, j), seat(g + by_group, j + by_column)))
            return send(x, pairs)

        def column_of(m):
            return jnp.where(m < half, 2 * m, 2 * (members - 1 - m) + 1) ^ (turn * (group // HALVES % 2))

        joint = joined_weight.reshape(-1, joined)
        square = block_weight.reshape(-1, block)
        deep1 = 3 * (3 * lidar_ch + rounded(3 * cam_ch, 256))
        w1, w2 = pl.pallas_call(
            lambda *refs: weights_kernel(*refs, lidar=lidar_ch, camera=cam_ch),
            out_shape=[
                jax.ShapeDtypeStruct((deep1, joined), BF),
                jax.ShapeDtypeStruct((4 * 3 * joined, 2 * block), BF),
            ],
            compiler_params=limit(14),
            name="weights",
        )(joint, square)
        w3 = down_weight.reshape(-1, down_weight.shape[3])
        b1 = joined_bias.reshape(1, -1)
        b2 = jnp.concatenate([block_bias, block_bias]).reshape(1, -1)
        b3 = down_bias.reshape(1, -1)
        bp = proj_bias.reshape(1, -1)

        span = rounded(tr + UP + DOWN, 8)
        lanes = frames * span
        turned = jnp.transpose(camera, (0, 2, 3, 1))
        strip = jax.ShapeDtypeStruct((sc, cam_ch, lanes), BF)
        packed = pl.pallas_call(
            lambda *refs: camera_pack_kernel(*refs, tr=tr, span=span),
            grid_spec=pltpu.PrefetchScalarGridSpec(
                num_scalar_prefetch=1,
                grid=(1,),
                in_specs=[whole(turned)],
                out_specs=[whole(strip)] * groups,
            ),
            out_shape=[strip] * groups,
            compiler_params=limit(14),
            name="camera_pack",
        )(place.reshape(1).astype(jnp.int32), turned)
        lidar, packed = lax.optimization_barrier((lidar, packed))
        arrived = [
            send(packed[p], [(s, seat((s + p) % groups, s // groups)) for s in range(total)])
            for p in range(groups)
        ]
        tail, head = pick(arrived, (group + 1) % groups, group, 0)
        left = across(tail, 0, 1)
        right = across(head, 0, -1)
        cam = pl.pallas_call(
            lambda *refs: camera_unpack_kernel(*refs, groups=groups, sc=sc, cam_ch=cam_ch),
            grid_spec=pltpu.PrefetchScalarGridSpec(
                num_scalar_prefetch=1,
                grid=(1,),
                in_specs=[whole(x) for x in arrived] + [whole(left), whole(right)],
                out_specs=pl.BlockSpec((lanes, pitch, rounded(3 * cam_ch, 256)), lambda i, p: (0, 0, 0)),
                scratch_shapes=[
                    pltpu.VMEM((tw + UP + DOWN, cam_ch, lanes), BF),
                    pltpu.VMEM((lanes, pitch, 128), jnp.float32),
                ],
            ),
            out_shape=jax.ShapeDtypeStruct((lanes, pitch, rounded(3 * cam_ch, 256)), BF),
            compiler_params=limit(16),
            name="camera_unpack",
        )(group.reshape(1).astype(jnp.int32), *arrived, left, right)
        cam = cam.reshape(frames, span, pitch, -1)

        padded = jnp.pad(lidar, ((0, 0), (0, 0), (SIDE, SIDE), (0, 0)))
        pos = jnp.stack([group, member, kgroup, column_of(member)]).astype(jnp.int32)
        pairs2 = (tr + 2) // 2
        half_rows = tr // 2
        n = HALVES * half_rows
        jd = rounded(w // 2, 8)
        blocks = jax.ShapeDtypeStruct((1, pairs2, 2, w, block), BF)
        flops = 2 * pitch * ((tr + 4) * w1.shape[0] * joined + pairs2 * w2.shape[0] * 2 * block)
        framed = lambda a: pl.BlockSpec((1,) + a.shape[1:], lambda f, p: (f,) + (0,) * (a.ndim - 1))
        encoded = None
        step = frames // CHUNKS
        for f0 in range(0, frames, step):
            windows = []
            for d in range(members):
                x = lax.dynamic_slice(padded, (f0, 0, column_of((member + d) % members) * tw, 0), (step, sh, wide, lidar_ch))
                if d:
                    x = send(x, [(g * members + j, g * members + (j + d) % members) for g in range(groups) for j in range(members)])
                windows.append(x)
            last, head = pick(windows, (member + 1) % members, member, 1)
            above = across(last, 1, 0)
            below = across(head, -1, 0)
            for f1 in range(f0, f0 + step):
                tiles = pl.pallas_call(
                    functools.partial(conv_kernel, parts=members, sh=sh, tr=tr, pitch=pitch, rows=rows, cols=cols, at=f1 - f0, cam_at=f1),
                    in_specs=[pl.BlockSpec(memory_space=pltpu.SMEM)] + [pl.BlockSpec(memory_space=pltpu.VMEM)] * (members + 7),
                    out_specs=[pl.BlockSpec(memory_space=pltpu.VMEM)] * HALVES,
                    scratch_shapes=conv_scratch(tr, pitch, lidar_ch, joined, block, pairs2),
                    out_shape=[blocks] * HALVES,
                    compiler_params=limit(28),
                    cost_estimate=pl.CostEstimate(flops=flops, bytes_accessed=2 * 10**6, transcendentals=0),
                )(pos, *windows, above, below, cam, w1, b1, w2, b2)
                pieces = []
                for h in range(HALVES):
                    pairs = []
                    for s in range(total):
                        r, c = divmod(s, n_cols)
                        k, m = divmod(c, members)
                        pairs.append((s, r * n_cols + HALVES * tile_of[r % 2][m] + (k + h) % HALVES))
                    pieces.append(send(tiles[h], pairs))
                old = [] if encoded is None else [encoded]
                encoded = pl.pallas_call(
                    lambda *refs: encode_kernel(*refs, parts=HALVES, half_rows=half_rows, w=w),
                    grid_spec=pltpu.PrefetchScalarGridSpec(
                        num_scalar_prefetch=1,
                        grid=(1,),
                        in_specs=[framed(x) for x in pieces] + [whole(x) for x in (w3, b3, proj_weight, bp)] + [pl.BlockSpec(memory_space=pl.ANY)] * len(old),
                        out_specs=pl.BlockSpec((1, n, 2, w, 2 * block), lambda f, p, f1=f1: (f + f1, 0, 0, 0, 0)),
                        scratch_shapes=[
                            pltpu.VMEM((n + 1, 2, rounded(w + 1, 8) + 16, block), jnp.float32),
                            pltpu.VMEM((n, 2 * jd, block), jnp.float32),
                        ],
                    ),
                    out_shape=jax.ShapeDtypeStruct((frames, n, 2, w, 2 * block), BF),
                    input_output_aliases={5 + HALVES: 0} if old else {},
                    compiler_params=limit(12),
                    cost_estimate=pl.CostEstimate(flops=2 * n * jd * w3.shape[0] * 256, bytes_accessed=10**6, transcendentals=0),
                )(cindex.reshape(1).astype(jnp.int32), *pieces, w3, b3, proj_weight, bp, *old)
        return encoded.reshape(frames, 2 * n, w, 2 * block)

    return jax.shard_map(
        local,
        mesh=mesh,
        in_specs=(
            P("frames", AXES, None, None),
            P("frames", None, AXES, None),
            P(), P(), P(), P(), P(), P(), P(), P(),
        ),
        out_specs=P("frames", "rows", "cols", None),
        check_vma=False,
    )
```

```python
import functools

import jax
import jax.numpy as jnp
from jax import lax
from jax.experimental import pallas as pl
from jax.experimental.pallas import tpu as pltpu
from jax.sharding import PartitionSpec as P


AXES = ("rows", "cols")
CHUNKS = 2
HALVES = 2
SIDE = 4
UP, DOWN = 3, 2
BF = jnp.bfloat16


def rounded(n, to):
    return -(-n // to) * to


def limit(mib):
    return pltpu.CompilerParams(vmem_limit_bytes=mib * 2**20)


def whole(a):
    return pl.BlockSpec(a.shape, lambda *_: (0,) * a.ndim)


def weights_kernel(joint, square, w1, w2, *, lidar, camera):
    joined, block = joint.shape[1], square.shape[1]
    ch = lidar + camera
    deep = w1.shape[0] // 3
    for dy in range(3):
        base = dy * deep
        for dx in range(3):
            at = (dy * 3 + dx) * ch
            to = base + (1, 0, 2)[dx] * lidar
            w1[to : to + lidar, :] = joint[at : at + lidar, :]
            to = base + 3 * lidar + dx * camera
            w1[to : to + camera, :] = joint[at + lidar : at + ch, :]
        w1[base + 3 * ch : base + deep, :] = jnp.zeros((deep - 3 * ch, joined), BF)
    tall = square.shape[0]
    gap = w2.shape[0] - tall
    w2[0:tall, 0:block] = square[...]
    w2[tall:, 0:block] = jnp.zeros((gap, block), BF)
    w2[gap:, block:] = square[...]
    w2[0:gap, block:] = jnp.zeros((gap, block), BF)


def camera_pack_kernel(pos, x, *refs, tr, span):
    frames, sc, ch, rows = x.shape
    groups = len(refs) // 2
    outs, rims = refs[:groups], refs[groups:]
    width = frames * span
    place = pos[0]
    row = lax.broadcasted_iota(jnp.int32, (rows, width), 0)
    lane = lax.broadcasted_iota(jnp.int32, (rows, width), 1)

    def picks(f, targets):
        parts = []
        for target in targets:
            start = target * tr - UP
            parts.append(jnp.where(row + f * span == lane + start, jnp.where(lane // span == f, 1.0, 0.0), 0.0).astype(BF))
        return jnp.concatenate(parts, axis=1)

    main, rim = None, None
    rightmost = lax.rem(place, groups) == groups - 1
    for f in range(frames):
        pick = picks(f, [lax.rem(place + p, groups) for p in range(groups)])
        part = jnp.dot(x[f].reshape(sc * ch, rows), pick, preferred_element_type=jnp.float32)
        main = part if main is None else main + part
        pick = picks(f, [lax.rem(e + jnp.where(rightmost, 0, 1), groups) for e in range(groups)])
        border = jnp.where(rightmost, x[f, sc - UP : sc].astype(jnp.float32), x[f, 0:UP].astype(jnp.float32)).astype(BF)
        part = jnp.dot(border.reshape(UP * ch, rows), pick, preferred_element_type=jnp.float32)
        rim = part if rim is None else rim + part
    for p in range(groups):
        outs[p][...] = main[:, p * width : (p + 1) * width].astype(BF).reshape(sc, ch, width)
        rims[p][...] = rim[:, p * width : (p + 1) * width].astype(BF).reshape(UP, ch, width)


def window_kernel(pos, x, *outs, tw):
    n = x.shape[2] // tw
    wide = tw + 2 * SIDE
    edge = jnp.zeros((x.shape[1], SIDE, x.shape[3]), BF)
    for d in range(len(outs)):
        for c in range(n):

            @pl.when(pos[d] == c)
            def _():
                lo, hi = max(c * tw - SIDE, 0), min((c + 1) * tw + SIDE, n * tw)
                at = lo - (c * tw - SIDE)
                if at:
                    outs[d][0, :, 0:at, :] = edge
                if at + hi - lo < wide:
                    outs[d][0, :, at + hi - lo :, :] = edge
                outs[d][0, :, at : at + hi - lo, :] = x[0, :, lo:hi, :]


def camera_unpack_kernel(pos, *refs, groups, sc, cam_ch):
    strips, rims = refs[:groups], refs[groups : 2 * groups]
    out, stage, cells = refs[2 * groups :]
    group = pos[0]
    lanes = stage.shape[2]
    pitch = cells.shape[1]
    for p in range(groups):
        q = lax.rem(group - p + groups, groups)
        stage[pl.ds(UP + q * sc, sc)] = strips[p][...]
    n = UP + groups * sc + DOWN
    for e in range(groups):

        @pl.when(group == e)
        def _():
            stage[0:UP] = rims[e][...]

        @pl.when(group == (e + 1) % groups)
        def _():
            stage[n - DOWN : n] = rims[e][0:DOWN]

    lead = SIDE - UP
    cells[:, 0:8, :] = jnp.zeros((lanes, 8, 128), jnp.float32)
    low = (lead + n) // 8 * 8
    cells[:, low:, :] = jnp.zeros((lanes, pitch - low, 128), jnp.float32)
    for c in range(n):
        x = stage[c].astype(jnp.float32)
        x = jnp.concatenate([x, jnp.zeros((128 - cam_ch, lanes), jnp.float32)], axis=0)
        cells[:, lead + c, :] = x.T
    step = 8
    flat = step * pitch
    lane = lax.broadcasted_iota(jnp.int32, (flat, 128), 1)

    def widen(i, _):
        x = cells[pl.ds(i * step, step)].reshape(flat, 128)
        taps = [pltpu.roll(x, 1, 0), x, pltpu.roll(x, flat - 1, 0)]
        for v in range(out.shape[2] // 128):
            y = jnp.zeros((flat, 128), jnp.float32)
            for t in range(3):
                lo, hi = t * cam_ch - v * 128, (t + 1) * cam_ch - v * 128
                if hi > 0 and lo < 128:
                    turned = pltpu.roll(taps[t], lo % 128, 1) if lo % 128 else taps[t]
                    y = jnp.where((lane >= lo) & (lane < hi), turned, y)
            out[pl.ds(i * step, step), :, v * 128 : (v + 1) * 128] = y.astype(BF).reshape(step, pitch, 128)
        return 0

    lax.fori_loop(0, lanes // step, widen, 0)


def pick_kernel(pos, *refs):
    parts = (len(refs) - 2) // 2
    tail, head = refs[-2:]
    for d in range(parts):

        @pl.when(pos[0] == d)
        def _():
            tail[...] = refs[d][...]

        @pl.when(pos[1] == d)
        def _():
            head[...] = refs[parts + d][...]


def pick(arrays, tail_of, head_of, dim):
    size = arrays[0].shape[dim]
    specs, shapes, outs = [], [], []
    for n, at in ((UP, size // UP - 1), (DOWN, 0)):
        shape = arrays[0].shape[:dim] + (n,) + arrays[0].shape[dim + 1 :]
        where = tuple(at if i == dim else 0 for i in range(len(shape)))
        specs += [pl.BlockSpec(shape, lambda i, p, where=where: where)] * len(arrays)
        shapes.append(jax.ShapeDtypeStruct(shape, BF))
        outs.append(pl.BlockSpec(shape, lambda i, p, n=len(shape): (0,) * n))
    return pl.pallas_call(
        pick_kernel,
        grid_spec=pltpu.PrefetchScalarGridSpec(num_scalar_prefetch=1, grid=(1,), in_specs=specs, out_specs=outs),
        out_shape=shapes,
        compiler_params=limit(3),
    )(jnp.stack([tail_of, head_of]).astype(jnp.int32), *arrays, *arrays)


def conv_scratch(tr, pitch, lidar, joined, block, pairs):
    return [
        pltpu.VMEM((tr + 6, pitch, lidar), BF),
        pltpu.VMEM((tr + 6, pitch, 2 * lidar), BF),
        pltpu.VMEM(((tr + 4) // 2, 2, pitch, 3 * joined), BF),
        pltpu.VMEM((pairs, 2, pitch, block), jnp.float32),
        pltpu.VMEM((pitch, joined), jnp.float32),
    ]


def conv_kernel(pos, *refs, parts, sh, tr, pitch, rows, cols, at, cam_at):
    windows = refs[:parts]
    above, below, camera, w1, b1, w2, b2 = refs[parts : parts + 7]
    outs = refs[parts + 7 : parts + 7 + HALVES]
    tile, taps, mid, cells, inside = refs[parts + 7 + HALVES :]
    group, member, half_id, column = pos[0], pos[1], pos[2], pos[3]
    wide = windows[0].shape[2]
    lidar = windows[0].shape[3]
    joined = w1.shape[1]
    block = w2.shape[1] // 2
    col0 = column * (wide - 2 * SIDE) - SIDE

    edge_cols = pitch - wide
    tile[:, wide:, :] = jnp.zeros((tr + 6, edge_cols, lidar), BF)
    tile[tr + UP + DOWN :, 0:wide, :] = jnp.zeros((tr + 6 - tr - UP - DOWN, wide, lidar), BF)
    col = lax.broadcasted_iota(jnp.int32, inside.shape, 0) + col0
    inside[...] = jnp.where((col >= 0) & (col < cols), 1.0, 0.0)

    tile[0:UP, 0:wide, :] = above[at]
    for d in range(parts):
        source = lax.rem(member - d + parts, parts)
        tile[pl.ds(UP + source * sh, sh), 0:wide, :] = windows[d][at]
    tile[UP + tr : UP + tr + DOWN, 0:wide, :] = below[at]

    step = 6
    flat = step * pitch

    def shift(i, _):
        r = i * step
        x = tile[pl.ds(r, step)].reshape(flat, lidar).astype(jnp.float32)
        taps[pl.ds(r, step), :, 0:lidar] = pltpu.roll(x, 1, 0).astype(BF).reshape(step, pitch, lidar)
        taps[pl.ds(r, step), :, lidar:] = pltpu.roll(x, flat - 1, 0).astype(BF).reshape(step, pitch, lidar)
        return 0

    lax.fori_loop(0, (tr + 6) // step, shift, 0)

    n1 = (tr + 4) // 2
    m1 = n1 * pitch

    def first(i, _):
        r = i * n1
        lhs = []
        for dy in range(3):
            lhs.append(tile[pl.ds(r + dy, n1)].reshape(m1, lidar))
            lhs.append(taps[pl.ds(r + dy, n1)].reshape(m1, 2 * lidar))
            lhs.append(camera[cam_at, pl.ds(r + dy, n1)].reshape(m1, camera.shape[3]))
        acc = jnp.dot(jnp.concatenate(lhs, axis=1), w1[...], preferred_element_type=jnp.float32)
        v = jnp.maximum(acc + b1[...], 0.0).reshape(n1, pitch, joined)
        kept = []
        for y in range(n1):
            row = group * tr - 2 + r + y
            kept.append(v[y] * (inside[...] * jnp.where((row >= 0) & (row < rows), 1.0, 0.0)))
        v = jnp.concatenate(kept, axis=0)
        shape = (n1 // 2, 2, pitch, joined)
        p = pl.ds(i * (n1 // 2), n1 // 2)
        mid[p, :, :, 0:joined] = pltpu.roll(v, 1, 0).astype(BF).reshape(shape)
        mid[p, :, :, joined : 2 * joined] = v.astype(BF).reshape(shape)
        mid[p, :, :, 2 * joined :] = pltpu.roll(v, m1 - 1, 0).astype(BF).reshape(shape)
        return 0

    lax.fori_loop(0, (tr + 4) // n1, first, 0)

    n2 = (tr + 2) // 2
    m2 = n2 * pitch
    lhs = [mid[i // 2 : i // 2 + n2, i % 2].reshape(m2, 3 * joined) for i in range(4)]
    acc = jnp.dot(jnp.concatenate(lhs, axis=1), w2[...], preferred_element_type=jnp.float32)
    v = pltpu.roll(jnp.maximum(acc + b2[...], 0.0), SIDE, 0)
    cells[:, 0] = v[:, :block].reshape(n2, pitch, block)
    cells[:, 1] = v[:, block:].reshape(n2, pitch, block)
    pairs = tr // 2
    w = (wide - 2 * SIDE) // HALVES
    for sub in range(HALVES):
        c = 2 * SIDE + sub * w
        even = cells[0:pairs, 1, c : c + w, :].astype(BF)
        odd = cells[1 : pairs + 1, 0, c : c + w, :].astype(BF)
        top = jnp.where(group > 0, cells[0, 0, c : c + w, :], 0.0)
        corner = jnp.broadcast_to(cells[pairs, 0, c - 1 : c, :], (w, block))
        beside = cells[0:pairs, :, c - 1, :].reshape(tr, block)
        if sub == 0:
            corner = jnp.where(column > 0, corner, 0.0)
            beside = jnp.where(column > 0, beside, 0.0)
        row = lax.broadcasted_iota(jnp.int32, beside.shape, 0)
        beside = jnp.where((row == 0) & (group == 0), 0.0, beside)
        edge = jnp.where(half_id == 0, top, corner).astype(BF)
        beside = beside.astype(BF)
        for h in range(HALVES):

            @pl.when(lax.rem(half_id + h, HALVES) == sub)
            def _():
                outs[h][0, 0:pairs, 0] = even
                outs[h][0, 0:pairs, 1] = odd
                outs[h][0, pairs, 0] = edge
                outs[h][0, pairs, 1] = beside


def encode_kernel(pos, *refs, parts, half_rows, w):
    pieces = refs[:parts]
    w3, b3, wp, bp = refs[parts : parts + 4]
    out, grid, grown = refs[-3:]
    me = pos[0]
    block = pieces[0].shape[4]
    for h in range(parts):
        part = lax.rem(me - h + parts, parts)
        base = part * half_rows
        x = pieces[h]
        grid[pl.ds(base, half_rows), 1, 1 : w + 1, :] = x[0, 0:half_rows, 0].astype(jnp.float32)
        grid[pl.ds(base + 1, half_rows), 0, 1 : w + 1, :] = x[0, 0:half_rows, 1].astype(jnp.float32)
        beside = x[0, half_rows, 1].astype(jnp.float32)
        for r in range(2 * half_rows):
            grid[base + r // 2, r % 2, 0:1, :] = beside[r : r + 1]
        edge = x[0, half_rows, 0].astype(jnp.float32)

        @pl.when(part == 0)
        def _():
            grid[0, 0, 1 : w + 1, :] = edge

        @pl.when(part == parts - 1)
        def _():
            grid[parts * half_rows, 0, 0:1, :] = edge[0:1]

    n = parts * half_rows
    jd = rounded(w // 2, 8)
    m = n * jd
    lhs = []
    for a in range(3):
        for b in range(3):
            x = grid[pl.ds(a // 2, n), a % 2, pl.ds(b, jd, stride=2), :]
            lhs.append(x.reshape(m, block).astype(BF))
    deep = jnp.dot(jnp.concatenate(lhs, axis=1), w3[...], preferred_element_type=jnp.float32)
    deep = jnp.maximum(deep + b3[...], 0.0).astype(BF)
    branch = jnp.dot(deep, wp[...], preferred_element_type=jnp.float32)
    branch = jnp.maximum(branch + bp[...], 0.0).astype(BF).astype(jnp.float32).reshape(n, jd, wp.shape[1])
    grown[:, pl.ds(0, jd, stride=2), :] = branch
    grown[:, pl.ds(1, jd, stride=2), :] = branch
    up = grown[:, 0:w, :].astype(BF)
    out[0, :, 0, :, 0:block] = grid[0:n, 1, 1 : w + 1, :].astype(BF)
    out[0, :, 1, :, 0:block] = grid[1 : n + 1, 0, 1 : w + 1, :].astype(BF)
    out[0, :, 0, :, block:] = up
    out[0, :, 1, :, block:] = up


def solution(mesh):
    n_rows, n_cols = mesh.shape["rows"], mesh.shape["cols"]
    members = n_cols // HALVES
    groups = n_rows * HALVES
    total = n_rows * n_cols
    half = members // 2
    turn = 2 if members % 4 == 0 else 0

    tile_of = [[(2 * m if m < half else 2 * (members - 1 - m) + 1) ^ t for m in range(members)] for t in (0, turn)]
    holder = [[tiles.index(j) for j in range(members)] for tiles in tile_of]

    def seat(g, j):
        return g * members + holder[g // HALVES % 2][j]

    def local(lidar, camera, joined_weight, joined_bias, block_weight, block_bias, down_weight, down_bias, proj_weight, proj_bias):
        frames, sh, cols, lidar_ch = lidar.shape
        rows, sc, cam_ch = camera.shape[1:]
        tr = sh * members
        tw = cols // members
        wide = tw + 2 * SIDE
        pitch = rounded(wide, 16)
        w = cols // n_cols
        joined = joined_weight.shape[3]
        block = block_weight.shape[3]
        place = lax.axis_index(AXES)
        group = place // members
        member = place % members
        cindex = lax.axis_index("cols")
        kgroup = cindex // members

        def send(x, pairs):
            return lax.ppermute(x, AXES, pairs)

        def across(x, by_group, by_column):
            pairs = []
            for g in range(groups):
                for j in range(members):
                    if 0 <= g + by_group < groups and 0 <= j + by_column < members:
                        pairs.append((seat(g, j), seat(g + by_group, j + by_column)))
            return send(x, pairs)

        def column_of(m):
            return jnp.where(m < half, 2 * m, 2 * (members - 1 - m) + 1) ^ (turn * (group // HALVES % 2))

        joint = joined_weight.reshape(-1, joined)
        square = block_weight.reshape(-1, block)
        deep1 = 3 * (3 * lidar_ch + rounded(3 * cam_ch, 256))
        w1, w2 = pl.pallas_call(
            lambda *refs: weights_kernel(*refs, lidar=lidar_ch, camera=cam_ch),
            out_shape=[
                jax.ShapeDtypeStruct((deep1, joined), BF),
                jax.ShapeDtypeStruct((4 * 3 * joined, 2 * block), BF),
            ],
            compiler_params=limit(14),
            name="weights",
        )(joint, square)
        w3 = down_weight.reshape(-1, down_weight.shape[3])
        b1 = joined_bias.reshape(1, -1)
        b2 = jnp.concatenate([block_bias, block_bias]).reshape(1, -1)
        b3 = down_bias.reshape(1, -1)
        bp = proj_bias.reshape(1, -1)

        span = rounded(tr + UP + DOWN, 8)
        lanes = frames * span
        turned = jnp.transpose(camera, (0, 2, 3, 1))
        strip = jax.ShapeDtypeStruct((sc, cam_ch, lanes), BF)
        rim = jax.ShapeDtypeStruct((UP, cam_ch, lanes), BF)
        packed = pl.pallas_call(
            lambda *refs: camera_pack_kernel(*refs, tr=tr, span=span),
            grid_spec=pltpu.PrefetchScalarGridSpec(
                num_scalar_prefetch=1,
                grid=(1,),
                in_specs=[whole(turned)],
                out_specs=[whole(strip)] * groups + [whole(rim)] * groups,
            ),
            out_shape=[strip] * groups + [rim] * groups,
            compiler_params=limit(14),
            name="camera_pack",
        )(place.reshape(1).astype(jnp.int32), turned)
        arrived = [send(packed[p], [(s, seat((s + p) % groups, s // groups)) for s in range(total)]) for p in range(groups)]
        for e in range(groups):
            pairs = [(groups * j + groups - 1, seat(e, j + 1)) for j in range(members - 1)]
            pairs += [(groups * j, seat((e + 1) % groups, j - 1)) for j in range(1, members)]
            arrived.append(send(packed[groups + e], pairs))
        cam = pl.pallas_call(
            lambda *refs: camera_unpack_kernel(*refs, groups=groups, sc=sc, cam_ch=cam_ch),
            grid_spec=pltpu.PrefetchScalarGridSpec(
                num_scalar_prefetch=1,
                grid=(1,),
                in_specs=[whole(x) for x in arrived],
                out_specs=pl.BlockSpec((lanes, pitch, rounded(3 * cam_ch, 256)), lambda i, p: (0, 0, 0)),
                scratch_shapes=[
                    pltpu.VMEM((tw + UP + DOWN, cam_ch, lanes), BF),
                    pltpu.VMEM((lanes, pitch, 128), jnp.float32),
                ],
            ),
            out_shape=jax.ShapeDtypeStruct((lanes, pitch, rounded(3 * cam_ch, 256)), BF),
            compiler_params=limit(16),
            name="camera_unpack",
        )(group.reshape(1).astype(jnp.int32), *arrived)
        cam = cam.reshape(frames, span, pitch, -1)

        pos = jnp.stack([group, member, kgroup, column_of(member)]).astype(jnp.int32)
        pairs2 = (tr + 2) // 2
        half_rows = tr // 2
        n = HALVES * half_rows
        jd = rounded(w // 2, 8)
        blocks = jax.ShapeDtypeStruct((1, pairs2, 2, w, block), BF)
        flops = 2 * pitch * ((tr + 4) * w1.shape[0] * joined + pairs2 * w2.shape[0] * 2 * block)
        framed = lambda a: pl.BlockSpec((1,) + a.shape[1:], lambda f, p: (f,) + (0,) * (a.ndim - 1))
        encoded = None
        step = frames // CHUNKS
        for f0 in range(0, frames, step):
            source = lidar if not f0 else lax.optimization_barrier((lidar, packed[0]))[0]
            window = jax.ShapeDtypeStruct((step, sh, wide, lidar_ch), BF)
            windows = pl.pallas_call(
                functools.partial(window_kernel, tw=tw),
                grid_spec=pltpu.PrefetchScalarGridSpec(
                    num_scalar_prefetch=1,
                    grid=(step,),
                    in_specs=[pl.BlockSpec((1, sh, cols, lidar_ch), lambda f, p, f0=f0: (f + f0, 0, 0, 0))],
                    out_specs=[framed(window)] * members,
                ),
                out_shape=[window] * members,
                compiler_params=limit(6),
                name="windows",
            )(jnp.stack([column_of((member + d) % members) for d in range(members)]).astype(jnp.int32), source)
            windows = [windows[0]] + [
                send(windows[d], [(g * members + m, g * members + (m + d) % members) for g in range(groups) for m in range(members)])
                for d in range(1, members)
            ]
            last, head = pick(windows, (member + 1) % members, member, 1)
            above = across(last, 1, 0)
            below = across(head, -1, 0)
            for f1 in range(f0, f0 + step):
                tiles = pl.pallas_call(
                    functools.partial(conv_kernel, parts=members, sh=sh, tr=tr, pitch=pitch, rows=rows, cols=cols, at=f1 - f0, cam_at=f1),
                    in_specs=[pl.BlockSpec(memory_space=pltpu.SMEM)] + [pl.BlockSpec(memory_space=pltpu.VMEM)] * (members + 7),
                    out_specs=[pl.BlockSpec(memory_space=pltpu.VMEM)] * HALVES,
                    scratch_shapes=conv_scratch(tr, pitch, lidar_ch, joined, block, pairs2),
                    out_shape=[blocks] * HALVES,
                    compiler_params=limit(28),
                    cost_estimate=pl.CostEstimate(flops=flops, bytes_accessed=2 * 10**6, transcendentals=0),
                )(pos, *windows, above, below, cam, w1, b1, w2, b2)
                pieces = []
                for h in range(HALVES):
                    pairs = []
                    for s in range(total):
                        r, c = divmod(s, n_cols)
                        k, m = divmod(c, members)
                        pairs.append((s, r * n_cols + HALVES * tile_of[r % 2][m] + (k + h) % HALVES))
                    pieces.append(send(tiles[h], pairs))
                old = [] if encoded is None else [encoded]
                encoded = pl.pallas_call(
                    lambda *refs: encode_kernel(*refs, parts=HALVES, half_rows=half_rows, w=w),
                    grid_spec=pltpu.PrefetchScalarGridSpec(
                        num_scalar_prefetch=1,
                        grid=(1,),
                        in_specs=[framed(x) for x in pieces] + [whole(x) for x in (w3, b3, proj_weight, bp)] + [pl.BlockSpec(memory_space=pl.ANY)] * len(old),
                        out_specs=pl.BlockSpec((1, n, 2, w, 2 * block), lambda f, p, f1=f1: (f + f1, 0, 0, 0, 0)),
                        scratch_shapes=[
                            pltpu.VMEM((n + 1, 2, rounded(w + 1, 8) + 16, block), jnp.float32),
                            pltpu.VMEM((n, 2 * jd, block), jnp.float32),
                        ],
                    ),
                    out_shape=jax.ShapeDtypeStruct((frames, n, 2, w, 2 * block), BF),
                    input_output_aliases={5 + HALVES: 0} if old else {},
                    compiler_params=limit(12),
                    cost_estimate=pl.CostEstimate(flops=2 * n * jd * w3.shape[0] * 256, bytes_accessed=10**6, transcendentals=0),
                )(cindex.reshape(1).astype(jnp.int32), *pieces, w3, b3, proj_weight, bp, *old)
        return encoded.reshape(frames, 2 * n, w, 2 * block)

    return jax.shard_map(
        local,
        mesh=mesh,
        in_specs=(
            P("frames", AXES, None, None),
            P("frames", None, AXES, None),
            P(), P(), P(), P(), P(), P(), P(), P(),
        ),
        out_specs=P("frames", "rows", "cols", None),
        check_vma=False,
    )
```

```python
import functools

import jax
import jax.numpy as jnp
from jax import lax
from jax.experimental import pallas as pl
from jax.experimental.pallas import tpu as pltpu
from jax.sharding import PartitionSpec as P


AXES = ("rows", "cols")
CHUNKS = 1
HALVES = 2
SIDE = 4
UP, DOWN = 3, 2
BF = jnp.bfloat16


def rounded(n, to):
    return -(-n // to) * to


def limit(mib):
    return pltpu.CompilerParams(vmem_limit_bytes=mib * 2**20)


def whole(a):
    return pl.BlockSpec(a.shape, lambda *_: (0,) * a.ndim)


def weights_kernel(joint, square, w1, w2, *, lidar, camera):
    joined, block = joint.shape[1], square.shape[1]
    ch = lidar + camera
    deep = w1.shape[0] // 3
    for dy in range(3):
        base = dy * deep
        for dx in range(3):
            at = (dy * 3 + dx) * ch
            to = base + (1, 0, 2)[dx] * lidar
            w1[to : to + lidar, :] = joint[at : at + lidar, :]
            to = base + 3 * lidar + dx * camera
            w1[to : to + camera, :] = joint[at + lidar : at + ch, :]
        w1[base + 3 * ch : base + deep, :] = jnp.zeros((deep - 3 * ch, joined), BF)
    tall = square.shape[0]
    gap = w2.shape[0] - tall
    w2[0:tall, 0:block] = square[...]
    w2[tall:, 0:block] = jnp.zeros((gap, block), BF)
    w2[gap:, block:] = square[...]
    w2[0:gap, block:] = jnp.zeros((gap, block), BF)


def camera_pack_kernel(pos, x, *refs, tr, span):
    frames, sc, ch, rows = x.shape
    groups = len(refs) // 2
    outs, rims = refs[:groups], refs[groups:]
    width = frames * span
    place = pos[0]
    row = lax.broadcasted_iota(jnp.int32, (rows, width), 0)
    lane = lax.broadcasted_iota(jnp.int32, (rows, width), 1)

    def picks(f, targets):
        parts = []
        for target in targets:
            start = target * tr - UP
            parts.append(jnp.where(row + f * span == lane + start, jnp.where(lane // span == f, 1.0, 0.0), 0.0).astype(BF))
        return jnp.concatenate(parts, axis=1)

    main, rim = None, None
    rightmost = lax.rem(place, groups) == groups - 1
    for f in range(frames):
        pick = picks(f, [lax.rem(place + p, groups) for p in range(groups)])
        part = jnp.dot(x[f].reshape(sc * ch, rows), pick, preferred_element_type=jnp.float32)
        main = part if main is None else main + part
        pick = picks(f, [lax.rem(e + jnp.where(rightmost, 0, 1), groups) for e in range(groups)])
        border = jnp.where(rightmost, x[f, sc - UP : sc].astype(jnp.float32), x[f, 0:UP].astype(jnp.float32)).astype(BF)
        part = jnp.dot(border.reshape(UP * ch, rows), pick, preferred_element_type=jnp.float32)
        rim = part if rim is None else rim + part
    for p in range(groups):
        outs[p][...] = main[:, p * width : (p + 1) * width].astype(BF).reshape(sc, ch, width)
        rims[p][...] = rim[:, p * width : (p + 1) * width].astype(BF).reshape(UP, ch, width)


def window_kernel(pos, x, *outs, tw):
    n = x.shape[2] // tw
    wide = tw + 2 * SIDE
    edge = jnp.zeros((x.shape[1], SIDE, x.shape[3]), BF)
    for d in range(len(outs)):
        for c in range(n):

            @pl.when(pos[d] == c)
            def _():
                lo, hi = max(c * tw - SIDE, 0), min((c + 1) * tw + SIDE, n * tw)
                at = lo - (c * tw - SIDE)
                if at:
                    outs[d][0, :, 0:at, :] = edge
                if at + hi - lo < wide:
                    outs[d][0, :, at + hi - lo :, :] = edge
                outs[d][0, :, at : at + hi - lo, :] = x[0, :, lo:hi, :]


def camera_unpack_kernel(pos, *refs, groups, sc, cam_ch):
    strips, rims = refs[:groups], refs[groups : 2 * groups]
    out, stage, cells = refs[2 * groups :]
    group = pos[0]
    lanes = stage.shape[2]
    pitch = cells.shape[1]
    for p in range(groups):
        q = lax.rem(group - p + groups, groups)
        stage[pl.ds(UP + q * sc, sc)] = strips[p][...]
    n = UP + groups * sc + DOWN
    for e in range(groups):

        @pl.when(group == e)
        def _():
            stage[0:UP] = rims[e][...]

        @pl.when(group == (e + 1) % groups)
        def _():
            stage[n - DOWN : n] = rims[e][0:DOWN]

    lead = SIDE - UP
    cells[:, 0:8, :] = jnp.zeros((lanes, 8, 128), jnp.float32)
    low = (lead + n) // 8 * 8
    cells[:, low:, :] = jnp.zeros((lanes, pitch - low, 128), jnp.float32)
    for c in range(n):
        x = stage[c].astype(jnp.float32)
        x = jnp.concatenate([x, jnp.zeros((128 - cam_ch, lanes), jnp.float32)], axis=0)
        cells[:, lead + c, :] = x.T
    step = 8
    flat = step * pitch
    lane = lax.broadcasted_iota(jnp.int32, (flat, 128), 1)

    def widen(i, _):
        x = cells[pl.ds(i * step, step)].reshape(flat, 128)
        taps = [pltpu.roll(x, 1, 0), x, pltpu.roll(x, flat - 1, 0)]
        for v in range(out.shape[2] // 128):
            y = jnp.zeros((flat, 128), jnp.float32)
            for t in range(3):
                lo, hi = t * cam_ch - v * 128, (t + 1) * cam_ch - v * 128
                if hi > 0 and lo < 128:
                    turned = pltpu.roll(taps[t], lo % 128, 1) if lo % 128 else taps[t]
                    y = jnp.where((lane >= lo) & (lane < hi), turned, y)
            out[pl.ds(i * step, step), :, v * 128 : (v + 1) * 128] = y.astype(BF).reshape(step, pitch, 128)
        return 0

    lax.fori_loop(0, lanes // step, widen, 0)


def pick_kernel(pos, *refs):
    parts = (len(refs) - 2) // 2
    tail, head = refs[-2:]
    for d in range(parts):

        @pl.when(pos[0] == d)
        def _():
            tail[...] = refs[d][...]

        @pl.when(pos[1] == d)
        def _():
            head[...] = refs[parts + d][...]


def pick(arrays, tail_of, head_of, dim):
    size = arrays[0].shape[dim]
    specs, shapes, outs = [], [], []
    for n, at in ((UP, size // UP - 1), (DOWN, 0)):
        shape = arrays[0].shape[:dim] + (n,) + arrays[0].shape[dim + 1 :]
        where = tuple(at if i == dim else 0 for i in range(len(shape)))
        specs += [pl.BlockSpec(shape, lambda i, p, where=where: where)] * len(arrays)
        shapes.append(jax.ShapeDtypeStruct(shape, BF))
        outs.append(pl.BlockSpec(shape, lambda i, p, n=len(shape): (0,) * n))
    return pl.pallas_call(
        pick_kernel,
        grid_spec=pltpu.PrefetchScalarGridSpec(num_scalar_prefetch=1, grid=(1,), in_specs=specs, out_specs=outs),
        out_shape=shapes,
        compiler_params=limit(3),
    )(jnp.stack([tail_of, head_of]).astype(jnp.int32), *arrays, *arrays)


def conv_scratch(tr, pitch, lidar, joined, block, pairs):
    return [
        pltpu.VMEM((tr + 6, pitch, lidar), BF),
        pltpu.VMEM((tr + 6, pitch, 2 * lidar), BF),
        pltpu.VMEM(((tr + 4) // 2, 2, pitch, 3 * joined), BF),
        pltpu.VMEM((pairs, 2, pitch, block), jnp.float32),
        pltpu.VMEM((pitch, joined), jnp.float32),
    ]


def conv_kernel(pos, *refs, parts, sh, tr, pitch, rows, cols, at, out_at, many):
    windows = refs[:parts]
    above, below, camera, w1, b1, w2, b2 = refs[parts : parts + 7]
    outs = refs[-5 - HALVES : -5]
    tile, taps, mid, cells, inside = refs[-5:]
    group, member, half_id, column = pos[0], pos[1], pos[2], pos[3]
    wide = windows[0].shape[2]
    lidar = windows[0].shape[3]
    joined = w1.shape[1]
    block = w2.shape[1] // 2
    col0 = column * (wide - 2 * SIDE) - SIDE

    edge_cols = pitch - wide
    tile[:, wide:, :] = jnp.zeros((tr + 6, edge_cols, lidar), BF)
    tile[tr + UP + DOWN :, 0:wide, :] = jnp.zeros((tr + 6 - tr - UP - DOWN, wide, lidar), BF)
    col = lax.broadcasted_iota(jnp.int32, inside.shape, 0) + col0
    inside[...] = jnp.where((col >= 0) & (col < cols), 1.0, 0.0)

    def frame(f, _):
        tile[0:UP, 0:wide, :] = above[at + f]
        for d in range(parts):
            source = lax.rem(member - d + parts, parts)
            tile[pl.ds(UP + source * sh, sh), 0:wide, :] = windows[d][at + f]
        tile[UP + tr : UP + tr + DOWN, 0:wide, :] = below[at + f]

        step = 6
        flat = step * pitch

        def shift(i, _):
            r = i * step
            x = tile[pl.ds(r, step)].reshape(flat, lidar).astype(jnp.float32)
            taps[pl.ds(r, step), :, 0:lidar] = pltpu.roll(x, 1, 0).astype(BF).reshape(step, pitch, lidar)
            taps[pl.ds(r, step), :, lidar:] = pltpu.roll(x, flat - 1, 0).astype(BF).reshape(step, pitch, lidar)
            return 0

        lax.fori_loop(0, (tr + 6) // step, shift, 0)

        n1 = (tr + 4) // 2
        m1 = n1 * pitch

        def first(i, _):
            r = i * n1
            lhs = []
            for dy in range(3):
                lhs.append(tile[pl.ds(r + dy, n1)].reshape(m1, lidar))
                lhs.append(taps[pl.ds(r + dy, n1)].reshape(m1, 2 * lidar))
                lhs.append(camera[at + f, pl.ds(r + dy, n1)].reshape(m1, camera.shape[3]))
            acc = jnp.dot(jnp.concatenate(lhs, axis=1), w1[...], preferred_element_type=jnp.float32)
            v = jnp.maximum(acc + b1[...], 0.0).reshape(n1, pitch, joined)
            kept = []
            for y in range(n1):
                row = group * tr - 2 + r + y
                kept.append(v[y] * (inside[...] * jnp.where((row >= 0) & (row < rows), 1.0, 0.0)))
            v = jnp.concatenate(kept, axis=0)
            shape = (n1 // 2, 2, pitch, joined)
            p = pl.ds(i * (n1 // 2), n1 // 2)
            mid[p, :, :, 0:joined] = pltpu.roll(v, 1, 0).astype(BF).reshape(shape)
            mid[p, :, :, joined : 2 * joined] = v.astype(BF).reshape(shape)
            mid[p, :, :, 2 * joined :] = pltpu.roll(v, m1 - 1, 0).astype(BF).reshape(shape)
            return 0

        lax.fori_loop(0, (tr + 4) // n1, first, 0)

        n2 = (tr + 2) // 2
        m2 = n2 * pitch
        lhs = [mid[i // 2 : i // 2 + n2, i % 2].reshape(m2, 3 * joined) for i in range(4)]
        acc = jnp.dot(jnp.concatenate(lhs, axis=1), w2[...], preferred_element_type=jnp.float32)
        v = pltpu.roll(jnp.maximum(acc + b2[...], 0.0), SIDE, 0)
        cells[:, 0] = v[:, :block].reshape(n2, pitch, block)
        cells[:, 1] = v[:, block:].reshape(n2, pitch, block)
        pairs = tr // 2
        w = (wide - 2 * SIDE) // HALVES
        for sub in range(HALVES):
            c = 2 * SIDE + sub * w
            even = cells[0:pairs, 1, c : c + w, :].astype(BF)
            odd = cells[1 : pairs + 1, 0, c : c + w, :].astype(BF)
            top = jnp.where(group > 0, cells[0, 0, c : c + w, :], 0.0)
            corner = jnp.broadcast_to(cells[pairs, 0, c - 1 : c, :], (w, block))
            beside = cells[0:pairs, :, c - 1, :].reshape(tr, block)
            if sub == 0:
                corner = jnp.where(column > 0, corner, 0.0)
                beside = jnp.where(column > 0, beside, 0.0)
            row = lax.broadcasted_iota(jnp.int32, beside.shape, 0)
            beside = jnp.where((row == 0) & (group == 0), 0.0, beside)
            edge = jnp.where(half_id == 0, top, corner).astype(BF)
            beside = beside.astype(BF)
            for h in range(HALVES):

                @pl.when(lax.rem(half_id + h, HALVES) == sub)
                def _():
                    outs[h][out_at + f, 0:pairs, 0] = even
                    outs[h][out_at + f, 0:pairs, 1] = odd
                    outs[h][out_at + f, pairs, 0] = edge
                    outs[h][out_at + f, pairs, 1] = beside
        return 0

    if many == 1:
        frame(0, 0)
    else:
        lax.fori_loop(0, many, frame, 0)


def encode_kernel(pos, *refs, parts, half_rows, w):
    pieces = refs[:parts]
    w3, b3, wp, bp = refs[parts : parts + 4]
    out, grid, grown = refs[-3:]
    me = pos[0]
    block = pieces[0].shape[4]
    for h in range(parts):
        part = lax.rem(me - h + parts, parts)
        base = part * half_rows
        x = pieces[h]
        grid[pl.ds(base, half_rows), 1, 1 : w + 1, :] = x[0, 0:half_rows, 0].astype(jnp.float32)
        grid[pl.ds(base + 1, half_rows), 0, 1 : w + 1, :] = x[0, 0:half_rows, 1].astype(jnp.float32)
        beside = x[0, half_rows, 1].astype(jnp.float32)
        for r in range(2 * half_rows):
            grid[base + r // 2, r % 2, 0:1, :] = beside[r : r + 1]
        edge = x[0, half_rows, 0].astype(jnp.float32)

        @pl.when(part == 0)
        def _():
            grid[0, 0, 1 : w + 1, :] = edge

        @pl.when(part == parts - 1)
        def _():
            grid[parts * half_rows, 0, 0:1, :] = edge[0:1]

    n = parts * half_rows
    jd = rounded(w // 2, 8)
    m = n * jd
    lhs = []
    for a in range(3):
        for b in range(3):
            x = grid[pl.ds(a // 2, n), a % 2, pl.ds(b, jd, stride=2), :]
            lhs.append(x.reshape(m, block).astype(BF))
    deep = jnp.dot(jnp.concatenate(lhs, axis=1), w3[...], preferred_element_type=jnp.float32)
    deep = jnp.maximum(deep + b3[...], 0.0).astype(BF)
    branch = jnp.dot(deep, wp[...], preferred_element_type=jnp.float32)
    branch = jnp.maximum(branch + bp[...], 0.0).astype(BF).astype(jnp.float32).reshape(n, jd, wp.shape[1])
    grown[:, pl.ds(0, jd, stride=2), :] = branch
    grown[:, pl.ds(1, jd, stride=2), :] = branch
    up = grown[:, 0:w, :].astype(BF)
    out[0, :, 0, :, 0:block] = grid[0:n, 1, 1 : w + 1, :].astype(BF)
    out[0, :, 1, :, 0:block] = grid[1 : n + 1, 0, 1 : w + 1, :].astype(BF)
    out[0, :, 0, :, block:] = up
    out[0, :, 1, :, block:] = up


def solution(mesh):
    n_rows, n_cols = mesh.shape["rows"], mesh.shape["cols"]
    members = n_cols // HALVES
    groups = n_rows * HALVES
    total = n_rows * n_cols
    half = members // 2
    turn = 2 if members % 4 == 0 else 0

    tile_of = [[(2 * m if m < half else 2 * (members - 1 - m) + 1) ^ t for m in range(members)] for t in (0, turn)]
    holder = [[tiles.index(j) for j in range(members)] for tiles in tile_of]

    def seat(g, j):
        return g * members + holder[g // HALVES % 2][j]

    def local(lidar, camera, joined_weight, joined_bias, block_weight, block_bias, down_weight, down_bias, proj_weight, proj_bias):
        frames, sh, cols, lidar_ch = lidar.shape
        rows, sc, cam_ch = camera.shape[1:]
        tr = sh * members
        tw = cols // members
        wide = tw + 2 * SIDE
        pitch = rounded(wide, 16)
        w = cols // n_cols
        joined = joined_weight.shape[3]
        block = block_weight.shape[3]
        place = lax.axis_index(AXES)
        group = place // members
        member = place % members
        cindex = lax.axis_index("cols")
        kgroup = cindex // members

        def send(x, pairs):
            return lax.ppermute(x, AXES, pairs)

        def across(x, by_group, by_column):
            pairs = []
            for g in range(groups):
                for j in range(members):
                    if 0 <= g + by_group < groups and 0 <= j + by_column < members:
                        pairs.append((seat(g, j), seat(g + by_group, j + by_column)))
            return send(x, pairs)

        def column_of(m):
            return jnp.where(m < half, 2 * m, 2 * (members - 1 - m) + 1) ^ (turn * (group // HALVES % 2))

        joint = joined_weight.reshape(-1, joined)
        square = block_weight.reshape(-1, block)
        deep1 = 3 * (3 * lidar_ch + rounded(3 * cam_ch, 256))
        w1, w2 = pl.pallas_call(
            lambda *refs: weights_kernel(*refs, lidar=lidar_ch, camera=cam_ch),
            out_shape=[
                jax.ShapeDtypeStruct((deep1, joined), BF),
                jax.ShapeDtypeStruct((4 * 3 * joined, 2 * block), BF),
            ],
            compiler_params=limit(14),
            name="weights",
        )(joint, square)
        w3 = down_weight.reshape(-1, down_weight.shape[3])
        b1 = joined_bias.reshape(1, -1)
        b2 = jnp.concatenate([block_bias, block_bias]).reshape(1, -1)
        b3 = down_bias.reshape(1, -1)
        bp = proj_bias.reshape(1, -1)

        span = rounded(tr + UP + DOWN, 8)
        lanes = frames * span
        turned = jnp.transpose(camera, (0, 2, 3, 1))
        strip = jax.ShapeDtypeStruct((sc, cam_ch, lanes), BF)
        rim = jax.ShapeDtypeStruct((UP, cam_ch, lanes), BF)
        packed = pl.pallas_call(
            lambda *refs: camera_pack_kernel(*refs, tr=tr, span=span),
            grid_spec=pltpu.PrefetchScalarGridSpec(
                num_scalar_prefetch=1,
                grid=(1,),
                in_specs=[whole(turned)],
                out_specs=[whole(strip)] * groups + [whole(rim)] * groups,
            ),
            out_shape=[strip] * groups + [rim] * groups,
            compiler_params=limit(14),
            name="camera_pack",
        )(place.reshape(1).astype(jnp.int32), turned)
        arrived = [send(packed[p], [(s, seat((s + p) % groups, s // groups)) for s in range(total)]) for p in range(groups)]
        for e in range(groups):
            pairs = [(groups * j + groups - 1, seat(e, j + 1)) for j in range(members - 1)]
            pairs += [(groups * j, seat((e + 1) % groups, j - 1)) for j in range(1, members)]
            arrived.append(send(packed[groups + e], pairs))
        cam = pl.pallas_call(
            lambda *refs: camera_unpack_kernel(*refs, groups=groups, sc=sc, cam_ch=cam_ch),
            grid_spec=pltpu.PrefetchScalarGridSpec(
                num_scalar_prefetch=1,
                grid=(1,),
                in_specs=[whole(x) for x in arrived],
                out_specs=pl.BlockSpec((lanes, pitch, rounded(3 * cam_ch, 256)), lambda i, p: (0, 0, 0)),
                scratch_shapes=[
                    pltpu.VMEM((tw + UP + DOWN, cam_ch, lanes), BF),
                    pltpu.VMEM((lanes, pitch, 128), jnp.float32),
                ],
            ),
            out_shape=jax.ShapeDtypeStruct((lanes, pitch, rounded(3 * cam_ch, 256)), BF),
            compiler_params=limit(16),
            name="camera_unpack",
        )(group.reshape(1).astype(jnp.int32), *arrived)
        cam = cam.reshape(frames, span, pitch, -1)

        pos = jnp.stack([group, member, kgroup, column_of(member)]).astype(jnp.int32)
        pairs2 = (tr + 2) // 2
        half_rows = tr // 2
        n = HALVES * half_rows
        jd = rounded(w // 2, 8)
        flops = 2 * pitch * ((tr + 4) * w1.shape[0] * joined + pairs2 * w2.shape[0] * 2 * block)
        framed = lambda a: pl.BlockSpec((1,) + a.shape[1:], lambda f, p: (f,) + (0,) * (a.ndim - 1))
        encoded = None
        step = frames // CHUNKS
        for f0 in range(0, frames, step):
            source = lidar if not f0 else lax.optimization_barrier((lidar, packed[0]))[0]
            window = jax.ShapeDtypeStruct((step, sh, wide, lidar_ch), BF)
            windows = pl.pallas_call(
                functools.partial(window_kernel, tw=tw),
                grid_spec=pltpu.PrefetchScalarGridSpec(
                    num_scalar_prefetch=1,
                    grid=(step,),
                    in_specs=[pl.BlockSpec((1, sh, cols, lidar_ch), lambda f, p, f0=f0: (f + f0, 0, 0, 0))],
                    out_specs=[framed(window)] * members,
                ),
                out_shape=[window] * members,
                compiler_params=limit(6),
                name="windows",
            )(jnp.stack([column_of((member + d) % members) for d in range(members)]).astype(jnp.int32), source)
            windows = [windows[0]] + [
                send(windows[d], [(g * members + m, g * members + (m + d) % members) for g in range(groups) for m in range(members)])
                for d in range(1, members)
            ]
            last, head = pick(windows, (member + 1) % members, member, 1)
            above = across(last, 1, 0)
            below = across(head, -1, 0)
            shifts = []
            for h in range(HALVES):
                shift = []
                for s in range(total):
                    r, c = divmod(s, n_cols)
                    k, m = divmod(c, members)
                    shift.append((s, r * n_cols + HALVES * tile_of[r % 2][m] + (k + h) % HALVES))
                shifts.append(shift)
            vmem = pl.BlockSpec(memory_space=pltpu.VMEM)
            batch = step // 2 if step % 2 == 0 else step
            for b0 in range(0, step, batch):
                blocks = jax.ShapeDtypeStruct((batch, pairs2, 2, w, block), BF)
                runs = [(0, batch)] if b0 == 0 else [(f, 1) for f in range(batch)]
                tiles = []
                for f1, many in runs:
                    tiles = pl.pallas_call(
                        functools.partial(conv_kernel, parts=members, sh=sh, tr=tr, pitch=pitch, rows=rows, cols=cols, at=b0 + f1, out_at=f1, many=many),
                        in_specs=[pl.BlockSpec(memory_space=pltpu.SMEM)] + [vmem] * (members + 7 + len(tiles)),
                        out_specs=[vmem] * HALVES,
                        scratch_shapes=conv_scratch(tr, pitch, lidar_ch, joined, block, pairs2),
                        out_shape=[blocks] * HALVES,
                        input_output_aliases={members + 8 + h: h for h in range(HALVES)} if tiles else {},
                        compiler_params=limit(20),
                        cost_estimate=pl.CostEstimate(flops=flops * many, bytes_accessed=2 * 10**6, transcendentals=0),
                    )(pos, *windows, above, below, cam, w1, b1, w2, b2, *tiles)
                pieces = []
                for h in range(HALVES):
                    pieces.append(send(tiles[h], shifts[h]))
                old = [] if encoded is None else [encoded]
                encoded = pl.pallas_call(
                    lambda *refs: encode_kernel(*refs, parts=HALVES, half_rows=half_rows, w=w),
                    grid_spec=pltpu.PrefetchScalarGridSpec(
                        num_scalar_prefetch=1,
                        grid=(batch,),
                        in_specs=[framed(x) for x in pieces] + [whole(x) for x in (w3, b3, proj_weight, bp)] + [pl.BlockSpec(memory_space=pl.ANY)] * len(old),
                        out_specs=pl.BlockSpec((1, n, 2, w, 2 * block), lambda f, p, lo=f0 + b0: (f + lo, 0, 0, 0, 0)),
                        scratch_shapes=[
                            pltpu.VMEM((n + 1, 2, rounded(w + 1, 8) + 16, block), jnp.float32),
                            pltpu.VMEM((n, 2 * jd, block), jnp.float32),
                        ],
                    ),
                    out_shape=jax.ShapeDtypeStruct((frames, n, 2, w, 2 * block), BF),
                    input_output_aliases={5 + HALVES: 0} if old else {},
                    compiler_params=limit(12),
                    cost_estimate=pl.CostEstimate(flops=2 * batch * n * jd * w3.shape[0] * 256, bytes_accessed=batch * 10**6, transcendentals=0),
                )(cindex.reshape(1).astype(jnp.int32), *pieces, w3, b3, proj_weight, bp, *old)
        return encoded.reshape(frames, 2 * n, w, 2 * block)

    return jax.shard_map(
        local,
        mesh=mesh,
        in_specs=(
            P("frames", AXES, None, None),
            P("frames", None, AXES, None),
            P(), P(), P(), P(), P(), P(), P(), P(),
        ),
        out_specs=P("frames", "rows", "cols", None),
        check_vma=False,
    )
```

```python
import functools

import jax
import jax.numpy as jnp
from jax import lax
from jax.experimental import pallas as pl
from jax.experimental.pallas import tpu as pltpu
from jax.sharding import PartitionSpec as P


AXES = ("rows", "cols")
CHUNKS = 2
HALVES = 2
SIDE = 4
UP, DOWN = 3, 2
BF = jnp.bfloat16


def rounded(n, to):
    return -(-n // to) * to


def limit(mib):
    return pltpu.CompilerParams(vmem_limit_bytes=mib * 2**20)


def whole(a):
    return pl.BlockSpec(a.shape, lambda *_: (0,) * a.ndim)


def weights_kernel(joint, square, w1, w2, *, lidar, camera):
    joined, block = joint.shape[1], square.shape[1]
    ch = lidar + camera
    deep = w1.shape[0] // 3
    for dy in range(3):
        base = dy * deep
        for dx in range(3):
            at = (dy * 3 + dx) * ch
            to = base + (1, 0, 2)[dx] * lidar
            w1[to : to + lidar, :] = joint[at : at + lidar, :]
            to = base + 3 * lidar + dx * camera
            w1[to : to + camera, :] = joint[at + lidar : at + ch, :]
        w1[base + 3 * ch : base + deep, :] = jnp.zeros((deep - 3 * ch, joined), BF)
    tall = square.shape[0]
    gap = w2.shape[0] - tall
    w2[0:tall, 0:block] = square[...]
    w2[tall:, 0:block] = jnp.zeros((gap, block), BF)
    w2[gap:, block:] = square[...]
    w2[0:gap, block:] = jnp.zeros((gap, block), BF)


def camera_pack_kernel(pos, x, *refs, tr, span):
    frames, sc, ch, rows = x.shape
    groups = len(refs) // 2
    outs, rims = refs[:groups], refs[groups:]
    width = frames * span
    place = pos[0]
    row = lax.broadcasted_iota(jnp.int32, (rows, width), 0)
    lane = lax.broadcasted_iota(jnp.int32, (rows, width), 1)

    def picks(f, targets):
        parts = []
        for target in targets:
            start = target * tr - UP
            parts.append(jnp.where(row + f * span == lane + start, jnp.where(lane // span == f, 1.0, 0.0), 0.0).astype(BF))
        return jnp.concatenate(parts, axis=1)

    main, rim = None, None
    rightmost = lax.rem(place, groups) == groups - 1
    for f in range(frames):
        pick = picks(f, [lax.rem(place + p, groups) for p in range(groups)])
        part = jnp.dot(x[f].reshape(sc * ch, rows), pick, preferred_element_type=jnp.float32)
        main = part if main is None else main + part
        pick = picks(f, [lax.rem(e + jnp.where(rightmost, 0, 1), groups) for e in range(groups)])
        border = jnp.where(rightmost, x[f, sc - UP : sc].astype(jnp.float32), x[f, 0:UP].astype(jnp.float32)).astype(BF)
        part = jnp.dot(border.reshape(UP * ch, rows), pick, preferred_element_type=jnp.float32)
        rim = part if rim is None else rim + part
    for p in range(groups):
        outs[p][...] = main[:, p * width : (p + 1) * width].astype(BF).reshape(sc, ch, width)
        rims[p][...] = rim[:, p * width : (p + 1) * width].astype(BF).reshape(UP, ch, width)


def window_kernel(pos, x, *outs, tw):
    n = x.shape[2] // tw
    wide = tw + 2 * SIDE
    edge = jnp.zeros((x.shape[1], SIDE, x.shape[3]), BF)
    for d in range(len(outs)):
        for c in range(n):

            @pl.when(pos[d] == c)
            def _():
                lo, hi = max(c * tw - SIDE, 0), min((c + 1) * tw + SIDE, n * tw)
                at = lo - (c * tw - SIDE)
                if at:
                    outs[d][0, :, 0:at, :] = edge
                if at + hi - lo < wide:
                    outs[d][0, :, at + hi - lo :, :] = edge
                outs[d][0, :, at : at + hi - lo, :] = x[0, :, lo:hi, :]


def camera_unpack_kernel(pos, *refs, groups, sc, cam_ch):
    strips, rims = refs[:groups], refs[groups : 2 * groups]
    out, stage, cells = refs[2 * groups :]
    group = pos[0]
    lanes = stage.shape[2]
    pitch = cells.shape[1]
    for p in range(groups):
        q = lax.rem(group - p + groups, groups)
        stage[pl.ds(UP + q * sc, sc)] = strips[p][...]
    n = UP + groups * sc + DOWN
    for e in range(groups):

        @pl.when(group == e)
        def _():
            stage[0:UP] = rims[e][...]

        @pl.when(group == (e + 1) % groups)
        def _():
            stage[n - DOWN : n] = rims[e][0:DOWN]

    lead = SIDE - UP
    cells[:, 0:8, :] = jnp.zeros((lanes, 8, 128), jnp.float32)
    low = (lead + n) // 8 * 8
    cells[:, low:, :] = jnp.zeros((lanes, pitch - low, 128), jnp.float32)
    for c in range(n):
        x = stage[c].astype(jnp.float32)
        x = jnp.concatenate([x, jnp.zeros((128 - cam_ch, lanes), jnp.float32)], axis=0)
        cells[:, lead + c, :] = x.T
    step = 8
    flat = step * pitch
    lane = lax.broadcasted_iota(jnp.int32, (flat, 128), 1)

    def widen(i, _):
        x = cells[pl.ds(i * step, step)].reshape(flat, 128)
        taps = [pltpu.roll(x, 1, 0), x, pltpu.roll(x, flat - 1, 0)]
        for v in range(out.shape[2] // 128):
            y = jnp.zeros((flat, 128), jnp.float32)
            for t in range(3):
                lo, hi = t * cam_ch - v * 128, (t + 1) * cam_ch - v * 128
                if hi > 0 and lo < 128:
                    turned = pltpu.roll(taps[t], lo % 128, 1) if lo % 128 else taps[t]
                    y = jnp.where((lane >= lo) & (lane < hi), turned, y)
            out[pl.ds(i * step, step), :, v * 128 : (v + 1) * 128] = y.astype(BF).reshape(step, pitch, 128)
        return 0

    lax.fori_loop(0, lanes // step, widen, 0)


def pick_kernel(pos, *refs):
    parts = (len(refs) - 2) // 2
    tail, head = refs[-2:]
    for d in range(parts):

        @pl.when(pos[0] == d)
        def _():
            tail[...] = refs[d][...]

        @pl.when(pos[1] == d)
        def _():
            head[...] = refs[parts + d][...]


def pick(arrays, tail_of, head_of, dim):
    size = arrays[0].shape[dim]
    specs, shapes, outs = [], [], []
    for n, at in ((UP, size // UP - 1), (DOWN, 0)):
        shape = arrays[0].shape[:dim] + (n,) + arrays[0].shape[dim + 1 :]
        where = tuple(at if i == dim else 0 for i in range(len(shape)))
        specs += [pl.BlockSpec(shape, lambda i, p, where=where: where)] * len(arrays)
        shapes.append(jax.ShapeDtypeStruct(shape, BF))
        outs.append(pl.BlockSpec(shape, lambda i, p, n=len(shape): (0,) * n))
    return pl.pallas_call(
        pick_kernel,
        grid_spec=pltpu.PrefetchScalarGridSpec(num_scalar_prefetch=1, grid=(1,), in_specs=specs, out_specs=outs),
        out_shape=shapes,
        compiler_params=limit(3),
    )(jnp.stack([tail_of, head_of]).astype(jnp.int32), *arrays, *arrays)


def conv_scratch(tr, pitch, lidar, joined, block, pairs):
    return [
        pltpu.VMEM((tr + 6, pitch, lidar), BF),
        pltpu.VMEM((tr + 6, pitch, 2 * lidar), BF),
        pltpu.VMEM(((tr + 4) // 2, 2, pitch, 3 * joined), BF),
        pltpu.VMEM((pairs, 2, pitch, block), jnp.float32),
        pltpu.VMEM((pitch, joined), jnp.float32),
    ]


def conv_kernel(pos, *refs, parts, sh, tr, pitch, rows, cols, at, cam_at, out_at, many):
    windows = refs[:parts]
    above, below, camera, w1, b1, w2, b2 = refs[parts : parts + 7]
    outs = refs[-5 - HALVES : -5]
    tile, taps, mid, cells, inside = refs[-5:]
    group, member, half_id, column = pos[0], pos[1], pos[2], pos[3]
    wide = windows[0].shape[2]
    lidar = windows[0].shape[3]
    joined = w1.shape[1]
    block = w2.shape[1] // 2
    col0 = column * (wide - 2 * SIDE) - SIDE

    edge_cols = pitch - wide
    tile[:, wide:, :] = jnp.zeros((tr + 6, edge_cols, lidar), BF)
    tile[tr + UP + DOWN :, 0:wide, :] = jnp.zeros((tr + 6 - tr - UP - DOWN, wide, lidar), BF)
    col = lax.broadcasted_iota(jnp.int32, inside.shape, 0) + col0
    inside[...] = jnp.where((col >= 0) & (col < cols), 1.0, 0.0)

    def frame(f, _):
        tile[0:UP, 0:wide, :] = above[at + f]
        for d in range(parts):
            source = lax.rem(member - d + parts, parts)
            tile[pl.ds(UP + source * sh, sh), 0:wide, :] = windows[d][at + f]
        tile[UP + tr : UP + tr + DOWN, 0:wide, :] = below[at + f]

        step = 6
        flat = step * pitch

        def shift(i, _):
            r = i * step
            x = tile[pl.ds(r, step)].reshape(flat, lidar).astype(jnp.float32)
            taps[pl.ds(r, step), :, 0:lidar] = pltpu.roll(x, 1, 0).astype(BF).reshape(step, pitch, lidar)
            taps[pl.ds(r, step), :, lidar:] = pltpu.roll(x, flat - 1, 0).astype(BF).reshape(step, pitch, lidar)
            return 0

        lax.fori_loop(0, (tr + 6) // step, shift, 0)

        n1 = (tr + 4) // 2
        m1 = n1 * pitch

        def first(i, _):
            r = i * n1
            lhs = []
            for dy in range(3):
                lhs.append(tile[pl.ds(r + dy, n1)].reshape(m1, lidar))
                lhs.append(taps[pl.ds(r + dy, n1)].reshape(m1, 2 * lidar))
                lhs.append(camera[cam_at + f, pl.ds(r + dy, n1)].reshape(m1, camera.shape[3]))
            acc = jnp.dot(jnp.concatenate(lhs, axis=1), w1[...], preferred_element_type=jnp.float32)
            v = jnp.maximum(acc + b1[...], 0.0).reshape(n1, pitch, joined)
            kept = []
            for y in range(n1):
                row = group * tr - 2 + r + y
                kept.append(v[y] * (inside[...] * jnp.where((row >= 0) & (row < rows), 1.0, 0.0)))
            v = jnp.concatenate(kept, axis=0)
            shape = (n1 // 2, 2, pitch, joined)
            p = pl.ds(i * (n1 // 2), n1 // 2)
            mid[p, :, :, 0:joined] = pltpu.roll(v, 1, 0).astype(BF).reshape(shape)
            mid[p, :, :, joined : 2 * joined] = v.astype(BF).reshape(shape)
            mid[p, :, :, 2 * joined :] = pltpu.roll(v, m1 - 1, 0).astype(BF).reshape(shape)
            return 0

        lax.fori_loop(0, (tr + 4) // n1, first, 0)

        n2 = (tr + 2) // 2
        m2 = n2 * pitch
        lhs = [mid[i // 2 : i // 2 + n2, i % 2].reshape(m2, 3 * joined) for i in range(4)]
        acc = jnp.dot(jnp.concatenate(lhs, axis=1), w2[...], preferred_element_type=jnp.float32)
        v = pltpu.roll(jnp.maximum(acc + b2[...], 0.0), SIDE, 0)
        cells[:, 0] = v[:, :block].reshape(n2, pitch, block)
        cells[:, 1] = v[:, block:].reshape(n2, pitch, block)
        pairs = tr // 2
        w = (wide - 2 * SIDE) // HALVES
        for sub in range(HALVES):
            c = 2 * SIDE + sub * w
            even = cells[0:pairs, 1, c : c + w, :].astype(BF)
            odd = cells[1 : pairs + 1, 0, c : c + w, :].astype(BF)
            top = jnp.where(group > 0, cells[0, 0, c : c + w, :], 0.0)
            corner = jnp.broadcast_to(cells[pairs, 0, c - 1 : c, :], (w, block))
            beside = cells[0:pairs, :, c - 1, :].reshape(tr, block)
            if sub == 0:
                corner = jnp.where(column > 0, corner, 0.0)
                beside = jnp.where(column > 0, beside, 0.0)
            row = lax.broadcasted_iota(jnp.int32, beside.shape, 0)
            beside = jnp.where((row == 0) & (group == 0), 0.0, beside)
            edge = jnp.where(half_id == 0, top, corner).astype(BF)
            beside = beside.astype(BF)
            for h in range(HALVES):

                @pl.when(lax.rem(half_id + h, HALVES) == sub)
                def _():
                    outs[h][out_at + f, 0:pairs, 0] = even
                    outs[h][out_at + f, 0:pairs, 1] = odd
                    outs[h][out_at + f, pairs, 0] = edge
                    outs[h][out_at + f, pairs, 1] = beside
        return 0

    if many == 1:
        frame(0, 0)
    else:
        lax.fori_loop(0, many, frame, 0)


def encode_kernel(pos, *refs, parts, half_rows, w):
    pieces = refs[:parts]
    w3, b3, wp, bp = refs[parts : parts + 4]
    out, grid, grown = refs[-3:]
    me = pos[0]
    block = pieces[0].shape[4]
    for h in range(parts):
        part = lax.rem(me - h + parts, parts)
        base = part * half_rows
        x = pieces[h]
        grid[pl.ds(base, half_rows), 1, 1 : w + 1, :] = x[0, 0:half_rows, 0].astype(jnp.float32)
        grid[pl.ds(base + 1, half_rows), 0, 1 : w + 1, :] = x[0, 0:half_rows, 1].astype(jnp.float32)
        beside = x[0, half_rows, 1].astype(jnp.float32)
        for r in range(2 * half_rows):
            grid[base + r // 2, r % 2, 0:1, :] = beside[r : r + 1]
        edge = x[0, half_rows, 0].astype(jnp.float32)

        @pl.when(part == 0)
        def _():
            grid[0, 0, 1 : w + 1, :] = edge

        @pl.when(part == parts - 1)
        def _():
            grid[parts * half_rows, 0, 0:1, :] = edge[0:1]

    n = parts * half_rows
    jd = rounded(w // 2, 8)
    m = n * jd
    lhs = []
    for a in range(3):
        for b in range(3):
            x = grid[pl.ds(a // 2, n), a % 2, pl.ds(b, jd, stride=2), :]
            lhs.append(x.reshape(m, block).astype(BF))
    deep = jnp.dot(jnp.concatenate(lhs, axis=1), w3[...], preferred_element_type=jnp.float32)
    deep = jnp.maximum(deep + b3[...], 0.0).astype(BF)
    branch = jnp.dot(deep, wp[...], preferred_element_type=jnp.float32)
    branch = jnp.maximum(branch + bp[...], 0.0).astype(BF).astype(jnp.float32).reshape(n, jd, wp.shape[1])
    grown[:, pl.ds(0, jd, stride=2), :] = branch
    grown[:, pl.ds(1, jd, stride=2), :] = branch
    up = grown[:, 0:w, :].astype(BF)
    out[0, :, 0, :, 0:block] = grid[0:n, 1, 1 : w + 1, :].astype(BF)
    out[0, :, 1, :, 0:block] = grid[1 : n + 1, 0, 1 : w + 1, :].astype(BF)
    out[0, :, 0, :, block:] = up
    out[0, :, 1, :, block:] = up


def solution(mesh):
    n_rows, n_cols = mesh.shape["rows"], mesh.shape["cols"]
    members = n_cols // HALVES
    groups = n_rows * HALVES
    total = n_rows * n_cols
    half = members // 2
    turn = 2 if members % 4 == 0 else 0

    tile_of = [[(2 * m if m < half else 2 * (members - 1 - m) + 1) ^ t for m in range(members)] for t in (0, turn)]
    holder = [[tiles.index(j) for j in range(members)] for tiles in tile_of]

    def seat(g, j):
        return g * members + holder[g // HALVES % 2][j]

    def local(lidar, camera, joined_weight, joined_bias, block_weight, block_bias, down_weight, down_bias, proj_weight, proj_bias):
        frames, sh, cols, lidar_ch = lidar.shape
        rows, sc, cam_ch = camera.shape[1:]
        tr = sh * members
        tw = cols // members
        wide = tw + 2 * SIDE
        pitch = rounded(wide, 16)
        w = cols // n_cols
        joined = joined_weight.shape[3]
        block = block_weight.shape[3]
        place = lax.axis_index(AXES)
        group = place // members
        member = place % members
        cindex = lax.axis_index("cols")
        kgroup = cindex // members

        def send(x, pairs):
            return lax.ppermute(x, AXES, pairs)

        def across(x, by_group, by_column):
            pairs = []
            for g in range(groups):
                for j in range(members):
                    if 0 <= g + by_group < groups and 0 <= j + by_column < members:
                        pairs.append((seat(g, j), seat(g + by_group, j + by_column)))
            return send(x, pairs)

        def column_of(m):
            return jnp.where(m < half, 2 * m, 2 * (members - 1 - m) + 1) ^ (turn * (group // HALVES % 2))

        joint = joined_weight.reshape(-1, joined)
        square = block_weight.reshape(-1, block)
        deep1 = 3 * (3 * lidar_ch + rounded(3 * cam_ch, 256))
        w1, w2 = pl.pallas_call(
            lambda *refs: weights_kernel(*refs, lidar=lidar_ch, camera=cam_ch),
            out_shape=[
                jax.ShapeDtypeStruct((deep1, joined), BF),
                jax.ShapeDtypeStruct((4 * 3 * joined, 2 * block), BF),
            ],
            compiler_params=limit(14),
            name="weights",
        )(joint, square)
        w3 = down_weight.reshape(-1, down_weight.shape[3])
        b1 = joined_bias.reshape(1, -1)
        b2 = jnp.concatenate([block_bias, block_bias]).reshape(1, -1)
        b3 = down_bias.reshape(1, -1)
        bp = proj_bias.reshape(1, -1)

        span = rounded(tr + UP + DOWN, 8)
        lanes = frames * span
        turned = jnp.transpose(camera, (0, 2, 3, 1))
        strip = jax.ShapeDtypeStruct((sc, cam_ch, lanes), BF)
        rim = jax.ShapeDtypeStruct((UP, cam_ch, lanes), BF)
        packed = pl.pallas_call(
            lambda *refs: camera_pack_kernel(*refs, tr=tr, span=span),
            grid_spec=pltpu.PrefetchScalarGridSpec(
                num_scalar_prefetch=1,
                grid=(1,),
                in_specs=[whole(turned)],
                out_specs=[whole(strip)] * groups + [whole(rim)] * groups,
            ),
            out_shape=[strip] * groups + [rim] * groups,
            compiler_params=limit(14),
            name="camera_pack",
        )(place.reshape(1).astype(jnp.int32), turned)
        arrived = [send(packed[p], [(s, seat((s + p) % groups, s // groups)) for s in range(total)]) for p in range(groups)]
        for e in range(groups):
            pairs = [(groups * j + groups - 1, seat(e, j + 1)) for j in range(members - 1)]
            pairs += [(groups * j, seat((e + 1) % groups, j - 1)) for j in range(1, members)]
            arrived.append(send(packed[groups + e], pairs))
        cam = pl.pallas_call(
            lambda *refs: camera_unpack_kernel(*refs, groups=groups, sc=sc, cam_ch=cam_ch),
            grid_spec=pltpu.PrefetchScalarGridSpec(
                num_scalar_prefetch=1,
                grid=(1,),
                in_specs=[whole(x) for x in arrived],
                out_specs=pl.BlockSpec((lanes, pitch, rounded(3 * cam_ch, 256)), lambda i, p: (0, 0, 0)),
                scratch_shapes=[
                    pltpu.VMEM((tw + UP + DOWN, cam_ch, lanes), BF),
                    pltpu.VMEM((lanes, pitch, 128), jnp.float32),
                ],
            ),
            out_shape=jax.ShapeDtypeStruct((lanes, pitch, rounded(3 * cam_ch, 256)), BF),
            compiler_params=limit(16),
            name="camera_unpack",
        )(group.reshape(1).astype(jnp.int32), *arrived)
        cam = cam.reshape(frames, span, pitch, -1)

        pos = jnp.stack([group, member, kgroup, column_of(member)]).astype(jnp.int32)
        pairs2 = (tr + 2) // 2
        half_rows = tr // 2
        n = HALVES * half_rows
        jd = rounded(w // 2, 8)
        flops = 2 * pitch * ((tr + 4) * w1.shape[0] * joined + pairs2 * w2.shape[0] * 2 * block)
        framed = lambda a: pl.BlockSpec((1,) + a.shape[1:], lambda f, p: (f,) + (0,) * (a.ndim - 1))
        encoded = None
        step = frames // CHUNKS
        for f0 in range(0, frames, step):
            source = lidar if not f0 else lax.optimization_barrier((lidar, packed[0]))[0]
            window = jax.ShapeDtypeStruct((step, sh, wide, lidar_ch), BF)
            windows = pl.pallas_call(
                functools.partial(window_kernel, tw=tw),
                grid_spec=pltpu.PrefetchScalarGridSpec(
                    num_scalar_prefetch=1,
                    grid=(step,),
                    in_specs=[pl.BlockSpec((1, sh, cols, lidar_ch), lambda f, p, f0=f0: (f + f0, 0, 0, 0))],
                    out_specs=[framed(window)] * members,
                ),
                out_shape=[window] * members,
                compiler_params=limit(6),
            )(jnp.stack([column_of((member + d) % members) for d in range(members)]).astype(jnp.int32), source)
            windows = [windows[0]] + [
                send(windows[d], [(g * members + m, g * members + (m + d) % members) for g in range(groups) for m in range(members)])
                for d in range(1, members)
            ]
            last, head = pick(windows, (member + 1) % members, member, 1)
            above = across(last, 1, 0)
            below = across(head, -1, 0)
            shifts = []
            for h in range(HALVES):
                shift = []
                for s in range(total):
                    r, c = divmod(s, n_cols)
                    k, m = divmod(c, members)
                    shift.append((s, r * n_cols + HALVES * tile_of[r % 2][m] + (k + h) % HALVES))
                shifts.append(shift)
            vmem = pl.BlockSpec(memory_space=pltpu.VMEM)
            batch = step
            for b0 in range(0, step, batch):
                blocks = jax.ShapeDtypeStruct((batch, pairs2, 2, w, block), BF)
                runs = [(f, 1) for f in range(batch)]
                tiles = []
                for f1, many in runs:
                    tiles = pl.pallas_call(
                        functools.partial(conv_kernel, parts=members, sh=sh, tr=tr, pitch=pitch, rows=rows, cols=cols, at=b0 + f1, cam_at=f0 + b0 + f1, out_at=f1, many=many),
                        in_specs=[pl.BlockSpec(memory_space=pltpu.SMEM)] + [vmem] * (members + 7 + len(tiles)),
                        out_specs=[vmem] * HALVES,
                        scratch_shapes=conv_scratch(tr, pitch, lidar_ch, joined, block, pairs2),
                        out_shape=[blocks] * HALVES,
                        input_output_aliases={members + 8 + h: h for h in range(HALVES)} if tiles else {},
                        compiler_params=limit(20),
                        cost_estimate=pl.CostEstimate(flops=flops * many, bytes_accessed=2 * 10**6, transcendentals=0),
                    )(pos, *windows, above, below, cam, w1, b1, w2, b2, *tiles)
                pieces = []
                for h in range(HALVES):
                    pieces.append(send(tiles[h], shifts[h]))
                old = [] if encoded is None else [encoded]
                encoded = pl.pallas_call(
                    lambda *refs: encode_kernel(*refs, parts=HALVES, half_rows=half_rows, w=w),
                    grid_spec=pltpu.PrefetchScalarGridSpec(
                        num_scalar_prefetch=1,
                        grid=(batch,),
                        in_specs=[framed(x) for x in pieces] + [whole(x) for x in (w3, b3, proj_weight, bp)] + [pl.BlockSpec(memory_space=pl.ANY)] * len(old),
                        out_specs=pl.BlockSpec((1, n, 2, w, 2 * block), lambda f, p, lo=f0 + b0: (f + lo, 0, 0, 0, 0)),
                        scratch_shapes=[
                            pltpu.VMEM((n + 1, 2, rounded(w + 1, 8) + 16, block), jnp.float32),
                            pltpu.VMEM((n, 2 * jd, block), jnp.float32),
                        ],
                    ),
                    out_shape=jax.ShapeDtypeStruct((frames, n, 2, w, 2 * block), BF),
                    input_output_aliases={5 + HALVES: 0} if old else {},
                    compiler_params=limit(12),
                    cost_estimate=pl.CostEstimate(flops=2 * batch * n * jd * w3.shape[0] * 256, bytes_accessed=batch * 10**6, transcendentals=0),
                )(cindex.reshape(1).astype(jnp.int32), *pieces, w3, b3, proj_weight, bp, *old)
        return encoded.reshape(frames, 2 * n, w, 2 * block)

    return jax.shard_map(
        local,
        mesh=mesh,
        in_specs=(
            P("frames", AXES, None, None),
            P("frames", None, AXES, None),
            P(), P(), P(), P(), P(), P(), P(), P(),
        ),
        out_specs=P("frames", "rows", "cols", None),
        check_vma=False,
    )
```

```python
import functools

import jax
import jax.numpy as jnp
from jax import lax
from jax.experimental import pallas as pl
from jax.experimental.pallas import tpu as pltpu
from jax.sharding import PartitionSpec as P


AXES = ("rows", "cols")
CHUNKS = 1
HALVES = 2
SIDE = 4
UP, DOWN = 3, 2
BF = jnp.bfloat16


def rounded(n, to):
    return -(-n // to) * to


def limit(mib):
    return pltpu.CompilerParams(vmem_limit_bytes=mib * 2**20)


def whole(a):
    return pl.BlockSpec(a.shape, lambda *_: (0,) * a.ndim)


def weights_kernel(joint, square, w1, w2, *, lidar, camera):
    joined, block = joint.shape[1], square.shape[1]
    ch = lidar + camera
    deep = w1.shape[0] // 3
    for dy in range(3):
        base = dy * deep
        for dx in range(3):
            at = (dy * 3 + dx) * ch
            to = base + (1, 0, 2)[dx] * lidar
            w1[to : to + lidar, :] = joint[at : at + lidar, :]
            to = base + 3 * lidar + dx * camera
            w1[to : to + camera, :] = joint[at + lidar : at + ch, :]
        w1[base + 3 * ch : base + deep, :] = jnp.zeros((deep - 3 * ch, joined), BF)
    tall = square.shape[0]
    gap = w2.shape[0] - tall
    w2[0:tall, 0:block] = square[...]
    w2[tall:, 0:block] = jnp.zeros((gap, block), BF)
    w2[gap:, block:] = square[...]
    w2[0:gap, block:] = jnp.zeros((gap, block), BF)


def camera_pack_kernel(pos, x, *refs, tr, span):
    frames, sc, ch, rows = x.shape
    groups = len(refs) // 2
    outs, rims = refs[:groups], refs[groups:]
    width = frames * span
    place = pos[0]
    row = lax.broadcasted_iota(jnp.int32, (rows, width), 0)
    lane = lax.broadcasted_iota(jnp.int32, (rows, width), 1)

    def picks(f, targets):
        parts = []
        for target in targets:
            start = target * tr - UP
            parts.append(jnp.where(row + f * span == lane + start, jnp.where(lane // span == f, 1.0, 0.0), 0.0).astype(BF))
        return jnp.concatenate(parts, axis=1)

    main, rim = None, None
    rightmost = lax.rem(place, groups) == groups - 1
    for f in range(frames):
        pick = picks(f, [lax.rem(place + p, groups) for p in range(groups)])
        part = jnp.dot(x[f].reshape(sc * ch, rows), pick, preferred_element_type=jnp.float32)
        main = part if main is None else main + part
        pick = picks(f, [lax.rem(e + jnp.where(rightmost, 0, 1), groups) for e in range(groups)])
        border = jnp.where(rightmost, x[f, sc - UP : sc].astype(jnp.float32), x[f, 0:UP].astype(jnp.float32)).astype(BF)
        part = jnp.dot(border.reshape(UP * ch, rows), pick, preferred_element_type=jnp.float32)
        rim = part if rim is None else rim + part
    for p in range(groups):
        outs[p][...] = main[:, p * width : (p + 1) * width].astype(BF).reshape(sc, ch, width)
        rims[p][...] = rim[:, p * width : (p + 1) * width].astype(BF).reshape(UP, ch, width)


def window_kernel(pos, x, *outs, tw):
    n = x.shape[2] // tw
    wide = tw + 2 * SIDE
    edge = jnp.zeros((x.shape[1], SIDE, x.shape[3]), BF)
    for d in range(len(outs)):
        for c in range(n):

            @pl.when(pos[d] == c)
            def _():
                lo, hi = max(c * tw - SIDE, 0), min((c + 1) * tw + SIDE, n * tw)
                at = lo - (c * tw - SIDE)
                if at:
                    outs[d][0, :, 0:at, :] = edge
                if at + hi - lo < wide:
                    outs[d][0, :, at + hi - lo :, :] = edge
                outs[d][0, :, at : at + hi - lo, :] = x[0, :, lo:hi, :]


def camera_unpack_kernel(pos, *refs, groups, sc, cam_ch):
    strips, rims = refs[:groups], refs[groups : 2 * groups]
    out, stage, cells = refs[2 * groups :]
    group = pos[0]
    lanes = stage.shape[2]
    pitch = cells.shape[1]
    for p in range(groups):
        q = lax.rem(group - p + groups, groups)
        stage[pl.ds(UP + q * sc, sc)] = strips[p][...]
    n = UP + groups * sc + DOWN
    for e in range(groups):

        @pl.when(group == e)
        def _():
            stage[0:UP] = rims[e][...]

        @pl.when(group == (e + 1) % groups)
        def _():
            stage[n - DOWN : n] = rims[e][0:DOWN]

    lead = SIDE - UP
    cells[:, 0:8, :] = jnp.zeros((lanes, 8, 128), jnp.float32)
    low = (lead + n) // 8 * 8
    cells[:, low:, :] = jnp.zeros((lanes, pitch - low, 128), jnp.float32)
    for c in range(n):
        x = stage[c].astype(jnp.float32)
        x = jnp.concatenate([x, jnp.zeros((128 - cam_ch, lanes), jnp.float32)], axis=0)
        cells[:, lead + c, :] = x.T
    step = 8
    flat = step * pitch
    lane = lax.broadcasted_iota(jnp.int32, (flat, 128), 1)

    def widen(i, _):
        x = cells[pl.ds(i * step, step)].reshape(flat, 128)
        taps = [pltpu.roll(x, 1, 0), x, pltpu.roll(x, flat - 1, 0)]
        for v in range(out.shape[2] // 128):
            y = jnp.zeros((flat, 128), jnp.float32)
            for t in range(3):
                lo, hi = t * cam_ch - v * 128, (t + 1) * cam_ch - v * 128
                if hi > 0 and lo < 128:
                    turned = pltpu.roll(taps[t], lo % 128, 1) if lo % 128 else taps[t]
                    y = jnp.where((lane >= lo) & (lane < hi), turned, y)
            out[pl.ds(i * step, step), :, v * 128 : (v + 1) * 128] = y.astype(BF).reshape(step, pitch, 128)
        return 0

    lax.fori_loop(0, lanes // step, widen, 0)


def pick_kernel(pos, *refs):
    parts = (len(refs) - 2) // 2
    tail, head = refs[-2:]
    for d in range(parts):

        @pl.when(pos[0] == d)
        def _():
            tail[...] = refs[d][...]

        @pl.when(pos[1] == d)
        def _():
            head[...] = refs[parts + d][...]


def pick(arrays, tail_of, head_of, dim):
    size = arrays[0].shape[dim]
    specs, shapes, outs = [], [], []
    for n, at in ((UP, size // UP - 1), (DOWN, 0)):
        shape = arrays[0].shape[:dim] + (n,) + arrays[0].shape[dim + 1 :]
        where = tuple(at if i == dim else 0 for i in range(len(shape)))
        specs += [pl.BlockSpec(shape, lambda i, p, where=where: where)] * len(arrays)
        shapes.append(jax.ShapeDtypeStruct(shape, BF))
        outs.append(pl.BlockSpec(shape, lambda i, p, n=len(shape): (0,) * n))
    return pl.pallas_call(
        pick_kernel,
        grid_spec=pltpu.PrefetchScalarGridSpec(num_scalar_prefetch=1, grid=(1,), in_specs=specs, out_specs=outs),
        out_shape=shapes,
        compiler_params=limit(3),
    )(jnp.stack([tail_of, head_of]).astype(jnp.int32), *arrays, *arrays)


def conv_scratch(tr, pitch, lidar, joined, block, pairs):
    return [
        pltpu.VMEM((tr + 6, pitch, lidar), BF),
        pltpu.VMEM((tr + 6, pitch, 2 * lidar), BF),
        pltpu.VMEM(((tr + 4) // 2, 2, pitch, 3 * joined), BF),
        pltpu.VMEM((pairs, 2, pitch, block), jnp.float32),
        pltpu.VMEM((pitch, joined), jnp.float32),
    ]


def conv_kernel(pos, *refs, parts, sh, tr, pitch, rows, cols, at, cam_at, out_at, many):
    windows = refs[:parts]
    above, below, camera, w1, b1, w2, b2 = refs[parts : parts + 7]
    outs = refs[-5 - HALVES : -5]
    tile, taps, mid, cells, inside = refs[-5:]
    group, member, half_id, column = pos[0], pos[1], pos[2], pos[3]
    wide = windows[0].shape[2]
    lidar = windows[0].shape[3]
    joined = w1.shape[1]
    block = w2.shape[1] // 2
    col0 = column * (wide - 2 * SIDE) - SIDE

    edge_cols = pitch - wide
    tile[:, wide:, :] = jnp.zeros((tr + 6, edge_cols, lidar), BF)
    tile[tr + UP + DOWN :, 0:wide, :] = jnp.zeros((tr + 6 - tr - UP - DOWN, wide, lidar), BF)
    col = lax.broadcasted_iota(jnp.int32, inside.shape, 0) + col0
    inside[...] = jnp.where((col >= 0) & (col < cols), 1.0, 0.0)

    def frame(f, _):
        tile[0:UP, 0:wide, :] = above[out_at + f]
        for d in range(parts):
            source = lax.rem(member - d + parts, parts)
            tile[pl.ds(UP + source * sh, sh), 0:wide, :] = windows[d][at + f]
        tile[UP + tr : UP + tr + DOWN, 0:wide, :] = below[out_at + f]

        step = 6
        flat = step * pitch

        def shift(i, _):
            r = i * step
            x = tile[pl.ds(r, step)].reshape(flat, lidar).astype(jnp.float32)
            taps[pl.ds(r, step), :, 0:lidar] = pltpu.roll(x, 1, 0).astype(BF).reshape(step, pitch, lidar)
            taps[pl.ds(r, step), :, lidar:] = pltpu.roll(x, flat - 1, 0).astype(BF).reshape(step, pitch, lidar)
            return 0

        lax.fori_loop(0, (tr + 6) // step, shift, 0)

        n1 = (tr + 4) // 2
        m1 = n1 * pitch

        def first(i, _):
            r = i * n1
            lhs = []
            for dy in range(3):
                lhs.append(tile[pl.ds(r + dy, n1)].reshape(m1, lidar))
                lhs.append(taps[pl.ds(r + dy, n1)].reshape(m1, 2 * lidar))
                lhs.append(camera[cam_at + f, pl.ds(r + dy, n1)].reshape(m1, camera.shape[3]))
            acc = jnp.dot(jnp.concatenate(lhs, axis=1), w1[...], preferred_element_type=jnp.float32)
            v = jnp.maximum(acc + b1[...], 0.0).reshape(n1, pitch, joined)
            kept = []
            for y in range(n1):
                row = group * tr - 2 + r + y
                kept.append(v[y] * (inside[...] * jnp.where((row >= 0) & (row < rows), 1.0, 0.0)))
            v = jnp.concatenate(kept, axis=0)
            shape = (n1 // 2, 2, pitch, joined)
            p = pl.ds(i * (n1 // 2), n1 // 2)
            mid[p, :, :, 0:joined] = pltpu.roll(v, 1, 0).astype(BF).reshape(shape)
            mid[p, :, :, joined : 2 * joined] = v.astype(BF).reshape(shape)
            mid[p, :, :, 2 * joined :] = pltpu.roll(v, m1 - 1, 0).astype(BF).reshape(shape)
            return 0

        lax.fori_loop(0, (tr + 4) // n1, first, 0)

        n2 = (tr + 2) // 2
        m2 = n2 * pitch
        lhs = [mid[i // 2 : i // 2 + n2, i % 2].reshape(m2, 3 * joined) for i in range(4)]
        acc = jnp.dot(jnp.concatenate(lhs, axis=1), w2[...], preferred_element_type=jnp.float32)
        v = pltpu.roll(jnp.maximum(acc + b2[...], 0.0), SIDE, 0)
        cells[:, 0] = v[:, :block].reshape(n2, pitch, block)
        cells[:, 1] = v[:, block:].reshape(n2, pitch, block)
        pairs = tr // 2
        w = (wide - 2 * SIDE) // HALVES
        for sub in range(HALVES):
            c = 2 * SIDE + sub * w
            even = cells[0:pairs, 1, c : c + w, :].astype(BF)
            odd = cells[1 : pairs + 1, 0, c : c + w, :].astype(BF)
            top = jnp.where(group > 0, cells[0, 0, c : c + w, :], 0.0)
            corner = jnp.broadcast_to(cells[pairs, 0, c - 1 : c, :], (w, block))
            beside = cells[0:pairs, :, c - 1, :].reshape(tr, block)
            if sub == 0:
                corner = jnp.where(column > 0, corner, 0.0)
                beside = jnp.where(column > 0, beside, 0.0)
            row = lax.broadcasted_iota(jnp.int32, beside.shape, 0)
            beside = jnp.where((row == 0) & (group == 0), 0.0, beside)
            edge = jnp.where(half_id == 0, top, corner).astype(BF)
            beside = beside.astype(BF)
            for h in range(HALVES):

                @pl.when(lax.rem(half_id + h, HALVES) == sub)
                def _():
                    outs[h][out_at + f, 0:pairs, 0] = even
                    outs[h][out_at + f, 0:pairs, 1] = odd
                    outs[h][out_at + f, pairs, 0] = edge
                    outs[h][out_at + f, pairs, 1] = beside
        return 0

    if many == 1:
        frame(0, 0)
    else:
        lax.fori_loop(0, many, frame, 0)


def encode_kernel(pos, *refs, parts, half_rows, w):
    pieces = refs[:parts]
    w3, b3, wp, bp = refs[parts : parts + 4]
    out, grid, grown = refs[-3:]
    me = pos[0]
    block = pieces[0].shape[4]
    for h in range(parts):
        part = lax.rem(me - h + parts, parts)
        base = part * half_rows
        x = pieces[h]
        grid[pl.ds(base, half_rows), 1, 1 : w + 1, :] = x[0, 0:half_rows, 0].astype(jnp.float32)
        grid[pl.ds(base + 1, half_rows), 0, 1 : w + 1, :] = x[0, 0:half_rows, 1].astype(jnp.float32)
        beside = x[0, half_rows, 1].astype(jnp.float32)
        for r in range(2 * half_rows):
            grid[base + r // 2, r % 2, 0:1, :] = beside[r : r + 1]
        edge = x[0, half_rows, 0].astype(jnp.float32)

        @pl.when(part == 0)
        def _():
            grid[0, 0, 1 : w + 1, :] = edge

        @pl.when(part == parts - 1)
        def _():
            grid[parts * half_rows, 0, 0:1, :] = edge[0:1]

    n = parts * half_rows
    jd = rounded(w // 2, 8)
    m = n * jd
    lhs = []
    for a in range(3):
        for b in range(3):
            x = grid[pl.ds(a // 2, n), a % 2, pl.ds(b, jd, stride=2), :]
            lhs.append(x.reshape(m, block).astype(BF))
    deep = jnp.dot(jnp.concatenate(lhs, axis=1), w3[...], preferred_element_type=jnp.float32)
    deep = jnp.maximum(deep + b3[...], 0.0).astype(BF)
    branch = jnp.dot(deep, wp[...], preferred_element_type=jnp.float32)
    branch = jnp.maximum(branch + bp[...], 0.0).astype(BF).astype(jnp.float32).reshape(n, jd, wp.shape[1])
    grown[:, pl.ds(0, jd, stride=2), :] = branch
    grown[:, pl.ds(1, jd, stride=2), :] = branch
    up = grown[:, 0:w, :].astype(BF)
    out[0, :, 0, :, 0:block] = grid[0:n, 1, 1 : w + 1, :].astype(BF)
    out[0, :, 1, :, 0:block] = grid[1 : n + 1, 0, 1 : w + 1, :].astype(BF)
    out[0, :, 0, :, block:] = up
    out[0, :, 1, :, block:] = up


def solution(mesh):
    n_rows, n_cols = mesh.shape["rows"], mesh.shape["cols"]
    members = n_cols // HALVES
    groups = n_rows * HALVES
    total = n_rows * n_cols
    half = members // 2
    turn = 2 if members % 4 == 0 else 0

    tile_of = [[(2 * m if m < half else 2 * (members - 1 - m) + 1) ^ t for m in range(members)] for t in (0, turn)]
    holder = [[tiles.index(j) for j in range(members)] for tiles in tile_of]

    def seat(g, j):
        return g * members + holder[g // HALVES % 2][j]

    def local(lidar, camera, joined_weight, joined_bias, block_weight, block_bias, down_weight, down_bias, proj_weight, proj_bias):
        frames, sh, cols, lidar_ch = lidar.shape
        rows, sc, cam_ch = camera.shape[1:]
        tr = sh * members
        tw = cols // members
        wide = tw + 2 * SIDE
        pitch = rounded(wide, 16)
        w = cols // n_cols
        joined = joined_weight.shape[3]
        block = block_weight.shape[3]
        place = lax.axis_index(AXES)
        group = place // members
        member = place % members
        cindex = lax.axis_index("cols")
        kgroup = cindex // members

        def send(x, pairs):
            return lax.ppermute(x, AXES, pairs)

        def across(x, by_group, by_column):
            pairs = []
            for g in range(groups):
                for j in range(members):
                    if 0 <= g + by_group < groups and 0 <= j + by_column < members:
                        pairs.append((seat(g, j), seat(g + by_group, j + by_column)))
            return send(x, pairs)

        def column_of(m):
            return jnp.where(m < half, 2 * m, 2 * (members - 1 - m) + 1) ^ (turn * (group // HALVES % 2))

        joint = joined_weight.reshape(-1, joined)
        square = block_weight.reshape(-1, block)
        deep1 = 3 * (3 * lidar_ch + rounded(3 * cam_ch, 256))
        w1, w2 = pl.pallas_call(
            lambda *refs: weights_kernel(*refs, lidar=lidar_ch, camera=cam_ch),
            out_shape=[
                jax.ShapeDtypeStruct((deep1, joined), BF),
                jax.ShapeDtypeStruct((4 * 3 * joined, 2 * block), BF),
            ],
            compiler_params=limit(14),
            name="weights",
        )(joint, square)
        w3 = down_weight.reshape(-1, down_weight.shape[3])
        b1 = joined_bias.reshape(1, -1)
        b2 = jnp.concatenate([block_bias, block_bias]).reshape(1, -1)
        b3 = down_bias.reshape(1, -1)
        bp = proj_bias.reshape(1, -1)

        span = rounded(tr + UP + DOWN, 8)
        lanes = frames * span
        turned = jnp.transpose(camera, (0, 2, 3, 1))
        strip = jax.ShapeDtypeStruct((sc, cam_ch, lanes), BF)
        rim = jax.ShapeDtypeStruct((UP, cam_ch, lanes), BF)
        packed = pl.pallas_call(
            lambda *refs: camera_pack_kernel(*refs, tr=tr, span=span),
            grid_spec=pltpu.PrefetchScalarGridSpec(
                num_scalar_prefetch=1,
                grid=(1,),
                in_specs=[whole(turned)],
                out_specs=[whole(strip)] * groups + [whole(rim)] * groups,
            ),
            out_shape=[strip] * groups + [rim] * groups,
            compiler_params=limit(14),
            name="camera_pack",
        )(place.reshape(1).astype(jnp.int32), turned)
        arrived = [send(packed[p], [(s, seat((s + p) % groups, s // groups)) for s in range(total)]) for p in range(groups)]
        for e in range(groups):
            pairs = [(groups * j + groups - 1, seat(e, j + 1)) for j in range(members - 1)]
            pairs += [(groups * j, seat((e + 1) % groups, j - 1)) for j in range(1, members)]
            arrived.append(send(packed[groups + e], pairs))
        cam = pl.pallas_call(
            lambda *refs: camera_unpack_kernel(*refs, groups=groups, sc=sc, cam_ch=cam_ch),
            grid_spec=pltpu.PrefetchScalarGridSpec(
                num_scalar_prefetch=1,
                grid=(1,),
                in_specs=[whole(x) for x in arrived],
                out_specs=pl.BlockSpec((lanes, pitch, rounded(3 * cam_ch, 256)), lambda i, p: (0, 0, 0)),
                scratch_shapes=[
                    pltpu.VMEM((tw + UP + DOWN, cam_ch, lanes), BF),
                    pltpu.VMEM((lanes, pitch, 128), jnp.float32),
                ],
            ),
            out_shape=jax.ShapeDtypeStruct((lanes, pitch, rounded(3 * cam_ch, 256)), BF),
            compiler_params=limit(16),
            name="camera_unpack",
        )(group.reshape(1).astype(jnp.int32), *arrived)
        cam = cam.reshape(frames, span, pitch, -1)

        pos = jnp.stack([group, member, kgroup, column_of(member)]).astype(jnp.int32)
        pairs2 = (tr + 2) // 2
        half_rows = tr // 2
        n = HALVES * half_rows
        jd = rounded(w // 2, 8)
        flops = 2 * pitch * ((tr + 4) * w1.shape[0] * joined + pairs2 * w2.shape[0] * 2 * block)
        framed = lambda a: pl.BlockSpec((1,) + a.shape[1:], lambda f, p: (f,) + (0,) * (a.ndim - 1))
        encoded = None
        step = frames // CHUNKS
        for f0 in range(0, frames, step):
            source = lidar if not f0 else lax.optimization_barrier((lidar, packed[0]))[0]
            window = jax.ShapeDtypeStruct((step, sh, wide, lidar_ch), BF)
            windows = pl.pallas_call(
                functools.partial(window_kernel, tw=tw),
                grid_spec=pltpu.PrefetchScalarGridSpec(
                    num_scalar_prefetch=1,
                    grid=(step,),
                    in_specs=[pl.BlockSpec((1, sh, cols, lidar_ch), lambda f, p, f0=f0: (f + f0, 0, 0, 0))],
                    out_specs=[framed(window)] * members,
                ),
                out_shape=[window] * members,
                compiler_params=limit(60),
            )(jnp.stack([column_of((member + d) % members) for d in range(members)]).astype(jnp.int32), source)
            windows = [windows[0]] + [
                send(windows[d], [(g * members + m, g * members + (m + d) % members) for g in range(groups) for m in range(members)])
                for d in range(1, members)
            ]
            last, head = pick(windows, (member + 1) % members, member, 1)
            batch = step // 2 if step % 2 == 0 else step
            rims = []
            for b0 in range(0, step, batch):
                rims.append((across(last[b0 : b0 + batch], 1, 0), across(head[b0 : b0 + batch], -1, 0)))
            shifts = []
            for h in range(HALVES):
                shift = []
                for s in range(total):
                    r, c = divmod(s, n_cols)
                    k, m = divmod(c, members)
                    shift.append((s, r * n_cols + HALVES * tile_of[r % 2][m] + (k + h) % HALVES))
                shifts.append(shift)
            vmem = pl.BlockSpec(memory_space=pltpu.VMEM)
            for b0 in range(0, step, batch):
                blocks = jax.ShapeDtypeStruct((batch, pairs2, 2, w, block), BF)
                above, below = rims[b0 // batch]
                runs = [(0, batch)] if b0 == 0 else [(f, 1) for f in range(batch)]
                tiles = []
                for f1, many in runs:
                    tiles = pl.pallas_call(
                        functools.partial(conv_kernel, parts=members, sh=sh, tr=tr, pitch=pitch, rows=rows, cols=cols, at=b0 + f1, cam_at=f0 + b0 + f1, out_at=f1, many=many),
                        in_specs=[pl.BlockSpec(memory_space=pltpu.SMEM)] + [vmem] * (members + 7 + len(tiles)),
                        out_specs=[vmem] * HALVES,
                        scratch_shapes=conv_scratch(tr, pitch, lidar_ch, joined, block, pairs2),
                        out_shape=[blocks] * HALVES,
                        input_output_aliases={members + 8 + h: h for h in range(HALVES)} if tiles else {},
                        compiler_params=limit(20),
                        cost_estimate=pl.CostEstimate(flops=flops * many, bytes_accessed=2 * 10**6, transcendentals=0),
                    )(pos, *windows, above, below, cam, w1, b1, w2, b2, *tiles)
                pieces = []
                for h in range(HALVES):
                    pieces.append(send(tiles[h], shifts[h]))
                old = [] if encoded is None else [encoded]
                encoded = pl.pallas_call(
                    lambda *refs: encode_kernel(*refs, parts=HALVES, half_rows=half_rows, w=w),
                    grid_spec=pltpu.PrefetchScalarGridSpec(
                        num_scalar_prefetch=1,
                        grid=(batch,),
                        in_specs=[framed(x) for x in pieces] + [whole(x) for x in (w3, b3, proj_weight, bp)] + [pl.BlockSpec(memory_space=pl.ANY)] * len(old),
                        out_specs=pl.BlockSpec((1, n, 2, w, 2 * block), lambda f, p, lo=f0 + b0: (f + lo, 0, 0, 0, 0)),
                        scratch_shapes=[
                            pltpu.VMEM((n + 1, 2, rounded(w + 1, 8) + 16, block), jnp.float32),
                            pltpu.VMEM((n, 2 * jd, block), jnp.float32),
                        ],
                    ),
                    out_shape=jax.ShapeDtypeStruct((frames, n, 2, w, 2 * block), BF),
                    input_output_aliases={5 + HALVES: 0} if old else {},
                    compiler_params=limit(12),
                    cost_estimate=pl.CostEstimate(flops=2 * batch * n * jd * w3.shape[0] * 256, bytes_accessed=batch * 10**6, transcendentals=0),
                )(cindex.reshape(1).astype(jnp.int32), *pieces, w3, b3, proj_weight, bp, *old)
        return encoded.reshape(frames, 2 * n, w, 2 * block)

    return jax.shard_map(
        local,
        mesh=mesh,
        in_specs=(
            P("frames", AXES, None, None),
            P("frames", None, AXES, None),
            P(), P(), P(), P(), P(), P(), P(), P(),
        ),
        out_specs=P("frames", "rows", "cols", None),
        check_vma=False,
    )
```

```python
import functools

import jax
import jax.numpy as jnp
from jax import lax
from jax.experimental import pallas as pl
from jax.experimental.pallas import tpu as pltpu
from jax.sharding import PartitionSpec as P


AXES = ("rows", "cols")
CHUNKS = 1
HALVES = 2
SIDE = 4
UP, DOWN = 3, 2
BF = jnp.bfloat16


def rounded(n, to):
    return -(-n // to) * to


def limit(mib):
    return pltpu.CompilerParams(vmem_limit_bytes=mib * 2**20)


def whole(a):
    return pl.BlockSpec(a.shape, lambda *_: (0,) * a.ndim)


def weights_kernel(joint, square, w1, w2, *, lidar, camera):
    joined, block = joint.shape[1], square.shape[1]
    ch = lidar + camera
    deep = w1.shape[0] // 3
    for dy in range(3):
        base = dy * deep
        for dx in range(3):
            at = (dy * 3 + dx) * ch
            to = base + (1, 0, 2)[dx] * lidar
            w1[to : to + lidar, :] = joint[at : at + lidar, :]
            to = base + 3 * lidar + dx * camera
            w1[to : to + camera, :] = joint[at + lidar : at + ch, :]
        w1[base + 3 * ch : base + deep, :] = jnp.zeros((deep - 3 * ch, joined), BF)
    tall = square.shape[0]
    gap = w2.shape[0] - tall
    w2[0:tall, 0:block] = square[...]
    w2[tall:, 0:block] = jnp.zeros((gap, block), BF)
    w2[gap:, block:] = square[...]
    w2[0:gap, block:] = jnp.zeros((gap, block), BF)


def camera_pack_kernel(pos, x, *refs, tr, span):
    frames, sc, ch, rows = x.shape
    groups = len(refs) // 2
    outs, rims = refs[:groups], refs[groups:]
    width = frames * span
    place = pos[0]
    row = lax.broadcasted_iota(jnp.int32, (rows, width), 0)
    lane = lax.broadcasted_iota(jnp.int32, (rows, width), 1)

    def picks(f, targets):
        parts = []
        for target in targets:
            start = target * tr - UP
            parts.append(jnp.where(row + f * span == lane + start, jnp.where(lane // span == f, 1.0, 0.0), 0.0).astype(BF))
        return jnp.concatenate(parts, axis=1)

    main, rim = None, None
    rightmost = lax.rem(place, groups) == groups - 1
    for f in range(frames):
        pick = picks(f, [lax.rem(place + p, groups) for p in range(groups)])
        part = jnp.dot(x[f].reshape(sc * ch, rows), pick, preferred_element_type=jnp.float32)
        main = part if main is None else main + part
        pick = picks(f, [lax.rem(e + jnp.where(rightmost, 0, 1), groups) for e in range(groups)])
        border = jnp.where(rightmost, x[f, sc - UP : sc].astype(jnp.float32), x[f, 0:UP].astype(jnp.float32)).astype(BF)
        part = jnp.dot(border.reshape(UP * ch, rows), pick, preferred_element_type=jnp.float32)
        rim = part if rim is None else rim + part
    for p in range(groups):
        outs[p][...] = main[:, p * width : (p + 1) * width].astype(BF).reshape(sc, ch, width)
        rims[p][...] = rim[:, p * width : (p + 1) * width].astype(BF).reshape(UP, ch, width)


def window_kernel(pos, x, *outs, tw):
    n = x.shape[2] // tw
    wide = tw + 2 * SIDE
    edge = jnp.zeros((x.shape[1], SIDE, x.shape[3]), BF)
    for d in range(len(outs)):
        for c in range(n):

            @pl.when(pos[d] == c)
            def _():
                lo, hi = max(c * tw - SIDE, 0), min((c + 1) * tw + SIDE, n * tw)
                at = lo - (c * tw - SIDE)
                if at:
                    outs[d][0, :, 0:at, :] = edge
                if at + hi - lo < wide:
                    outs[d][0, :, at + hi - lo :, :] = edge
                outs[d][0, :, at : at + hi - lo, :] = x[0, :, lo:hi, :]


def camera_unpack_kernel(pos, *refs, groups, sc, cam_ch):
    strips, rims = refs[:groups], refs[groups : 2 * groups]
    out, stage, cells = refs[2 * groups :]
    group = pos[0]
    lanes = stage.shape[2]
    pitch = cells.shape[1]
    for p in range(groups):
        q = lax.rem(group - p + groups, groups)
        stage[pl.ds(UP + q * sc, sc)] = strips[p][...]
    n = UP + groups * sc + DOWN
    for e in range(groups):

        @pl.when(group == e)
        def _():
            stage[0:UP] = rims[e][...]

        @pl.when(group == (e + 1) % groups)
        def _():
            stage[n - DOWN : n] = rims[e][0:DOWN]

    lead = SIDE - UP
    cells[:, 0:8, :] = jnp.zeros((lanes, 8, 128), jnp.float32)
    low = (lead + n) // 8 * 8
    cells[:, low:, :] = jnp.zeros((lanes, pitch - low, 128), jnp.float32)
    for c in range(n):
        x = stage[c].astype(jnp.float32)
        x = jnp.concatenate([x, jnp.zeros((128 - cam_ch, lanes), jnp.float32)], axis=0)
        cells[:, lead + c, :] = x.T
    step = 8
    flat = step * pitch
    lane = lax.broadcasted_iota(jnp.int32, (flat, 128), 1)

    def widen(i, _):
        x = cells[pl.ds(i * step, step)].reshape(flat, 128)
        taps = [pltpu.roll(x, 1, 0), x, pltpu.roll(x, flat - 1, 0)]
        for v in range(out.shape[2] // 128):
            y = jnp.zeros((flat, 128), jnp.float32)
            for t in range(3):
                lo, hi = t * cam_ch - v * 128, (t + 1) * cam_ch - v * 128
                if hi > 0 and lo < 128:
                    turned = pltpu.roll(taps[t], lo % 128, 1) if lo % 128 else taps[t]
                    y = jnp.where((lane >= lo) & (lane < hi), turned, y)
            out[pl.ds(i * step, step), :, v * 128 : (v + 1) * 128] = y.astype(BF).reshape(step, pitch, 128)
        return 0

    lax.fori_loop(0, lanes // step, widen, 0)


def pick_kernel(pos, *refs):
    parts = (len(refs) - 2) // 2
    tail, head = refs[-2:]
    for d in range(parts):

        @pl.when(pos[0] == d)
        def _():
            tail[...] = refs[d][...]

        @pl.when(pos[1] == d)
        def _():
            head[...] = refs[parts + d][...]


def pick(arrays, tail_of, head_of, dim):
    size = arrays[0].shape[dim]
    specs, shapes, outs = [], [], []
    for n, at in ((UP, size // UP - 1), (DOWN, 0)):
        shape = arrays[0].shape[:dim] + (n,) + arrays[0].shape[dim + 1 :]
        where = tuple(at if i == dim else 0 for i in range(len(shape)))
        specs += [pl.BlockSpec(shape, lambda i, p, where=where: where)] * len(arrays)
        shapes.append(jax.ShapeDtypeStruct(shape, BF))
        outs.append(pl.BlockSpec(shape, lambda i, p, n=len(shape): (0,) * n))
    return pl.pallas_call(
        pick_kernel,
        grid_spec=pltpu.PrefetchScalarGridSpec(num_scalar_prefetch=1, grid=(1,), in_specs=specs, out_specs=outs),
        out_shape=shapes,
        compiler_params=limit(3),
    )(jnp.stack([tail_of, head_of]).astype(jnp.int32), *arrays, *arrays)


def conv_scratch(tr, pitch, lidar, joined, block, pairs):
    return [
        pltpu.VMEM((tr + 6, pitch, lidar), BF),
        pltpu.VMEM((tr + 6, pitch, 2 * lidar), BF),
        pltpu.VMEM(((tr + 4) // 2, 2, pitch, 3 * joined), BF),
        pltpu.VMEM((pairs, 2, pitch, block), jnp.float32),
        pltpu.VMEM((pitch, joined), jnp.float32),
    ]


def conv_kernel(pos, *refs, parts, sh, tr, pitch, rows, cols, at, cam_at, rim_at, many):
    windows = refs[:parts]
    above, below, camera, w1, b1, w2, b2 = refs[parts : parts + 7]
    outs = refs[-5 - HALVES : -5]
    tile, taps, mid, cells, inside = refs[-5:]
    group, member, half_id, column = pos[0], pos[1], pos[2], pos[3]
    wide = windows[0].shape[2]
    lidar = windows[0].shape[3]
    joined = w1.shape[1]
    block = w2.shape[1] // 2
    col0 = column * (wide - 2 * SIDE) - SIDE

    edge_cols = pitch - wide
    tile[:, wide:, :] = jnp.zeros((tr + 6, edge_cols, lidar), BF)
    tile[tr + UP + DOWN :, 0:wide, :] = jnp.zeros((tr + 6 - tr - UP - DOWN, wide, lidar), BF)
    col = lax.broadcasted_iota(jnp.int32, inside.shape, 0) + col0
    inside[...] = jnp.where((col >= 0) & (col < cols), 1.0, 0.0)

    def frame(f, _):
        tile[0:UP, 0:wide, :] = above[rim_at + f]
        for d in range(parts):
            source = lax.rem(member - d + parts, parts)
            tile[pl.ds(UP + source * sh, sh), 0:wide, :] = windows[d][at + f]
        tile[UP + tr : UP + tr + DOWN, 0:wide, :] = below[rim_at + f]

        step = 6
        flat = step * pitch

        def shift(i, _):
            r = i * step
            x = tile[pl.ds(r, step)].reshape(flat, lidar).astype(jnp.float32)
            taps[pl.ds(r, step), :, 0:lidar] = pltpu.roll(x, 1, 0).astype(BF).reshape(step, pitch, lidar)
            taps[pl.ds(r, step), :, lidar:] = pltpu.roll(x, flat - 1, 0).astype(BF).reshape(step, pitch, lidar)
            return 0

        lax.fori_loop(0, (tr + 6) // step, shift, 0)

        n1 = (tr + 4) // 2
        m1 = n1 * pitch

        def first(i, _):
            r = i * n1
            lhs = []
            for dy in range(3):
                lhs.append(tile[pl.ds(r + dy, n1)].reshape(m1, lidar))
                lhs.append(taps[pl.ds(r + dy, n1)].reshape(m1, 2 * lidar))
                lhs.append(camera[cam_at + f, pl.ds(r + dy, n1)].reshape(m1, camera.shape[3]))
            acc = jnp.dot(jnp.concatenate(lhs, axis=1), w1[...], preferred_element_type=jnp.float32)
            v = jnp.maximum(acc + b1[...], 0.0).reshape(n1, pitch, joined)
            kept = []
            for y in range(n1):
                row = group * tr - 2 + r + y
                kept.append(v[y] * (inside[...] * jnp.where((row >= 0) & (row < rows), 1.0, 0.0)))
            v = jnp.concatenate(kept, axis=0)
            shape = (n1 // 2, 2, pitch, joined)
            p = pl.ds(i * (n1 // 2), n1 // 2)
            mid[p, :, :, 0:joined] = pltpu.roll(v, 1, 0).astype(BF).reshape(shape)
            mid[p, :, :, joined : 2 * joined] = v.astype(BF).reshape(shape)
            mid[p, :, :, 2 * joined :] = pltpu.roll(v, m1 - 1, 0).astype(BF).reshape(shape)
            return 0

        lax.fori_loop(0, (tr + 4) // n1, first, 0)

        n2 = (tr + 2) // 2
        m2 = n2 * pitch
        lhs = [mid[i // 2 : i // 2 + n2, i % 2].reshape(m2, 3 * joined) for i in range(4)]
        acc = jnp.dot(jnp.concatenate(lhs, axis=1), w2[...], preferred_element_type=jnp.float32)
        v = pltpu.roll(jnp.maximum(acc + b2[...], 0.0), SIDE, 0)
        cells[:, 0] = v[:, :block].reshape(n2, pitch, block)
        cells[:, 1] = v[:, block:].reshape(n2, pitch, block)
        pairs = tr // 2
        w = (wide - 2 * SIDE) // HALVES
        for sub in range(HALVES):
            c = 2 * SIDE + sub * w
            even = cells[0:pairs, 1, c : c + w, :].astype(BF)
            odd = cells[1 : pairs + 1, 0, c : c + w, :].astype(BF)
            top = jnp.where(group > 0, cells[0, 0, c : c + w, :], 0.0)
            corner = jnp.broadcast_to(cells[pairs, 0, c - 1 : c, :], (w, block))
            beside = cells[0:pairs, :, c - 1, :].reshape(tr, block)
            if sub == 0:
                corner = jnp.where(column > 0, corner, 0.0)
                beside = jnp.where(column > 0, beside, 0.0)
            row = lax.broadcasted_iota(jnp.int32, beside.shape, 0)
            beside = jnp.where((row == 0) & (group == 0), 0.0, beside)
            edge = jnp.where(half_id == 0, top, corner).astype(BF)
            beside = beside.astype(BF)
            for h in range(HALVES):

                @pl.when(lax.rem(half_id + h, HALVES) == sub)
                def _():
                    outs[h][f, 0:pairs, 0] = even
                    outs[h][f, 0:pairs, 1] = odd
                    outs[h][f, pairs, 0] = edge
                    outs[h][f, pairs, 1] = beside
        return 0

    if many == 1:
        frame(0, 0)
    else:
        lax.fori_loop(0, many, frame, 0)


def encode_kernel(pos, *refs, parts, half_rows, w):
    pieces = refs[:parts]
    w3, b3, wp, bp = refs[parts : parts + 4]
    out, grid, grown = refs[-3:]
    me = pos[0]
    block = pieces[0].shape[4]
    for h in range(parts):
        part = lax.rem(me - h + parts, parts)
        base = part * half_rows
        x = pieces[h]
        grid[pl.ds(base, half_rows), 1, 1 : w + 1, :] = x[0, 0:half_rows, 0].astype(jnp.float32)
        grid[pl.ds(base + 1, half_rows), 0, 1 : w + 1, :] = x[0, 0:half_rows, 1].astype(jnp.float32)
        beside = x[0, half_rows, 1].astype(jnp.float32)
        for r in range(2 * half_rows):
            grid[base + r // 2, r % 2, 0:1, :] = beside[r : r + 1]
        edge = x[0, half_rows, 0].astype(jnp.float32)

        @pl.when(part == 0)
        def _():
            grid[0, 0, 1 : w + 1, :] = edge

        @pl.when(part == parts - 1)
        def _():
            grid[parts * half_rows, 0, 0:1, :] = edge[0:1]

    n = parts * half_rows
    jd = rounded(w // 2, 8)
    m = n * jd
    lhs = []
    for a in range(3):
        for b in range(3):
            x = grid[pl.ds(a // 2, n), a % 2, pl.ds(b, jd, stride=2), :]
            lhs.append(x.reshape(m, block).astype(BF))
    deep = jnp.dot(jnp.concatenate(lhs, axis=1), w3[...], preferred_element_type=jnp.float32)
    deep = jnp.maximum(deep + b3[...], 0.0).astype(BF)
    branch = jnp.dot(deep, wp[...], preferred_element_type=jnp.float32)
    branch = jnp.maximum(branch + bp[...], 0.0).astype(BF).astype(jnp.float32).reshape(n, jd, wp.shape[1])
    grown[:, pl.ds(0, jd, stride=2), :] = branch
    grown[:, pl.ds(1, jd, stride=2), :] = branch
    up = grown[:, 0:w, :].astype(BF)
    out[0, :, 0, :, 0:block] = grid[0:n, 1, 1 : w + 1, :].astype(BF)
    out[0, :, 1, :, 0:block] = grid[1 : n + 1, 0, 1 : w + 1, :].astype(BF)
    out[0, :, 0, :, block:] = up
    out[0, :, 1, :, block:] = up


def solution(mesh):
    n_rows, n_cols = mesh.shape["rows"], mesh.shape["cols"]
    members = n_cols // HALVES
    groups = n_rows * HALVES
    total = n_rows * n_cols
    half = members // 2
    turn = 2 if members % 4 == 0 else 0

    tile_of = [[(2 * m if m < half else 2 * (members - 1 - m) + 1) ^ t for m in range(members)] for t in (0, turn)]
    holder = [[tiles.index(j) for j in range(members)] for tiles in tile_of]

    def seat(g, j):
        return g * members + holder[g // HALVES % 2][j]

    def local(lidar, camera, joined_weight, joined_bias, block_weight, block_bias, down_weight, down_bias, proj_weight, proj_bias):
        frames, sh, cols, lidar_ch = lidar.shape
        rows, sc, cam_ch = camera.shape[1:]
        tr = sh * members
        tw = cols // members
        wide = tw + 2 * SIDE
        pitch = rounded(wide, 16)
        w = cols // n_cols
        joined = joined_weight.shape[3]
        block = block_weight.shape[3]
        place = lax.axis_index(AXES)
        group = place // members
        member = place % members
        cindex = lax.axis_index("cols")
        kgroup = cindex // members

        def send(x, pairs):
            return lax.ppermute(x, AXES, pairs)

        def across(x, by_group, by_column):
            pairs = []
            for g in range(groups):
                for j in range(members):
                    if 0 <= g + by_group < groups and 0 <= j + by_column < members:
                        pairs.append((seat(g, j), seat(g + by_group, j + by_column)))
            return send(x, pairs)

        def column_of(m):
            return jnp.where(m < half, 2 * m, 2 * (members - 1 - m) + 1) ^ (turn * (group // HALVES % 2))

        joint = joined_weight.reshape(-1, joined)
        square = block_weight.reshape(-1, block)
        deep1 = 3 * (3 * lidar_ch + rounded(3 * cam_ch, 256))
        w1, w2 = pl.pallas_call(
            lambda *refs: weights_kernel(*refs, lidar=lidar_ch, camera=cam_ch),
            out_shape=[
                jax.ShapeDtypeStruct((deep1, joined), BF),
                jax.ShapeDtypeStruct((4 * 3 * joined, 2 * block), BF),
            ],
            compiler_params=limit(14),
            name="weights",
        )(joint, square)
        w3 = down_weight.reshape(-1, down_weight.shape[3])
        b1 = joined_bias.reshape(1, -1)
        b2 = jnp.concatenate([block_bias, block_bias]).reshape(1, -1)
        b3 = down_bias.reshape(1, -1)
        bp = proj_bias.reshape(1, -1)

        span = rounded(tr + UP + DOWN, 8)
        lanes = frames * span
        turned = jnp.transpose(camera, (0, 2, 3, 1))
        strip = jax.ShapeDtypeStruct((sc, cam_ch, lanes), BF)
        rim = jax.ShapeDtypeStruct((UP, cam_ch, lanes), BF)
        packed = pl.pallas_call(
            lambda *refs: camera_pack_kernel(*refs, tr=tr, span=span),
            grid_spec=pltpu.PrefetchScalarGridSpec(
                num_scalar_prefetch=1,
                grid=(1,),
                in_specs=[whole(turned)],
                out_specs=[whole(strip)] * groups + [whole(rim)] * groups,
            ),
            out_shape=[strip] * groups + [rim] * groups,
            compiler_params=limit(14),
            name="camera_pack",
        )(place.reshape(1).astype(jnp.int32), turned)
        arrived = [send(packed[p], [(s, seat((s + p) % groups, s // groups)) for s in range(total)]) for p in range(groups)]
        for e in range(groups):
            pairs = [(groups * j + groups - 1, seat(e, j + 1)) for j in range(members - 1)]
            pairs += [(groups * j, seat((e + 1) % groups, j - 1)) for j in range(1, members)]
            arrived.append(send(packed[groups + e], pairs))
        cam = pl.pallas_call(
            lambda *refs: camera_unpack_kernel(*refs, groups=groups, sc=sc, cam_ch=cam_ch),
            grid_spec=pltpu.PrefetchScalarGridSpec(
                num_scalar_prefetch=1,
                grid=(1,),
                in_specs=[whole(x) for x in arrived],
                out_specs=pl.BlockSpec((lanes, pitch, rounded(3 * cam_ch, 256)), lambda i, p: (0, 0, 0)),
                scratch_shapes=[
                    pltpu.VMEM((tw + UP + DOWN, cam_ch, lanes), BF),
                    pltpu.VMEM((lanes, pitch, 128), jnp.float32),
                ],
            ),
            out_shape=jax.ShapeDtypeStruct((lanes, pitch, rounded(3 * cam_ch, 256)), BF),
            compiler_params=limit(16),
            name="camera_unpack",
        )(group.reshape(1).astype(jnp.int32), *arrived)
        cam = cam.reshape(frames, span, pitch, -1)

        pos = jnp.stack([group, member, kgroup, column_of(member)]).astype(jnp.int32)
        pairs2 = (tr + 2) // 2
        half_rows = tr // 2
        n = HALVES * half_rows
        jd = rounded(w // 2, 8)
        flops = 2 * pitch * ((tr + 4) * w1.shape[0] * joined + pairs2 * w2.shape[0] * 2 * block)
        framed = lambda a: pl.BlockSpec((1,) + a.shape[1:], lambda f, p: (f,) + (0,) * (a.ndim - 1))
        encoded = None
        step = frames // CHUNKS
        for f0 in range(0, frames, step):
            source = lidar if not f0 else lax.optimization_barrier((lidar, packed[0]))[0]
            window = jax.ShapeDtypeStruct((step, sh, wide, lidar_ch), BF)
            windows = pl.pallas_call(
                functools.partial(window_kernel, tw=tw),
                grid_spec=pltpu.PrefetchScalarGridSpec(
                    num_scalar_prefetch=1,
                    grid=(step,),
                    in_specs=[pl.BlockSpec((1, sh, cols, lidar_ch), lambda f, p, f0=f0: (f + f0, 0, 0, 0))],
                    out_specs=[framed(window)] * members,
                ),
                out_shape=[window] * members,
                compiler_params=limit(6),
            )(jnp.stack([column_of((member + d) % members) for d in range(members)]).astype(jnp.int32), source)
            windows = [windows[0]] + [
                send(windows[d], [(g * members + m, g * members + (m + d) % members) for g in range(groups) for m in range(members)])
                for d in range(1, members)
            ]
            last, head = pick(windows, (member + 1) % members, member, 1)
            batch = step // 2 if step % 2 == 0 else step
            rims = []
            for b0 in range(0, step, batch):
                rims.append((across(last[b0 : b0 + batch], 1, 0), across(head[b0 : b0 + batch], -1, 0)))
            shifts = []
            for h in range(HALVES):
                shift = []
                for s in range(total):
                    r, c = divmod(s, n_cols)
                    k, m = divmod(c, members)
                    shift.append((s, r * n_cols + HALVES * tile_of[r % 2][m] + (k + h) % HALVES))
                shifts.append(shift)
            vmem = pl.BlockSpec(memory_space=pltpu.VMEM)
            batches = [(0, batch)] + [(f, 1) for f in range(batch, step)]
            for b0, many in batches:
                blocks = jax.ShapeDtypeStruct((many, pairs2, 2, w, block), BF)
                above, below = rims[b0 // batch]
                tiles = pl.pallas_call(
                    functools.partial(conv_kernel, parts=members, sh=sh, tr=tr, pitch=pitch, rows=rows, cols=cols, at=b0, cam_at=f0 + b0, rim_at=b0 % batch, many=many),
                    in_specs=[pl.BlockSpec(memory_space=pltpu.SMEM)] + [vmem] * (members + 7),
                    out_specs=[vmem] * HALVES,
                    scratch_shapes=conv_scratch(tr, pitch, lidar_ch, joined, block, pairs2),
                    out_shape=[blocks] * HALVES,
                    compiler_params=limit(20),
                    cost_estimate=pl.CostEstimate(flops=flops * many, bytes_accessed=2 * 10**6, transcendentals=0),
                )(pos, *windows, above, below, cam, w1, b1, w2, b2)
                pieces = []
                for h in range(HALVES):
                    pieces.append(send(tiles[h], shifts[h]))
                old = [] if encoded is None else [encoded]
                encoded = pl.pallas_call(
                    lambda *refs: encode_kernel(*refs, parts=HALVES, half_rows=half_rows, w=w),
                    grid_spec=pltpu.PrefetchScalarGridSpec(
                        num_scalar_prefetch=1,
                        grid=(many,),
                        in_specs=[framed(x) for x in pieces] + [whole(x) for x in (w3, b3, proj_weight, bp)] + [pl.BlockSpec(memory_space=pl.ANY)] * len(old),
                        out_specs=pl.BlockSpec((1, n, 2, w, 2 * block), lambda f, p, lo=f0 + b0: (f + lo, 0, 0, 0, 0)),
                        scratch_shapes=[
                            pltpu.VMEM((n + 1, 2, rounded(w + 1, 8) + 16, block), jnp.float32),
                            pltpu.VMEM((n, 2 * jd, block), jnp.float32),
                        ],
                    ),
                    out_shape=jax.ShapeDtypeStruct((frames, n, 2, w, 2 * block), BF),
                    input_output_aliases={5 + HALVES: 0} if old else {},
                    compiler_params=limit(12),
                    cost_estimate=pl.CostEstimate(flops=2 * many * n * jd * w3.shape[0] * 256, bytes_accessed=many * 10**6, transcendentals=0),
                )(cindex.reshape(1).astype(jnp.int32), *pieces, w3, b3, proj_weight, bp, *old)
        return encoded.reshape(frames, 2 * n, w, 2 * block)

    return jax.shard_map(
        local,
        mesh=mesh,
        in_specs=(
            P("frames", AXES, None, None),
            P("frames", None, AXES, None),
            P(), P(), P(), P(), P(), P(), P(), P(),
        ),
        out_specs=P("frames", "rows", "cols", None),
        check_vma=False,
    )
```

```python
import functools

import jax
import jax.numpy as jnp
from jax import lax
from jax.experimental import pallas as pl
from jax.experimental.pallas import tpu as pltpu
from jax.sharding import PartitionSpec as P


AXES = ("rows", "cols")
CHUNKS = 2
HALVES = 2
SIDE = 4
UP, DOWN = 3, 2
BF = jnp.bfloat16


def rounded(n, to):
    return -(-n // to) * to


def limit(mib):
    return pltpu.CompilerParams(vmem_limit_bytes=mib * 2**20)


def whole(a):
    return pl.BlockSpec(a.shape, lambda *_: (0,) * a.ndim)


def weights_kernel(joint, square, w1, w2, *, lidar, camera):
    joined, block = joint.shape[1], square.shape[1]
    ch = lidar + camera
    deep = w1.shape[0] // 3
    for dy in range(3):
        base = dy * deep
        for dx in range(3):
            at = (dy * 3 + dx) * ch
            to = base + (1, 0, 2)[dx] * lidar
            w1[to : to + lidar, :] = joint[at : at + lidar, :]
            to = base + 3 * lidar + dx * camera
            w1[to : to + camera, :] = joint[at + lidar : at + ch, :]
        w1[base + 3 * ch : base + deep, :] = jnp.zeros((deep - 3 * ch, joined), BF)
    tall = square.shape[0]
    gap = w2.shape[0] - tall
    w2[0:tall, 0:block] = square[...]
    w2[tall:, 0:block] = jnp.zeros((gap, block), BF)
    w2[gap:, block:] = square[...]
    w2[0:gap, block:] = jnp.zeros((gap, block), BF)


def camera_pack_kernel(pos, x, *refs, tr, span):
    frames, sc, ch, rows = x.shape
    groups = len(refs) // 2
    outs, rims = refs[:groups], refs[groups:]
    width = frames * span
    place = pos[0]
    row = lax.broadcasted_iota(jnp.int32, (rows, width), 0)
    lane = lax.broadcasted_iota(jnp.int32, (rows, width), 1)

    def picks(f, targets):
        parts = []
        for target in targets:
            start = target * tr - UP
            parts.append(jnp.where(row + f * span == lane + start, jnp.where(lane // span == f, 1.0, 0.0), 0.0).astype(BF))
        return jnp.concatenate(parts, axis=1)

    main, rim = None, None
    rightmost = lax.rem(place, groups) == groups - 1
    for f in range(frames):
        pick = picks(f, [lax.rem(place + p, groups) for p in range(groups)])
        part = jnp.dot(x[f].reshape(sc * ch, rows), pick, preferred_element_type=jnp.float32)
        main = part if main is None else main + part
        pick = picks(f, [lax.rem(e + jnp.where(rightmost, 0, 1), groups) for e in range(groups)])
        border = jnp.where(rightmost, x[f, sc - UP : sc].astype(jnp.float32), x[f, 0:UP].astype(jnp.float32)).astype(BF)
        part = jnp.dot(border.reshape(UP * ch, rows), pick, preferred_element_type=jnp.float32)
        rim = part if rim is None else rim + part
    for p in range(groups):
        outs[p][...] = main[:, p * width : (p + 1) * width].astype(BF).reshape(sc, ch, width)
        rims[p][...] = rim[:, p * width : (p + 1) * width].astype(BF).reshape(UP, ch, width)


def window_kernel(pos, x, *outs, tw):
    n = x.shape[2] // tw
    wide = tw + 2 * SIDE
    edge = jnp.zeros((x.shape[1], SIDE, x.shape[3]), BF)
    for d in range(len(outs)):
        for c in range(n):

            @pl.when(pos[d] == c)
            def _():
                lo, hi = max(c * tw - SIDE, 0), min((c + 1) * tw + SIDE, n * tw)
                at = lo - (c * tw - SIDE)
                if at:
                    outs[d][0, :, 0:at, :] = edge
                if at + hi - lo < wide:
                    outs[d][0, :, at + hi - lo :, :] = edge
                outs[d][0, :, at : at + hi - lo, :] = x[0, :, lo:hi, :]


def camera_unpack_kernel(pos, *refs, groups, sc, cam_ch):
    strips, rims = refs[:groups], refs[groups : 2 * groups]
    out, stage, cells = refs[2 * groups :]
    group = pos[0]
    lanes = stage.shape[2]
    pitch = cells.shape[1]
    for p in range(groups):
        q = lax.rem(group - p + groups, groups)
        stage[pl.ds(UP + q * sc, sc)] = strips[p][...]
    n = UP + groups * sc + DOWN
    for e in range(groups):

        @pl.when(group == e)
        def _():
            stage[0:UP] = rims[e][...]

        @pl.when(group == (e + 1) % groups)
        def _():
            stage[n - DOWN : n] = rims[e][0:DOWN]

    lead = SIDE - UP
    cells[:, 0:8, :] = jnp.zeros((lanes, 8, 128), jnp.float32)
    low = (lead + n) // 8 * 8
    cells[:, low:, :] = jnp.zeros((lanes, pitch - low, 128), jnp.float32)
    for c in range(n):
        x = stage[c].astype(jnp.float32)
        x = jnp.concatenate([x, jnp.zeros((128 - cam_ch, lanes), jnp.float32)], axis=0)
        cells[:, lead + c, :] = x.T
    step = 8
    flat = step * pitch
    lane = lax.broadcasted_iota(jnp.int32, (flat, 128), 1)

    def widen(i, _):
        x = cells[pl.ds(i * step, step)].reshape(flat, 128)
        taps = [pltpu.roll(x, 1, 0), x, pltpu.roll(x, flat - 1, 0)]
        for v in range(out.shape[2] // 128):
            y = jnp.zeros((flat, 128), jnp.float32)
            for t in range(3):
                lo, hi = t * cam_ch - v * 128, (t + 1) * cam_ch - v * 128
                if hi > 0 and lo < 128:
                    turned = pltpu.roll(taps[t], lo % 128, 1) if lo % 128 else taps[t]
                    y = jnp.where((lane >= lo) & (lane < hi), turned, y)
            out[pl.ds(i * step, step), :, v * 128 : (v + 1) * 128] = y.astype(BF).reshape(step, pitch, 128)
        return 0

    lax.fori_loop(0, lanes // step, widen, 0)


def pick_kernel(pos, *refs):
    parts = (len(refs) - 2) // 2
    tail, head = refs[-2:]
    for d in range(parts):

        @pl.when(pos[0] == d)
        def _():
            tail[...] = refs[d][...]

        @pl.when(pos[1] == d)
        def _():
            head[...] = refs[parts + d][...]


def pick(arrays, tail_of, head_of, dim):
    size = arrays[0].shape[dim]
    specs, shapes, outs = [], [], []
    for n, at in ((UP, size // UP - 1), (DOWN, 0)):
        shape = arrays[0].shape[:dim] + (n,) + arrays[0].shape[dim + 1 :]
        where = tuple(at if i == dim else 0 for i in range(len(shape)))
        specs += [pl.BlockSpec(shape, lambda i, p, where=where: where)] * len(arrays)
        shapes.append(jax.ShapeDtypeStruct(shape, BF))
        outs.append(pl.BlockSpec(shape, lambda i, p, n=len(shape): (0,) * n))
    return pl.pallas_call(
        pick_kernel,
        grid_spec=pltpu.PrefetchScalarGridSpec(num_scalar_prefetch=1, grid=(1,), in_specs=specs, out_specs=outs),
        out_shape=shapes,
        compiler_params=limit(3),
    )(jnp.stack([tail_of, head_of]).astype(jnp.int32), *arrays, *arrays)


def conv_scratch(tr, pitch, lidar, joined, block, pairs):
    return [
        pltpu.VMEM((tr + 6, pitch, lidar), BF),
        pltpu.VMEM((tr + 6, pitch, 2 * lidar), BF),
        pltpu.VMEM(((tr + 4) // 2, 2, pitch, 3 * joined), BF),
        pltpu.VMEM((pairs, 2, pitch, block), jnp.float32),
        pltpu.VMEM((pitch, joined), jnp.float32),
    ]


def conv_kernel(pos, *refs, parts, sh, tr, pitch, rows, cols, at, cam_at, rim_at, many):
    windows = refs[:parts]
    above, below, camera, w1, b1, w2, b2 = refs[parts : parts + 7]
    outs = refs[-5 - HALVES : -5]
    tile, taps, mid, cells, inside = refs[-5:]
    group, member, half_id, column = pos[0], pos[1], pos[2], pos[3]
    wide = windows[0].shape[2]
    lidar = windows[0].shape[3]
    joined = w1.shape[1]
    block = w2.shape[1] // 2
    col0 = column * (wide - 2 * SIDE) - SIDE

    edge_cols = pitch - wide
    tile[:, wide:, :] = jnp.zeros((tr + 6, edge_cols, lidar), BF)
    tile[tr + UP + DOWN :, 0:wide, :] = jnp.zeros((tr + 6 - tr - UP - DOWN, wide, lidar), BF)
    col = lax.broadcasted_iota(jnp.int32, inside.shape, 0) + col0
    inside[...] = jnp.where((col >= 0) & (col < cols), 1.0, 0.0)

    def frame(f, _):
        tile[0:UP, 0:wide, :] = above[rim_at + f]
        for d in range(parts):
            source = lax.rem(member - d + parts, parts)
            tile[pl.ds(UP + source * sh, sh), 0:wide, :] = windows[d][at + f]
        tile[UP + tr : UP + tr + DOWN, 0:wide, :] = below[rim_at + f]

        step = 6
        flat = step * pitch

        def shift(i, _):
            r = i * step
            x = tile[pl.ds(r, step)].reshape(flat, lidar).astype(jnp.float32)
            taps[pl.ds(r, step), :, 0:lidar] = pltpu.roll(x, 1, 0).astype(BF).reshape(step, pitch, lidar)
            taps[pl.ds(r, step), :, lidar:] = pltpu.roll(x, flat - 1, 0).astype(BF).reshape(step, pitch, lidar)
            return 0

        lax.fori_loop(0, (tr + 6) // step, shift, 0)

        n1 = (tr + 4) // 2
        m1 = n1 * pitch

        def first(i, _):
            r = i * n1
            lhs = []
            for dy in range(3):
                lhs.append(tile[pl.ds(r + dy, n1)].reshape(m1, lidar))
                lhs.append(taps[pl.ds(r + dy, n1)].reshape(m1, 2 * lidar))
                lhs.append(camera[cam_at + f, pl.ds(r + dy, n1)].reshape(m1, camera.shape[3]))
            acc = jnp.dot(jnp.concatenate(lhs, axis=1), w1[...], preferred_element_type=jnp.float32)
            v = jnp.maximum(acc + b1[...], 0.0).reshape(n1, pitch, joined)
            kept = []
            for y in range(n1):
                row = group * tr - 2 + r + y
                kept.append(v[y] * (inside[...] * jnp.where((row >= 0) & (row < rows), 1.0, 0.0)))
            v = jnp.concatenate(kept, axis=0)
            shape = (n1 // 2, 2, pitch, joined)
            p = pl.ds(i * (n1 // 2), n1 // 2)
            mid[p, :, :, 0:joined] = pltpu.roll(v, 1, 0).astype(BF).reshape(shape)
            mid[p, :, :, joined : 2 * joined] = v.astype(BF).reshape(shape)
            mid[p, :, :, 2 * joined :] = pltpu.roll(v, m1 - 1, 0).astype(BF).reshape(shape)
            return 0

        lax.fori_loop(0, (tr + 4) // n1, first, 0)

        n2 = (tr + 2) // 2
        m2 = n2 * pitch
        lhs = [mid[i // 2 : i // 2 + n2, i % 2].reshape(m2, 3 * joined) for i in range(4)]
        acc = jnp.dot(jnp.concatenate(lhs, axis=1), w2[...], preferred_element_type=jnp.float32)
        v = pltpu.roll(jnp.maximum(acc + b2[...], 0.0), SIDE, 0)
        cells[:, 0] = v[:, :block].reshape(n2, pitch, block)
        cells[:, 1] = v[:, block:].reshape(n2, pitch, block)
        pairs = tr // 2
        w = (wide - 2 * SIDE) // HALVES
        for sub in range(HALVES):
            c = 2 * SIDE + sub * w
            even = cells[0:pairs, 1, c : c + w, :].astype(BF)
            odd = cells[1 : pairs + 1, 0, c : c + w, :].astype(BF)
            top = jnp.where(group > 0, cells[0, 0, c : c + w, :], 0.0)
            corner = jnp.broadcast_to(cells[pairs, 0, c - 1 : c, :], (w, block))
            beside = cells[0:pairs, :, c - 1, :].reshape(tr, block)
            if sub == 0:
                corner = jnp.where(column > 0, corner, 0.0)
                beside = jnp.where(column > 0, beside, 0.0)
            row = lax.broadcasted_iota(jnp.int32, beside.shape, 0)
            beside = jnp.where((row == 0) & (group == 0), 0.0, beside)
            edge = jnp.where(half_id == 0, top, corner).astype(BF)
            beside = beside.astype(BF)
            for h in range(HALVES):

                @pl.when(lax.rem(half_id + h, HALVES) == sub)
                def _():
                    outs[h][f, 0:pairs, 0] = even
                    outs[h][f, 0:pairs, 1] = odd
                    outs[h][f, pairs, 0] = edge
                    outs[h][f, pairs, 1] = beside
        return 0

    if many == 1:
        frame(0, 0)
    else:
        lax.fori_loop(0, many, frame, 0)


def encode_kernel(pos, *refs, parts, half_rows, w):
    pieces = refs[:parts]
    w3, b3, wp, bp = refs[parts : parts + 4]
    out, grid, grown = refs[-3:]
    me = pos[0]
    block = pieces[0].shape[4]
    for h in range(parts):
        part = lax.rem(me - h + parts, parts)
        base = part * half_rows
        x = pieces[h]
        grid[pl.ds(base, half_rows), 1, 1 : w + 1, :] = x[0, 0:half_rows, 0].astype(jnp.float32)
        grid[pl.ds(base + 1, half_rows), 0, 1 : w + 1, :] = x[0, 0:half_rows, 1].astype(jnp.float32)
        beside = x[0, half_rows, 1].astype(jnp.float32)
        for r in range(2 * half_rows):
            grid[base + r // 2, r % 2, 0:1, :] = beside[r : r + 1]
        edge = x[0, half_rows, 0].astype(jnp.float32)

        @pl.when(part == 0)
        def _():
            grid[0, 0, 1 : w + 1, :] = edge

        @pl.when(part == parts - 1)
        def _():
            grid[parts * half_rows, 0, 0:1, :] = edge[0:1]

    n = parts * half_rows
    jd = rounded(w // 2, 8)
    m = n * jd
    lhs = []
    for a in range(3):
        for b in range(3):
            x = grid[pl.ds(a // 2, n), a % 2, pl.ds(b, jd, stride=2), :]
            lhs.append(x.reshape(m, block).astype(BF))
    deep = jnp.dot(jnp.concatenate(lhs, axis=1), w3[...], preferred_element_type=jnp.float32)
    deep = jnp.maximum(deep + b3[...], 0.0).astype(BF)
    branch = jnp.dot(deep, wp[...], preferred_element_type=jnp.float32)
    branch = jnp.maximum(branch + bp[...], 0.0).astype(BF).astype(jnp.float32).reshape(n, jd, wp.shape[1])
    grown[:, pl.ds(0, jd, stride=2), :] = branch
    grown[:, pl.ds(1, jd, stride=2), :] = branch
    up = grown[:, 0:w, :].astype(BF)
    out[0, :, 0, :, 0:block] = grid[0:n, 1, 1 : w + 1, :].astype(BF)
    out[0, :, 1, :, 0:block] = grid[1 : n + 1, 0, 1 : w + 1, :].astype(BF)
    out[0, :, 0, :, block:] = up
    out[0, :, 1, :, block:] = up


def solution(mesh):
    n_rows, n_cols = mesh.shape["rows"], mesh.shape["cols"]
    members = n_cols // HALVES
    groups = n_rows * HALVES
    total = n_rows * n_cols
    half = members // 2
    turn = 2 if members % 4 == 0 else 0

    tile_of = [[(2 * m if m < half else 2 * (members - 1 - m) + 1) ^ t for m in range(members)] for t in (0, turn)]
    holder = [[tiles.index(j) for j in range(members)] for tiles in tile_of]

    def seat(g, j):
        return g * members + holder[g // HALVES % 2][j]

    def local(lidar, camera, joined_weight, joined_bias, block_weight, block_bias, down_weight, down_bias, proj_weight, proj_bias):
        frames, sh, cols, lidar_ch = lidar.shape
        rows, sc, cam_ch = camera.shape[1:]
        tr = sh * members
        tw = cols // members
        wide = tw + 2 * SIDE
        pitch = rounded(wide, 16)
        w = cols // n_cols
        joined = joined_weight.shape[3]
        block = block_weight.shape[3]
        place = lax.axis_index(AXES)
        group = place // members
        member = place % members
        cindex = lax.axis_index("cols")
        kgroup = cindex // members

        def send(x, pairs):
            return lax.ppermute(x, AXES, pairs)

        def across(x, by_group, by_column):
            pairs = []
            for g in range(groups):
                for j in range(members):
                    if 0 <= g + by_group < groups and 0 <= j + by_column < members:
                        pairs.append((seat(g, j), seat(g + by_group, j + by_column)))
            return send(x, pairs)

        def column_of(m):
            return jnp.where(m < half, 2 * m, 2 * (members - 1 - m) + 1) ^ (turn * (group // HALVES % 2))

        joint = joined_weight.reshape(-1, joined)
        square = block_weight.reshape(-1, block)
        deep1 = 3 * (3 * lidar_ch + rounded(3 * cam_ch, 256))
        w1, w2 = pl.pallas_call(
            lambda *refs: weights_kernel(*refs, lidar=lidar_ch, camera=cam_ch),
            out_shape=[
                jax.ShapeDtypeStruct((deep1, joined), BF),
                jax.ShapeDtypeStruct((4 * 3 * joined, 2 * block), BF),
            ],
            compiler_params=limit(14),
            name="weights",
        )(joint, square)
        w3 = down_weight.reshape(-1, down_weight.shape[3])
        b1 = joined_bias.reshape(1, -1)
        b2 = jnp.concatenate([block_bias, block_bias]).reshape(1, -1)
        b3 = down_bias.reshape(1, -1)
        bp = proj_bias.reshape(1, -1)

        span = rounded(tr + UP + DOWN, 8)
        lanes = frames * span
        turned = jnp.transpose(camera, (0, 2, 3, 1))
        strip = jax.ShapeDtypeStruct((sc, cam_ch, lanes), BF)
        rim = jax.ShapeDtypeStruct((UP, cam_ch, lanes), BF)
        packed = pl.pallas_call(
            lambda *refs: camera_pack_kernel(*refs, tr=tr, span=span),
            grid_spec=pltpu.PrefetchScalarGridSpec(
                num_scalar_prefetch=1,
                grid=(1,),
                in_specs=[whole(turned)],
                out_specs=[whole(strip)] * groups + [whole(rim)] * groups,
            ),
            out_shape=[strip] * groups + [rim] * groups,
            compiler_params=limit(14),
            name="camera_pack",
        )(place.reshape(1).astype(jnp.int32), turned)
        arrived = [send(packed[p], [(s, seat((s + p) % groups, s // groups)) for s in range(total)]) for p in range(groups)]
        for e in range(groups):
            pairs = [(groups * j + groups - 1, seat(e, j + 1)) for j in range(members - 1)]
            pairs += [(groups * j, seat((e + 1) % groups, j - 1)) for j in range(1, members)]
            arrived.append(send(packed[groups + e], pairs))
        cam = pl.pallas_call(
            lambda *refs: camera_unpack_kernel(*refs, groups=groups, sc=sc, cam_ch=cam_ch),
            grid_spec=pltpu.PrefetchScalarGridSpec(
                num_scalar_prefetch=1,
                grid=(1,),
                in_specs=[whole(x) for x in arrived],
                out_specs=pl.BlockSpec((lanes, pitch, rounded(3 * cam_ch, 256)), lambda i, p: (0, 0, 0)),
                scratch_shapes=[
                    pltpu.VMEM((tw + UP + DOWN, cam_ch, lanes), BF),
                    pltpu.VMEM((lanes, pitch, 128), jnp.float32),
                ],
            ),
            out_shape=jax.ShapeDtypeStruct((lanes, pitch, rounded(3 * cam_ch, 256)), BF),
            compiler_params=limit(16),
            name="camera_unpack",
        )(group.reshape(1).astype(jnp.int32), *arrived)
        cam = cam.reshape(frames, span, pitch, -1)

        pos = jnp.stack([group, member, kgroup, column_of(member)]).astype(jnp.int32)
        pairs2 = (tr + 2) // 2
        half_rows = tr // 2
        n = HALVES * half_rows
        jd = rounded(w // 2, 8)
        flops = 2 * pitch * ((tr + 4) * w1.shape[0] * joined + pairs2 * w2.shape[0] * 2 * block)
        framed = lambda a: pl.BlockSpec((1,) + a.shape[1:], lambda f, p: (f,) + (0,) * (a.ndim - 1))
        encoded = None
        step = frames // CHUNKS
        for f0 in range(0, frames, step):
            source = lidar if not f0 else lax.optimization_barrier((lidar, packed[0]))[0]
            window = jax.ShapeDtypeStruct((step, sh, wide, lidar_ch), BF)
            windows = pl.pallas_call(
                functools.partial(window_kernel, tw=tw),
                grid_spec=pltpu.PrefetchScalarGridSpec(
                    num_scalar_prefetch=1,
                    grid=(step,),
                    in_specs=[pl.BlockSpec((1, sh, cols, lidar_ch), lambda f, p, f0=f0: (f + f0, 0, 0, 0))],
                    out_specs=[framed(window)] * members,
                ),
                out_shape=[window] * members,
                compiler_params=limit(6),
            )(jnp.stack([column_of((member + d) % members) for d in range(members)]).astype(jnp.int32), source)
            windows = [windows[0]] + [
                send(windows[d], [(g * members + m, g * members + (m + d) % members) for g in range(groups) for m in range(members)])
                for d in range(1, members)
            ]
            last, head = pick(windows, (member + 1) % members, member, 1)
            above, below = across(last, 1, 0), across(head, -1, 0)
            shifts = []
            for h in range(HALVES):
                shift = []
                for s in range(total):
                    r, c = divmod(s, n_cols)
                    k, m = divmod(c, members)
                    shift.append((s, r * n_cols + HALVES * tile_of[r % 2][m] + (k + h) % HALVES))
                shifts.append(shift)
            vmem = pl.BlockSpec(memory_space=pltpu.VMEM)
            for b0, many in [(0, step)] if f0 == 0 else [(f, 1) for f in range(step)]:
                blocks = jax.ShapeDtypeStruct((many, pairs2, 2, w, block), BF)
                tiles = pl.pallas_call(
                    functools.partial(conv_kernel, parts=members, sh=sh, tr=tr, pitch=pitch, rows=rows, cols=cols, at=b0, cam_at=f0 + b0, rim_at=b0, many=many),
                    in_specs=[pl.BlockSpec(memory_space=pltpu.SMEM)] + [vmem] * (members + 7),
                    out_specs=[vmem] * HALVES,
                    scratch_shapes=conv_scratch(tr, pitch, lidar_ch, joined, block, pairs2),
                    out_shape=[blocks] * HALVES,
                    compiler_params=limit(20),
                    cost_estimate=pl.CostEstimate(flops=flops * many, bytes_accessed=2 * 10**6, transcendentals=0),
                )(pos, *windows, above, below, cam, w1, b1, w2, b2)
                pieces = []
                for h in range(HALVES):
                    pieces.append(send(tiles[h], shifts[h]))
                old = [] if encoded is None else [encoded]
                encoded = pl.pallas_call(
                    lambda *refs: encode_kernel(*refs, parts=HALVES, half_rows=half_rows, w=w),
                    grid_spec=pltpu.PrefetchScalarGridSpec(
                        num_scalar_prefetch=1,
                        grid=(many,),
                        in_specs=[framed(x) for x in pieces] + [whole(x) for x in (w3, b3, proj_weight, bp)] + [pl.BlockSpec(memory_space=pl.ANY)] * len(old),
                        out_specs=pl.BlockSpec((1, n, 2, w, 2 * block), lambda f, p, lo=f0 + b0: (f + lo, 0, 0, 0, 0)),
                        scratch_shapes=[
                            pltpu.VMEM((n + 1, 2, rounded(w + 1, 8) + 16, block), jnp.float32),
                            pltpu.VMEM((n, 2 * jd, block), jnp.float32),
                        ],
                    ),
                    out_shape=jax.ShapeDtypeStruct((frames, n, 2, w, 2 * block), BF),
                    input_output_aliases={5 + HALVES: 0} if old else {},
                    compiler_params=limit(12),
                    cost_estimate=pl.CostEstimate(flops=2 * many * n * jd * w3.shape[0] * 256, bytes_accessed=many * 10**6, transcendentals=0),
                )(cindex.reshape(1).astype(jnp.int32), *pieces, w3, b3, proj_weight, bp, *old)
        return encoded.reshape(frames, 2 * n, w, 2 * block)

    return jax.shard_map(
        local,
        mesh=mesh,
        in_specs=(
            P("frames", AXES, None, None),
            P("frames", None, AXES, None),
            P(), P(), P(), P(), P(), P(), P(), P(),
        ),
        out_specs=P("frames", "rows", "cols", None),
        check_vma=False,
    )
```
